16 devices in a mesh: stage: 2 (over z), data: 8 (over y, x, core).
Axes of the slice: x: 2, y: 2, z: 2, core: 2. Of those that a mesh axis runs over, the one named last changes fastest.
Arguments:
- tokens_in: bfloat16 [16, 512, 896], P('data')
- targets: bfloat16 [16, 512, 896], P('data')
- w_up: bfloat16 [2, 6, 896, 4864], P(None, 'stage')
- w_down: bfloat16 [2, 6, 4864, 896], P(None, 'stage')
Outputs:
- output 1: float32 [], replicated
- output 2: float32 [2, 6, 896, 4864], P(None, 'stage', 'data')
- output 3: float32 [2, 6, 4864, 896], P(None, 'stage', 'data')
All inputs are finite; a program needn't handle non-finite values.
Results may differ from the reference program's by a relative error of at most 0.00136694.
Values are sent between devices in bfloat16 or wider.
A program may use at most 1 GiB of HBM per device.

```python
import jax
import jax.numpy as jnp
from jax import lax

D_MODEL = 896
FF = 4864
TOKENS = 512
BATCH_MB = 16
HALF_LAYERS = 6
N_LAYERS = 2 * HALF_LAYERS
N_TOKENS = BATCH_MB * TOKENS


def setup_inputs(seed: int = 0) -> dict:
    key_list = jax.random.split(jax.random.key(seed), 8)
    noise_in = jax.random.normal(key_list[0], (BATCH_MB, TOKENS, D_MODEL), jnp.float32)
    shift_in = 2.0 * jax.random.normal(key_list[1], (BATCH_MB, 1, D_MODEL), jnp.float32)
    noise_out = jax.random.normal(key_list[2], (BATCH_MB, TOKENS, D_MODEL), jnp.float32)
    shift_out = 2.0 * jax.random.normal(key_list[3], (BATCH_MB, 1, D_MODEL), jnp.float32)
    in_gain = jnp.exp(jax.random.uniform(key_list[6], (), jnp.float32, -0.8, 0.8))
    out_gain = jnp.exp(jax.random.uniform(key_list[7], (), jnp.float32, -1.0, 1.0))
    up_scale = D_MODEL ** -0.5
    down_scale = (2.0 / (N_LAYERS * FF)) ** 0.5
    w_up = up_scale * jax.random.normal(key_list[4], (2, HALF_LAYERS, D_MODEL, FF), jnp.float32)
    w_down = down_scale * jax.random.normal(key_list[5], (2, HALF_LAYERS, FF, D_MODEL), jnp.float32)
    return {
        "tokens_in": ((noise_in + shift_in) * in_gain).astype(jnp.bfloat16),
        "targets": ((noise_out + shift_out) * out_gain).astype(jnp.bfloat16),
        "w_up": w_up.astype(jnp.bfloat16),
        "w_down": w_down.astype(jnp.bfloat16),
    }


def gelu_fn(pre_act):
    return jax.nn.gelu(pre_act, approximate=True)


def layer_fwd(h_in, w_one, w_two):
    pre_act = jnp.dot(h_in, w_one, preferred_element_type=jnp.float32)
    act_bf = gelu_fn(pre_act).astype(jnp.bfloat16)
    out_val = h_in.astype(jnp.float32) + jnp.dot(act_bf, w_two, preferred_element_type=jnp.float32)
    return out_val.astype(jnp.bfloat16)


def layer_bwd(h_in, grad_out, w_one, w_two):
    pre_act = jnp.dot(h_in, w_one, preferred_element_type=jnp.float32)
    act_val, gelu_vjp = jax.vjp(gelu_fn, pre_act)
    act_bf = act_val.astype(jnp.bfloat16)
    g_down = jnp.dot(act_bf.T, grad_out, preferred_element_type=jnp.float32)
    d_act = jnp.dot(grad_out, w_two.T, preferred_element_type=jnp.float32).astype(jnp.bfloat16)
    d_pre = gelu_vjp(d_act.astype(jnp.float32))[0].astype(jnp.bfloat16)
    g_up = jnp.dot(h_in.T, d_pre, preferred_element_type=jnp.float32)
    back_val = jnp.dot(d_pre, w_one.T, preferred_element_type=jnp.float32)
    d_in = (grad_out.astype(jnp.float32) + back_val).astype(jnp.bfloat16)
    return d_in, g_up, g_down


def reference(tokens_in, targets, w_up, w_down):
    up_flat = w_up.reshape(N_LAYERS, D_MODEL, FF)
    down_flat = w_down.reshape(N_LAYERS, FF, D_MODEL)

    def fwd_body(h_cur, layer_w):
        return layer_fwd(h_cur, layer_w[0], layer_w[1]), h_cur

    def bwd_body(g_cur, layer_items):
        d_in, g_up, g_down = layer_bwd(layer_items[0], g_cur, layer_items[1], layer_items[2])
        return d_in, (g_up, g_down)

    def micro_step(scan_state, mb_pair):
        loss_acc, acc_up, acc_down = scan_state
        h_last, saved_in = lax.scan(fwd_body, mb_pair[0], (up_flat, down_flat))
        out_err = h_last.astype(jnp.float32) - mb_pair[1].astype(jnp.float32)
        loss_acc = loss_acc + jnp.sum(out_err * out_err) / (2.0 * N_TOKENS)
        grad_top = (out_err / N_TOKENS).astype(jnp.bfloat16)
        _, (g_ups, g_downs) = lax.scan(bwd_body, grad_top, (saved_in, up_flat, down_flat), reverse=True)
        return (loss_acc, acc_up + g_ups, acc_down + g_downs), None

    init_state = (
        jnp.zeros((), jnp.float32),
        jnp.zeros((N_LAYERS, D_MODEL, FF), jnp.float32),
        jnp.zeros((N_LAYERS, FF, D_MODEL), jnp.float32),
    )
    (loss, acc_up, acc_down), _ = lax.scan(micro_step, init_state, (tokens_in, targets))
    return loss, acc_up.reshape(2, HALF_LAYERS, D_MODEL, FF), acc_down.reshape(2, HALF_LAYERS, FF, D_MODEL)
```

```python
import jax
import jax.numpy as jnp
import numpy as np
from jax import lax
from jax.experimental import pallas as pl
from jax.experimental.pallas import tpu as pltpu
from jax.sharding import PartitionSpec as P


F32, BF16 = jnp.float32, jnp.bfloat16
N_CHUNK = 4
LAG = 2
AXIS_OF = ("y", "x", "y")
BIT = {"y": 4, "x": 2, "core": 1}
NT = (((1,), (1,)), ((), ()))
TN = (((0,), (0,)), ((), ()))
C0 = 0.7978845608028654
C1 = 0.044715
ANY = pl.BlockSpec(memory_space=pl.ANY)


def gelu(z):
    return z * (0.5 * (1.0 + jnp.tanh(C0 * (z + C1 * (z * z * z)))))


def gelu_and_slope(z):
    z2 = z * z
    t = jnp.tanh(C0 * (z + C1 * (z2 * z)))
    cdf = 0.5 * (1.0 + t)
    slope = cdf + (0.5 * z) * ((1.0 - t * t) * (C0 + (3.0 * C0 * C1) * z2))
    return cdf * z, slope


def params(n_dims, vmem):
    return pltpu.CompilerParams(dimension_semantics=("arbitrary",) * n_dims, vmem_limit_bytes=vmem * 2**20)


def flops(n):
    return pl.CostEstimate(flops=int(n), bytes_accessed=0, transcendentals=0)


SLOT = {0: ("y", 0), 1: ("x", 0), 2: ("y", 1)}

FWD_AT = 1
BWD_AT = FWD_AT + 2 * N_CHUNK + LAG
_GRAD_AT = BWD_AT + 2 * (2 * N_CHUNK + LAG)
GRAD_AT = {"y": _GRAD_AT, "x": _GRAD_AT + 16}


def schedule(n_data, d, ff, width):
    n_q = 2 * N_CHUNK
    table = []
    for stage in range(2):
        for dev in range(n_data):
            row = [stage]
            for t in range(n_q + LAG):
                row.append(min(max(t - LAG * stage, 0), n_q - 1) // N_CHUNK)
            for t in range(n_q + LAG):
                q = min(max(t - LAG * (1 - stage), 0), n_q - 1)
                virt = 1 - q // N_CHUNK
                row += [virt, N_CHUNK * virt + q % N_CHUNK + LAG * stage]
            y, x, c = dev // 4, (dev // 2) % 2, dev % 2
            seg, spare = ff // n_data, ff // 2 - width
            for axis in "yx":
                a, b = (y, x) if axis == "y" else (x, y)

                def window(a_, c_):
                    p, q = (a_, c_) if axis == "y" else (c_, a_)
                    return (ff // 2) * p + spare * q, (ff // 4 - spare) * q

                start, base = window(a, c)
                row += [start, base + seg * c, base + seg * (1 - c)]
                for i in range(8):
                    b_ = b if i < 4 else 1 - b
                    a_ = a if (i // 2) % 2 == 0 else 1 - a
                    c_ = c if i % 2 == 0 else 1 - c
                    y_, x_ = (a_, b_) if axis == "y" else (b_, a_)
                    row.append((d // n_data) * (4 * y_ + 2 * x_ + c_))
                row.append(int(b == c))
                for a_, c_ in ((a, c), (1 - a, c), (a, 1 - c), (1 - a, 1 - c)):
                    row.append(window(a_, c_)[0])
            table.append(row)
    return np.array(table, np.int32)


def write_pairs(k, value, y_ref, x_ref):
    axis, i = SLOT[k]
    (y_ref if axis == "y" else x_ref)[0, i] = value


def fwd_kernel(n_f, scal, h_ref, wu_ref, wd_ref, tok, *rest):
    big_ref, py_ref, px_ref, out_ref, _, cur, acc = rest[-7:]
    l, f = pl.program_id(0), pl.program_id(1)

    @pl.when((l == 0) & (f == 0))
    def _():
        cur[...] = h_ref[...]

    @pl.when(f == 0)
    def _():
        big_ref[0, 0] = cur[...]
        acc[...] = cur[...].astype(F32)
        for k in range(3):
            pl.when(l == k)(lambda k=k: write_pairs(k, cur[...], py_ref, px_ref))

    z = jnp.dot(cur[...], wu_ref[0, 0], preferred_element_type=F32)
    a = gelu(z).astype(BF16)
    acc[...] += jnp.dot(a, wd_ref[0, 0], preferred_element_type=F32)

    @pl.when(f == n_f - 1)
    def _():
        cur[...] = acc[...].astype(BF16)
        out_ref[...] = cur[...]


def bwd_kernel(n_f, scal, st_ref, g_ref, wu_ref, wd_ref, tok, *rest):
    py_ref, px_ref, out_ref, _, cur, acc = rest[-6:]
    l, f = pl.program_id(0), pl.program_id(1)

    @pl.when((l == 0) & (f == 0))
    def _():
        cur[...] = g_ref[...]

    @pl.when(f == 0)
    def _():
        acc[...] = cur[...].astype(F32)
        for k in range(3):
            pl.when(l == 2 - k)(lambda k=k: write_pairs(k, cur[...], py_ref, px_ref))

    z = jnp.dot(st_ref[0, 0], wu_ref[0, 0], preferred_element_type=F32)
    da = lax.dot_general(cur[...], wd_ref[0, 0], NT, preferred_element_type=F32).astype(BF16).astype(F32)
    _, slope = gelu_and_slope(z)
    dz = (slope * da).astype(BF16)
    acc[...] += lax.dot_general(dz, wu_ref[0, 0], NT, preferred_element_type=F32)

    @pl.when(f == n_f - 1)
    def _():
        cur[...] = acc[...].astype(BF16)
        out_ref[...] = cur[...]


def tick_call(kind, t, scal, at, ins, wu, wd, tok, big, pairs):
    rows, d = ins[-1].shape
    ff = wu.shape[-1]
    tf = ff // 2
    n_f = ff // tf
    fwd = kind == "fwd"
    lay = (lambda l: l) if fwd else (lambda l: 2 - l)
    in_specs = []
    if not fwd:
        in_specs.append(pl.BlockSpec((1, 1, rows, d), lambda l, f, s: (s[at + 1], 2 - l, 0, 0)))
    in_specs += [
        pl.BlockSpec(memory_space=pltpu.VMEM),
        pl.BlockSpec((1, 1, d, tf), lambda l, f, s: (s[at], lay(l), 0, f)),
        pl.BlockSpec((1, 1, tf, d), lambda l, f, s: (s[at], lay(l), f, 0)),
        ANY,
    ]
    args = [*ins, wu, wd, tok]
    out_specs, out_shape, alias = [], [], {}

    def out(spec, shape, dtype, source=None):
        if source is not None:
            alias[1 + len(args)] = len(out_shape)
            args.append(source)
            in_specs.append(ANY)
        out_specs.append(spec)
        out_shape.append(jax.ShapeDtypeStruct(shape, dtype))

    if fwd:
        n_ticks = 2 * N_CHUNK + LAG
        out(pl.BlockSpec((1, 1, rows, d), lambda l, f, s: (t, l, 0, 0)), (n_ticks, 3, rows, d), BF16, big)
    for i, axis in enumerate("yx"):
        n = AXIS_OF.count(axis)
        out(
            pl.BlockSpec((1, n, rows, d), lambda l, f, s: (t % 2, 0, 0, 0)),
            (2, n, rows, d),
            BF16,
            pairs[i] if pairs is not None else None,
        )
    out(pl.BlockSpec((rows, d), lambda l, f, s: (0, 0)), (rows, d), BF16)
    alias[1 + len(ins) + 2] = len(out_shape)
    out_specs.append(ANY)
    out_shape.append(jax.ShapeDtypeStruct(tok.shape, tok.dtype))
    body = fwd_kernel if fwd else bwd_kernel
    return pl.pallas_call(
        lambda *r: body(n_f, *r),
        grid_spec=pltpu.PrefetchScalarGridSpec(
            num_scalar_prefetch=1,
            grid=(3, n_f),
            in_specs=in_specs,
            out_specs=out_specs,
            scratch_shapes=[pltpu.VMEM((rows, d), BF16), pltpu.VMEM((rows, d), F32)],
        ),
        out_shape=out_shape,
        input_output_aliases=alias,
        compiler_params=params(2, 44),
        cost_estimate=flops((2 if fwd else 3) * 2 * 3 * rows * d * ff),
        name=f"{kind}_tick",
    )(scal, *args)


def wgrad_kernel(v, k, n_step, at, scal, wu, wd, tok, *rest):
    hs, gs = rest[:12], rest[12:24]
    down_ref, up_refs = rest[24], rest[25:27]
    wub, wdb, hb, gb, gd, gu, wsem, hsem, gsem, osem = rest[28:]
    t = pl.program_id(0)
    s, start = scal[0], pl.multiple_of(scal[at], 128)
    i_layer = SLOT[k][1]
    width = wub.shape[1]

    copies = [
        pltpu.make_async_copy(wu.at[v, k, :, pl.ds(start, width)], wub, wsem.at[0]),
        pltpu.make_async_copy(wd.at[v, k, pl.ds(start, width), :], wdb, wsem.at[1]),
    ]

    def fetch(step, slot):
        for j in range(2):
            for m in range(4):
                for sv in range(2):

                    @pl.when((step == j * 4 + m) & (s == sv))
                    def _():
                        pltpu.make_async_copy(hs[(sv + j) * 4 + m].at[:, i_layer], hb.at[slot], hsem.at[slot]).start()
                        pltpu.make_async_copy(gs[(1 - sv + j) * 4 + m].at[:, i_layer], gb.at[slot], gsem.at[slot]).start()

    @pl.when(t == 0)
    def _():
        fetch(0, 0)
        for cp in copies:
            cp.start()
        gd[...] = jnp.zeros_like(gd)
        gu[...] = jnp.zeros_like(gu)

    @pl.when(t + 1 < n_step)
    def _():
        fetch(t + 1, (t + 1) % 2)

    slot = t % 2
    pltpu.make_async_copy(hs[0].at[:, i_layer], hb.at[slot], hsem.at[slot]).wait()
    pltpu.make_async_copy(gs[0].at[:, i_layer], gb.at[slot], gsem.at[slot]).wait()

    @pl.when(t == 0)
    def _():
        for cp in copies:
            cp.wait()

    h = hb[slot].reshape(-1, hb.shape[-1])
    g = gb[slot].reshape(-1, gb.shape[-1])
    z = jnp.dot(h, wub[...], preferred_element_type=F32)
    da = lax.dot_general(g, wdb[...], NT, preferred_element_type=F32).astype(BF16).astype(F32)
    a, slope = gelu_and_slope(z)
    a = a.astype(BF16)
    dz = (slope * da).astype(BF16)
    gd[...] += lax.dot_general(a, g, TN, preferred_element_type=F32)
    gu[...] += lax.dot_general(h, dz, TN, preferred_element_type=F32)

    @pl.when(t == n_step - 1)
    def _():
        outs = []
        rows_d = down_ref.shape[1]
        for i in range(2):
            src = pl.multiple_of(scal[at + 1 + i], 8)
            outs.append(pltpu.make_async_copy(gd.at[pl.ds(src, rows_d), :], down_ref.at[i], osem.at[i]))
        rows_u = up_refs[0].shape[2]
        for i in range(8):
            src = pl.multiple_of(scal[at + 3 + i], 8)
            outs.append(
                pltpu.make_async_copy(
                    gu.at[pl.ds(src, rows_u), :], up_refs[i // 4].at[(i // 2) % 2, i % 2], osem.at[2 + i]
                )
            )
        for cp in outs:
            cp.start()
        for cp in outs:
            cp.wait()


def wgrad_call(v, k, scal, at, wu, wd, tok, hs, gs, width, n_data):
    d, ff = wu.shape[2:]
    n_tick, _, rows, _ = hs[0].shape
    n_step = 8
    return pl.pallas_call(
        lambda *r: wgrad_kernel(v, k, n_step, at, *r),
        grid_spec=pltpu.PrefetchScalarGridSpec(
            num_scalar_prefetch=1,
            grid=(n_step,),
            in_specs=[ANY] * 27,
            out_specs=[ANY] * 4,
            scratch_shapes=[
                pltpu.VMEM((d, width), BF16),
                pltpu.VMEM((width, d), BF16),
                pltpu.VMEM((2, n_tick, rows, d), BF16),
                pltpu.VMEM((2, n_tick, rows, d), BF16),
                pltpu.VMEM((width, d), F32),
                pltpu.VMEM((d, width), F32),
                pltpu.SemaphoreType.DMA((2,)),
                pltpu.SemaphoreType.DMA((2,)),
                pltpu.SemaphoreType.DMA((2,)),
                pltpu.SemaphoreType.DMA((10,)),
            ],
        ),
        out_shape=[
            jax.ShapeDtypeStruct((2, ff // n_data, d), F32),
            jax.ShapeDtypeStruct((2, 2, d // n_data, width), F32),
            jax.ShapeDtypeStruct((2, 2, d // n_data, width), F32),
            jax.ShapeDtypeStruct(tok.shape, tok.dtype),
        ],
        input_output_aliases={3: 3},
        compiler_params=params(1, 60),
        cost_estimate=flops(4 * 2 * 4 * n_tick * rows * 2 * d * width),
        name=f"wgrad_{v}_{k}",
    )(scal, wu, wd, tok, *hs, *gs)


def final_kernel(at, scal, own, recv, core, p0, p1, p2, p3, *rest):
    down_ref, up_ref = rest[-2:]
    r = pl.program_id(0)
    down_ref[0, 0] = jnp.where(scal[at] == 1, own[0] + recv[0], core[...])

    @pl.when(r == 0)
    def _():
        width = p0.shape[-1]
        for i, piece in enumerate((p0, p1, p2, p3)):
            up_ref[0, 0, :, pl.ds(pl.multiple_of(scal[at + 1 + i], 128), width)] = piece[...]


def final_call(v, k, scal, at, down, recv, core, pieces, outs, shapes):
    rows, d = core.shape
    n_r = 4
    step = rows // n_r
    blk = pl.BlockSpec((step, d), lambda r, s: (r, 0))
    full = pl.BlockSpec(pieces[0].shape, lambda r, s: (0, 0))
    args = [down, recv, core, *pieces]
    first = pl.BlockSpec((1, step, d), lambda r, s: (0, r, 0))
    in_specs = [first, first, blk] + [full] * 4
    alias = {}
    if outs is not None:
        alias = {1 + len(args) + i: i for i in range(2)}
        args += outs
        in_specs += [ANY] * 2
    (_, _, ru, ff) = shapes[1]
    return pl.pallas_call(
        lambda *r: final_kernel(at, *r),
        grid_spec=pltpu.PrefetchScalarGridSpec(
            num_scalar_prefetch=1,
            grid=(n_r,),
            in_specs=in_specs,
            out_specs=[
                pl.BlockSpec((1, 1, step, d), lambda r, s: (v, k, r, 0)),
                pl.BlockSpec((1, 1, ru, ff), lambda r, s: (v, k, 0, 0)),
            ],
        ),
        out_shape=[jax.ShapeDtypeStruct(shape, F32) for shape in shapes],
        input_output_aliases=alias,
        compiler_params=params(1, 32),
        cost_estimate=flops(4e9),
        name="final",
    )(scal, *args)


def solution(mesh):
    n_stage = mesh.shape["stage"]
    n_data = mesh.shape["data"]

    def swap(value, axis):
        if axis == "stage":
            return lax.ppermute(value, "stage", [(i, (i + 1) % n_stage) for i in range(n_stage)])
        return lax.ppermute(value, "data", [(i, i ^ BIT[axis]) for i in range(n_data)])

    def exchange(pairs):
        got = {}
        for axis, own in zip("yx", pairs):
            far = swap(own, axis)
            got[axis] = (own, far, swap(own, "core"), swap(far, "core"))
        return got

    def device_fn(tokens_loc, targets_loc, wu, wd):
        n_micro, seq_len, d = tokens_loc.shape
        n_tok = n_data * n_micro * seq_len
        ff = wu.shape[-1]
        rows = n_micro * seq_len // N_CHUNK
        width = (ff // 4 + 127) // 128 * 128
        stage = lax.axis_index("stage")
        dev = lax.axis_index("data")
        tokens = tokens_loc.reshape(N_CHUNK, rows, d)
        targets = targets_loc.reshape(N_CHUNK, rows, d)
        n_q = 2 * N_CHUNK
        n_ticks = n_q + LAG
        tok = jnp.zeros((8, 128), F32)

        scal = lax.dynamic_index_in_dim(jnp.asarray(schedule(n_data, d, ff, width)), stage * n_data + dev, 0, keepdims=False)
        here = {axis: scal[GRAD_AT[axis] + 11] == 1 for axis in "yx"}

        raw, hop, h_ex = [], [], []
        big, pairs = None, None
        for t in range(n_ticks):
            h_in = tokens[t] if t < LAG else hop[t - LAG]
            if LAG <= t < N_CHUNK:
                h_in = jnp.where(stage == 0, tokens[t], h_in)
            big, py, px, out, tok = tick_call("fwd", t, scal, FWD_AT + t, [h_in], wu, wd, tok, big, pairs)
            raw.append(out)
            if t < n_q:
                hop.append(swap(out, "stage"))
            pairs = (py, px)
            if t % 2 == 1:
                h_ex.append(exchange(pairs))
                pairs = None

        top = [r.astype(F32) - targets[m].astype(F32) for m, r in enumerate(raw[-N_CHUNK:])]
        loss = sum(jnp.sum(e * e) for e in top) / (2.0 * n_tok)
        loss = jnp.broadcast_to(jnp.where(stage == n_stage - 1, loss, 0.0), (8, 128))
        g_top = [(e / n_tok).astype(BF16) for e in top]

        hop, g_ex = [], []
        pairs = None

        def bwd_tick(t, tok, pairs):
            g_in = g_top[t] if t < LAG else hop[t - LAG]
            if LAG <= t < N_CHUNK:
                g_in = jnp.where(stage == n_stage - 1, g_top[t], g_in)
            py, px, out, tok = tick_call("bwd", t, scal, BWD_AT + 2 * t, [big, g_in], wu, wd, tok, None, pairs)
            if t < n_q:
                hop.append(swap(out, "stage"))
            if t % 2 == 1:
                g_ex.append(exchange((py, px)))
                return tok, None
            return tok, (py, px)

        shapes = ((2, 3, ff // n_data, d), (2, 3, d // n_data, ff))
        state = {}

        def wgrad(v, k, tok):
            axis = AXIS_OF[k]
            other = "x" if axis == "y" else "y"
            hs = [m for e in h_ex[2 * v : 2 * v + 3] for m in e[axis]]
            gs = [m for e in g_ex[2 * (1 - v) : 2 * (1 - v) + 3] for m in e[axis]]
            down, up_keep, up_send, tok = wgrad_call(v, k, scal, GRAD_AT[axis], wu, wd, tok, hs, gs, width, n_data)
            other = "x" if axis == "y" else "y"
            far = BIT[other]
            pairs_ = [(i, i ^ far) for i in range(n_data) if (i % 2 == 1) != bool(i & far)]
            state[v, k] = {
                "down": down,
                "keep": up_keep,
                "down_b": lax.ppermute(down, "data", pairs_),
                "up_b": swap(up_send, other),
            }
            return tok

        def first_sum(v, k, tok):
            st = state[v, k]
            down_b, up_b, tok = lax.optimization_barrier((st["down_b"], st["up_b"], tok))
            keep = st["keep"]
            st["down_b"] = down_b
            to_a = keep[1] + up_b[1]
            to_core = keep[0, 1] + up_b[0, 1]
            st["mine"] = keep[0, 0] + up_b[0, 0]
            down_o = st["down"][1] + down_b[1]
            to_a, to_core, down_o, tok = lax.optimization_barrier((to_a, to_core, down_o, tok))
            st["up_a"] = swap(to_a, AXIS_OF[k])
            st["up_c"] = swap(to_core, "core")
            st["down_c"] = swap(down_o, "core")
            return tok

        def second_swap(v, k, tok):
            st = state[v, k]
            up_a, tok = lax.optimization_barrier((st["up_a"], tok))
            to_core, st["up_a"] = up_a[1], up_a[0]
            to_core, tok = lax.optimization_barrier((to_core, tok))
            st["up_ac"] = swap(to_core, "core")
            return tok

        def finish(v, k, grads):
            st = state[v, k]
            pieces = [st["mine"], st["up_a"], st["up_c"], st["up_ac"]]
            at = GRAD_AT[AXIS_OF[k]] + 11
            return final_call(v, k, scal, at, st["down"], st["down_b"], st["down_c"], pieces, grads, shapes)

        for t in range(n_q):
            tok, pairs = bwd_tick(t, tok, pairs)
            if t < 4:
                axis = ("core", "x", "y", "stage")[t]
                loss, tok = lax.optimization_barrier((loss + swap(loss, axis), tok))
        tok = wgrad(1, 2, tok)
        for t in range(n_q, n_ticks):
            tok, pairs = bwd_tick(t, tok, pairs)
        tok = wgrad(1, 0, tok)
        tok = wgrad(1, 1, tok)
        tok = first_sum(1, 2, tok)
        tok = wgrad(0, 2, tok)
        tok = first_sum(1, 0, tok)
        tok = second_swap(1, 2, tok)
        tok = wgrad(0, 0, tok)
        tok = first_sum(1, 1, tok)
        tok = second_swap(1, 0, tok)
        tok = wgrad(0, 1, tok)
        tok = second_swap(1, 1, tok)
        tok = first_sum(0, 2, tok)
        grads = None
        for k in (2, 0, 1):
            grads = finish(1, k, grads)
        tok = second_swap(0, 2, tok)
        tok = first_sum(0, 1, tok)
        grads = finish(0, 2, grads)
        tok = second_swap(0, 1, tok)
        tok = first_sum(0, 0, tok)
        grads = finish(0, 1, grads)
        tok = second_swap(0, 0, tok)
        grads = finish(0, 0, grads)
        loss = loss[0, 0]
        return loss, grads[1], grads[0]

    return jax.shard_map(
        device_fn,
        mesh=mesh,
        in_specs=(P("data"), P("data"), P(None, "stage"), P(None, "stage")),
        out_specs=(P(), P(None, "stage", "data"), P(None, "stage", "data")),
        check_vma=False,
    )
```

```python
import jax
import jax.numpy as jnp
import numpy as np
from jax import lax
from jax.experimental import pallas as pl
from jax.experimental.pallas import tpu as pltpu
from jax.sharding import PartitionSpec as P


F32, BF16 = jnp.float32, jnp.bfloat16
N_CHUNK = 4
DELAY = 6
N_RECV = 16
MESH = pl.DeviceIdType.MESH
BIT = {"y": 4, "x": 2, "core": 1}
NT = (((1,), (1,)), ((), ()))
TN = (((0,), (0,)), ((), ()))
C0 = 0.7978845608028654
C1 = 0.044715
ANY = pl.BlockSpec(memory_space=pl.ANY)


def gelu(z):
    return z * (0.5 * (1.0 + jnp.tanh(C0 * (z + C1 * (z * z * z)))))


def gelu_and_slope(z):
    z2 = z * z
    t = jnp.tanh(C0 * (z + C1 * (z2 * z)))
    cdf = 0.5 * (1.0 + t)
    slope = cdf + (0.5 * z) * ((1.0 - t * t) * (C0 + (3.0 * C0 * C1) * z2))
    return cdf * z, slope


def params(n_dims, vmem):
    return pltpu.CompilerParams(dimension_semantics=("arbitrary",) * n_dims, vmem_limit_bytes=vmem * 2**20)


def flops(n):
    return pl.CostEstimate(flops=int(n), bytes_accessed=0, transcendentals=0)


GRAD_AT = {"y": 0, "x": 16}


def schedule(n_data, d, ff, width):
    table = []
    for dev in range(n_data):
        row = []
        y, x, c = dev // 4, (dev // 2) % 2, dev % 2
        seg, spare = ff // n_data, ff // 2 - width
        for axis in "yx":
            a, b = (y, x) if axis == "y" else (x, y)

            def window(a_, c_):
                p, q = (a_, c_) if axis == "y" else (c_, a_)
                return (ff // 2) * p + spare * q, (ff // 4 - spare) * q

            start, base = window(a, c)
            row += [start, base + seg * c, base + seg * (1 - c)]
            for i in range(8):
                b_ = b if i < 4 else 1 - b
                a_ = a if (i // 2) % 2 == 0 else 1 - a
                c_ = c if i % 2 == 0 else 1 - c
                y_, x_ = (a_, b_) if axis == "y" else (b_, a_)
                row.append((d // n_data) * (4 * y_ + 2 * x_ + c_))
            row.append(int(b == c))
            for a_, c_ in ((a, c), (1 - a, c), (a, 1 - c), (1 - a, 1 - c)):
                row.append(window(a_, c_)[0])
        table.append(row)
    return np.array(table, np.int32)


def axis_of(v, k):
    return "y" if (v + k) % 2 else "x"


def sub_blocks(ff):
    step = 1280
    return [(o, min(step, ff - o)) for o in range(0, ff, step)]


def chain_kernel(n_tok, tokens, targets, wu, wd, hg, loss_ref, wub, wdb, ring, zin, zout, hld, tgt, acc, wsem, ld_sem,
                 h_sem, t_sem, z_send, z_recv, a_send, a_recv, c_send, c_recv, f_send, f_recv):
    stage, dev = lax.axis_index("stage"), lax.axis_index("data")
    y, x, c = dev // 4, (dev // 2) % 2, dev % 2
    ff = wub.shape[2]
    subs = sub_blocks(ff)
    z_peer = (1 - stage, dev)
    y_peer = (stage, dev + 4 - 8 * y)
    x_peer = (stage, dev + 2 - 4 * x)
    c_peer = (stage, dev + 1 - 2 * c)
    n_e = 4 * N_CHUNK
    half = 2 * N_CHUNK
    n_sem = a_recv.shape[0]

    def weight_copies(v, l, i):
        off, w = subs[i]
        return (
            pltpu.make_async_copy(wu.at[v, l, :, pl.ds(off, w)], wub.at[l, :, pl.ds(off, w)], wsem.at[l, 0, i]),
            pltpu.make_async_copy(wd.at[v, l, pl.ds(off, w), :], wdb.at[l, pl.ds(off, w), :], wsem.at[l, 1, i]),
        )

    def load_weights(v, l):
        for i in range(len(subs)):
            for cp in weight_copies(v, l, i):
                cp.start()

    def wait_weights(first, l, i):
        @pl.when(first)
        def _():
            for cp in weight_copies(0, l, i):
                cp.wait()

    def z_copy(m):
        return pltpu.make_async_remote_copy(zout, zin.at[m], z_send, z_recv.at[m], z_peer, MESH)

    def sent(e):
        fwd = (e < half) & ((stage == 0) | (e < N_CHUNK))
        return fwd | ((e >= half) & ((stage == 1) | (e < half + N_CHUNK)))

    def a_copy(e, l):
        b = e - half * (e // half)
        v = (b // N_CHUNK) * (1 - e // half) + (1 - b // N_CHUNK) * (e // half)
        is_y = (v + l) % 2
        peer = (stage, dev + is_y * (4 - 8 * y) + (1 - is_y) * (2 - 4 * x))
        s = 3 * e + jnp.where(e < half, l, 2 - l)
        return pltpu.make_async_remote_copy(hg.at[0, e, l], hg.at[1, e, l], a_send, a_recv.at[s % n_sem], peer, MESH)

    def c_copy(e, l):
        return pltpu.make_async_remote_copy(hg.at[0, e, l], hg.at[2, e, l], c_send, c_recv, c_peer, MESH)

    def f_copy(e, l):
        return pltpu.make_async_remote_copy(hg.at[1, e, l], hg.at[3, e, l], f_send, f_recv, c_peer, MESH)

    def layer_of(s):
        e = s // 3
        r = s - 3 * e
        back = e // half
        return e, r + back * (2 - 2 * r)

    def forward_core(s):
        e, l = layer_of(s)
        a_copy(e, l).wait_recv()
        f_copy(e, l).start()

    def publish(s):
        e, l = layer_of(s)
        pltpu.make_async_copy(ring.at[s % 3], hg.at[0, e, l], ld_sem).wait()
        a_copy(e, l).start()
        c_copy(e, l).start()

        @pl.when(s >= DELAY)
        def _():
            forward_core(s - DELAY)

    def start_tile(s, e, l, first):
        m = e % N_CHUNK

        @pl.when(first)
        def _():
            @pl.when(jnp.logical_not((stage == 1) & (e >= half) & (e < half + N_CHUNK)))
            def _():
                z_copy(m).wait_recv()

            ring[s % 3] = zin[m]

        pltpu.make_async_copy(ring.at[s % 3], hg.at[0, e, l], ld_sem).start()

    def end_chunk_send(e):
        @pl.when(sent(e))
        def _():
            z_copy(e % N_CHUNK).start()

    def wait_last_send(e, l_is_last):
        @pl.when(l_is_last & (e >= 1))
        def _():
            @pl.when(sent(e - 1))
            def _():
                z_copy(0).wait_send()

    @pl.when(stage == 0)
    def _():
        for m in range(N_CHUNK):
            pltpu.make_async_copy(tokens.at[m], zin.at[m], z_recv.at[m]).start()

    for l in range(3):
        load_weights(0, l)
    loss_ref[...] = jnp.zeros_like(loss_ref)
    barrier = pltpu.get_barrier_semaphore()
    for peer in (z_peer, y_peer, x_peer, c_peer):
        pl.semaphore_signal(barrier, inc=1, device_id=peer, device_id_type=MESH)
    pl.semaphore_wait(barrier, 4)

    def fwd_step(s, _):
        e, l = layer_of(s)
        v, m = e // N_CHUNK, e % N_CHUNK
        first = m == 0
        slot = s % 3
        top = (stage == 1) & (v == 1)
        start_tile(s, e, l, l == 0)

        @pl.when(top & (l == 0))
        def _():
            pltpu.make_async_copy(targets.at[m], tgt, t_sem).start()

        for i, (off, w) in enumerate(subs):
            wait_weights(first, l, i)
            if i == 1:
                publish(s)
                wait_last_send(e, l == 2)
            h = ring[slot]
            z = jnp.dot(h, wub[l, :, off : off + w], preferred_element_type=F32)
            a = gelu(z).astype(BF16)
            part = jnp.dot(a, wdb[l, off : off + w, :], preferred_element_type=F32)
            acc[...] = (h.astype(F32) if i == 0 else acc[...]) + part

        @pl.when(l < 2)
        def _():
            ring[(s + 1) % 3] = acc[...].astype(BF16)

        @pl.when(l == 2)
        def _():
            @pl.when(top)
            def _():
                pltpu.make_async_copy(targets.at[m], tgt, t_sem).wait()
                err = acc[...].astype(BF16).astype(F32) - tgt[...].astype(F32)
                loss_ref[...] += jnp.sum(err * err, axis=0, keepdims=True)
                zin[m] = (err * (1.0 / n_tok)).astype(BF16)

            @pl.when(jnp.logical_not(top))
            def _():
                zout[...] = acc[...].astype(BF16)

            end_chunk_send(e)

        @pl.when(e == N_CHUNK - 1)
        def _():
            load_weights(1, l)

        return 0

    lax.fori_loop(0, 3 * half, fwd_step, 0)

    def h_copy(s):
        e, l = layer_of(s)
        b = e - half
        src = N_CHUNK * (1 - b // N_CHUNK) + b % N_CHUNK
        return pltpu.make_async_copy(hg.at[0, src, l], hld.at[s % 2], h_sem.at[s % 2])

    h_copy(3 * half).start()

    def bwd_step(s, _):
        e, l = layer_of(s)
        m = e % N_CHUNK
        first = e == half + N_CHUNK
        reload = (e - half >= N_CHUNK) & (m == 0)
        slot = s % 3

        @pl.when(s + 1 < 3 * n_e)
        def _():
            h_copy(s + 1).start()

        start_tile(s, e, l, l == 2)
        h_copy(s).wait()
        for i, (off, w) in enumerate(subs):
            wait_weights(reload, l, i)
            if i == 1:
                publish(s)
                wait_last_send(e, l == 0)
            g = ring[slot]
            z = jnp.dot(hld[s % 2], wub[l, :, off : off + w], preferred_element_type=F32)
            da = lax.dot_general(g, wdb[l, off : off + w, :], NT, preferred_element_type=F32).astype(BF16).astype(F32)
            _, slope = gelu_and_slope(z)
            dz = (slope * da).astype(BF16)
            part = lax.dot_general(dz, wub[l, :, off : off + w], NT, preferred_element_type=F32)
            acc[...] = (g.astype(F32) if i == 0 else acc[...]) + part

        @pl.when(l > 0)
        def _():
            ring[(s + 1) % 3] = acc[...].astype(BF16)

        @pl.when(l == 0)
        def _():
            zout[...] = acc[...].astype(BF16)
            end_chunk_send(e)

        @pl.when(e == half + N_CHUNK - 1)
        def _():
            load_weights(0, l)

        return 0

    lax.fori_loop(3 * half, 3 * n_e, bwd_step, 0)

    def drain(s, _):
        forward_core(s)
        return 0

    lax.fori_loop(3 * n_e - DELAY, 3 * n_e, drain, 0)

    @pl.when(sent(n_e - 1))
    def _():
        z_copy(0).wait_send()

    def whole(member, send, recv):
        return pltpu.make_async_remote_copy(hg.at[member], hg.at[member], send, recv, c_peer, MESH)

    whole(0, a_send, c_recv).wait_send()
    whole(2, c_send, c_recv).wait()
    whole(3, f_send, f_recv).wait()


def chain_call(tokens, targets, wu, wd, n_tok):
    n_chunk, rows, d = tokens.shape
    ff = wu.shape[-1]
    tile = (rows, d)
    n_sub = len(sub_blocks(ff))
    dma = pltpu.SemaphoreType.DMA
    return pl.pallas_call(
        lambda *r: chain_kernel(n_tok, *r),
        in_specs=[ANY] * 4,
        out_specs=[ANY, pl.BlockSpec(memory_space=pltpu.VMEM)],
        out_shape=[
            jax.ShapeDtypeStruct((4, 4 * n_chunk, 3, *tile), BF16),
            jax.ShapeDtypeStruct((1, d), F32),
        ],
        scratch_shapes=[
            pltpu.VMEM((3, d, ff), BF16),
            pltpu.VMEM((3, ff, d), BF16),
            pltpu.VMEM((3, *tile), BF16),
            pltpu.VMEM((n_chunk, *tile), BF16),
            pltpu.VMEM(tile, BF16),
            pltpu.VMEM((2, *tile), BF16),
            pltpu.VMEM(tile, BF16),
            pltpu.VMEM(tile, F32),
            dma((3, 2, n_sub)),
            dma(()),
            dma((2,)),
            dma(()),
            dma(()),
            dma((n_chunk,)),
            dma(()),
            dma((N_RECV,)),
            dma(()),
            dma(()),
            dma(()),
            dma(()),
        ],
        compiler_params=pltpu.CompilerParams(collective_id=0, has_side_effects=True, vmem_limit_bytes=67043328),
        cost_estimate=flops(5 * 2 * 6 * n_chunk * rows * d * ff),
        name="chain",
    )(tokens, targets, wu, wd)


def wgrad_kernel(v, k, n_step, at, scal, wu, wd, tok, hg, *rest):
    down_ref, up_refs = rest[0], rest[1:3]
    wub, wdb, hb, gb, gd, gu, wsem, hsem, gsem, osem = rest[4:]
    t = pl.program_id(0)
    start = pl.multiple_of(scal[at], 128)
    width = wub.shape[1]

    copies = [
        pltpu.make_async_copy(wu.at[v, k, :, pl.ds(start, width)], wub, wsem.at[0]),
        pltpu.make_async_copy(wd.at[v, k, pl.ds(start, width), :], wdb, wsem.at[1]),
    ]

    def fetches(step, slot):
        m, j = step // 2, 2 * (step % 2)
        h_at = N_CHUNK * v + j
        g_at = 2 * N_CHUNK + N_CHUNK * (1 - v) + j
        return (
            pltpu.make_async_copy(hg.at[m, pl.ds(h_at, 2), k], hb.at[slot], hsem.at[slot]),
            pltpu.make_async_copy(hg.at[m, pl.ds(g_at, 2), k], gb.at[slot], gsem.at[slot]),
        )

    def fetch(step, slot):
        for cp in fetches(step, slot):
            cp.start()

    @pl.when(t == 0)
    def _():
        fetch(0, 0)
        for cp in copies:
            cp.start()
        gd[...] = jnp.zeros_like(gd)
        gu[...] = jnp.zeros_like(gu)

    @pl.when(t + 1 < n_step)
    def _():
        fetch(t + 1, (t + 1) % 2)

    slot = t % 2
    for cp in fetches(t, slot):
        cp.wait()

    @pl.when(t == 0)
    def _():
        for cp in copies:
            cp.wait()

    h = hb[slot].reshape(-1, hb.shape[-1])
    g = gb[slot].reshape(-1, gb.shape[-1])
    z = jnp.dot(h, wub[...], preferred_element_type=F32)
    da = lax.dot_general(g, wdb[...], NT, preferred_element_type=F32).astype(BF16).astype(F32)
    a, slope = gelu_and_slope(z)
    a = a.astype(BF16)
    dz = (slope * da).astype(BF16)
    gd[...] += lax.dot_general(a, g, TN, preferred_element_type=F32)
    gu[...] += lax.dot_general(h, dz, TN, preferred_element_type=F32)

    @pl.when(t == n_step - 1)
    def _():
        outs = []
        rows_d = down_ref.shape[1]
        for i in range(2):
            src = pl.multiple_of(scal[at + 1 + i], 8)
            outs.append(pltpu.make_async_copy(gd.at[pl.ds(src, rows_d), :], down_ref.at[i], osem.at[i]))
        rows_u = up_refs[0].shape[2]
        for i in range(8):
            src = pl.multiple_of(scal[at + 3 + i], 8)
            outs.append(
                pltpu.make_async_copy(
                    gu.at[pl.ds(src, rows_u), :], up_refs[i // 4].at[(i // 2) % 2, i % 2], osem.at[2 + i]
                )
            )
        for cp in outs:
            cp.start()
        for cp in outs:
            cp.wait()


def wgrad_call(v, k, scal, at, wu, wd, tok, hg, width, n_data):
    d, ff = wu.shape[2:]
    n_tick, rows = 2, hg.shape[3]
    n_step = 8
    return pl.pallas_call(
        lambda *r: wgrad_kernel(v, k, n_step, at, *r),
        grid_spec=pltpu.PrefetchScalarGridSpec(
            num_scalar_prefetch=1,
            grid=(n_step,),
            in_specs=[ANY] * 4,
            out_specs=[ANY] * 4,
            scratch_shapes=[
                pltpu.VMEM((d, width), BF16),
                pltpu.VMEM((width, d), BF16),
                pltpu.VMEM((2, n_tick, rows, d), BF16),
                pltpu.VMEM((2, n_tick, rows, d), BF16),
                pltpu.VMEM((width, d), F32),
                pltpu.VMEM((d, width), F32),
                pltpu.SemaphoreType.DMA((2,)),
                pltpu.SemaphoreType.DMA((2,)),
                pltpu.SemaphoreType.DMA((2,)),
                pltpu.SemaphoreType.DMA((10,)),
            ],
        ),
        out_shape=[
            jax.ShapeDtypeStruct((2, ff // n_data, d), F32),
            jax.ShapeDtypeStruct((2, 2, d // n_data, width), F32),
            jax.ShapeDtypeStruct((2, 2, d // n_data, width), F32),
            jax.ShapeDtypeStruct(tok.shape, tok.dtype),
        ],
        input_output_aliases={3: 3},
        compiler_params=params(1, 60),
        cost_estimate=flops(4 * 2 * 4 * n_tick * rows * 2 * d * width),
        name=f"wgrad_{v}_{k}",
    )(scal, wu, wd, tok, hg)


def final_kernel(at, scal, own, recv, core, p0, p1, p2, p3, *rest):
    down_ref, up_ref = rest[-2:]
    r = pl.program_id(0)
    down_ref[0, 0] = jnp.where(scal[at] == 1, own[0] + recv[0], core[...])

    @pl.when(r == 0)
    def _():
        width = p0.shape[-1]
        for i, piece in enumerate((p0, p1, p2, p3)):
            up_ref[0, 0, :, pl.ds(pl.multiple_of(scal[at + 1 + i], 128), width)] = piece[...]


def final_call(v, k, scal, at, down, recv, core, pieces, outs, shapes):
    rows, d = core.shape
    n_r = 4
    step = rows // n_r
    blk = pl.BlockSpec((step, d), lambda r, s: (r, 0))
    full = pl.BlockSpec(pieces[0].shape, lambda r, s: (0, 0))
    args = [down, recv, core, *pieces]
    first = pl.BlockSpec((1, step, d), lambda r, s: (0, r, 0))
    in_specs = [first, first, blk] + [full] * 4
    alias = {}
    if outs is not None:
        alias = {1 + len(args) + i: i for i in range(2)}
        args += outs
        in_specs += [ANY] * 2
    (_, _, ru, ff) = shapes[1]
    return pl.pallas_call(
        lambda *r: final_kernel(at, *r),
        grid_spec=pltpu.PrefetchScalarGridSpec(
            num_scalar_prefetch=1,
            grid=(n_r,),
            in_specs=in_specs,
            out_specs=[
                pl.BlockSpec((1, 1, step, d), lambda r, s: (v, k, r, 0)),
                pl.BlockSpec((1, 1, ru, ff), lambda r, s: (v, k, 0, 0)),
            ],
        ),
        out_shape=[jax.ShapeDtypeStruct(shape, F32) for shape in shapes],
        input_output_aliases=alias,
        compiler_params=params(1, 32),
        cost_estimate=flops(4e9),
        name="final",
    )(scal, *args)


def solution(mesh):
    n_stage = mesh.shape["stage"]
    n_data = mesh.shape["data"]

    def swap(value, axis):
        if axis == "stage":
            return lax.ppermute(value, "stage", [(i, (i + 1) % n_stage) for i in range(n_stage)])
        return lax.ppermute(value, "data", [(i, i ^ BIT[axis]) for i in range(n_data)])

    def device_fn(tokens_loc, targets_loc, wu, wd):
        n_micro, seq_len, d = tokens_loc.shape
        n_tok = n_data * n_micro * seq_len
        ff = wu.shape[-1]
        rows = n_micro * seq_len // N_CHUNK
        width = (ff // 4 + 127) // 128 * 128
        dev = lax.axis_index("data")
        tokens = tokens_loc.reshape(N_CHUNK, rows, d)
        targets = targets_loc.reshape(N_CHUNK, rows, d)
        tok = jnp.zeros((8, 128), F32)
        scal = lax.dynamic_index_in_dim(jnp.asarray(schedule(n_data, d, ff, width)), dev, 0, keepdims=False)

        hg, loss = chain_call(tokens, targets, wu, wd, n_tok)
        loss = jnp.broadcast_to(jnp.sum(loss) / (2.0 * n_tok), (8, 128))

        shapes = ((2, 3, ff // n_data, d), (2, 3, d // n_data, ff))
        state = {}

        def wgrad(v, k, tok):
            axis = axis_of(v, k)
            down, up_keep, up_send, tok = wgrad_call(v, k, scal, GRAD_AT[axis], wu, wd, tok, hg, width, n_data)
            other = "x" if axis == "y" else "y"
            far = BIT[other]
            pairs_ = [(i, i ^ far) for i in range(n_data) if (i % 2 == 1) != bool(i & far)]
            state[v, k] = {
                "down": down,
                "keep": up_keep,
                "down_b": lax.ppermute(down, "data", pairs_),
                "up_b": swap(up_send, other),
            }
            return tok

        def first_sum(v, k, tok):
            st = state[v, k]
            down_b, up_b, tok = lax.optimization_barrier((st["down_b"], st["up_b"], tok))
            keep = st["keep"]
            st["down_b"] = down_b
            to_a = keep[1] + up_b[1]
            to_core = keep[0, 1] + up_b[0, 1]
            st["mine"] = keep[0, 0] + up_b[0, 0]
            down_o = st["down"][1] + down_b[1]
            to_a, to_core, down_o, tok = lax.optimization_barrier((to_a, to_core, down_o, tok))
            st["up_a"] = swap(to_a, axis_of(v, k))
            st["up_c"] = swap(to_core, "core")
            st["down_c"] = swap(down_o, "core")
            return tok

        def second_swap(v, k, tok):
            st = state[v, k]
            up_a, tok = lax.optimization_barrier((st["up_a"], tok))
            to_core, st["up_a"] = up_a[1], up_a[0]
            to_core, tok = lax.optimization_barrier((to_core, tok))
            st["up_ac"] = swap(to_core, "core")
            return tok

        def finish(v, k, grads):
            st = state[v, k]
            pieces = [st["mine"], st["up_a"], st["up_c"], st["up_ac"]]
            at = GRAD_AT[axis_of(v, k)] + 11
            return final_call(v, k, scal, at, st["down"], st["down_b"], st["down_c"], pieces, grads, shapes)

        order = [(1, 2), (1, 1), (1, 0), (0, 2), (0, 1), (0, 0)]
        for i, (v, k) in enumerate(order):
            tok = wgrad(v, k, tok)
            if i < 4:
                step = ("core", "x", "y", "stage")[i]
                loss, tok = lax.optimization_barrier((loss + swap(loss, step), tok))
            if i >= 2:
                tok = first_sum(*order[i - 2], tok)
            if i >= 3:
                tok = second_swap(*order[i - 3], tok)
        grads = None
        for v, k in order[:3]:
            grads = finish(v, k, grads)
        tok = second_swap(*order[3], tok)
        tok = first_sum(*order[4], tok)
        grads = finish(*order[3], grads)
        tok = second_swap(*order[4], tok)
        tok = first_sum(*order[5], tok)
        grads = finish(*order[4], grads)
        tok = second_swap(*order[5], tok)
        grads = finish(*order[5], grads)
        loss = loss[0, 0]
        return loss, grads[1], grads[0]

    return jax.shard_map(
        device_fn,
        mesh=mesh,
        in_specs=(P("data"), P("data"), P(None, "stage"), P(None, "stage")),
        out_specs=(P(), P(None, "stage", "data"), P(None, "stage", "data")),
        check_vma=False,
    )
```

```python
import jax
import jax.numpy as jnp
import numpy as np
from jax import lax
from jax.experimental import pallas as pl
from jax.experimental.pallas import tpu as pltpu
from jax.sharding import PartitionSpec as P

F32, BF16 = jnp.float32, jnp.bfloat16
MESH = pl.DeviceIdType.MESH
N_CHUNK = 4
N_LAYER = 3
HALF = 2 * N_CHUNK
N_TILE = 2 * HALF * N_LAYER
N_GRAD = 2 * N_LAYER
N_STEP = 8
LONG, SHORT = 8 * N_LAYER, 4 * N_LAYER
NT = (((1,), (1,)), ((), ()))
TN = (((0,), (0,)), ((), ()))
C0 = 0.7978845608028654
C1 = 0.044715
ANY = pl.BlockSpec(memory_space=pl.ANY)


def gelu(z):
    return z * (0.5 * (1.0 + jnp.tanh(C0 * (z + C1 * (z * z * z)))))


def gelu_and_slope(z):
    z2 = z * z
    t = jnp.tanh(C0 * (z + C1 * (z2 * z)))
    cdf = 0.5 * (1.0 + t)
    slope = cdf + (0.5 * z) * ((1.0 - t * t) * (C0 + (3.0 * C0 * C1) * z2))
    return cdf * z, slope


def sub_blocks(ff):
    step = 1280
    return [(o, min(step, ff - o)) for o in range(0, ff, step)]


def window_width(ff):
    return (ff // 4 + 127) // 128 * 128


class Place:
    def __init__(self, stage, dev):
        self.stage, self.dev = stage, dev
        self.y, self.x, self.c = dev // 4, (dev // 2) % 2, dev % 2

    def flip(self, fy, fx, fc):
        return self.dev + fy * (4 - 8 * self.y) + fx * (2 - 4 * self.x) + fc * (1 - 2 * self.c)

    def gather(self, v, k):
        is_y = (v + k) % 2
        kind_c = (1 - v) * (1 - k // 2)
        one = self.flip(is_y, 1 - is_y, 0)
        two = self.flip(kind_c * (1 - is_y), kind_c * is_y, 1 - kind_c)
        return one, two

    def layer(self, j):
        return 1 - j // N_LAYER, N_LAYER - 1 - j % N_LAYER

    def share(self, j):
        y, x, c = self.y, self.x, self.c
        v, k = self.layer(j)
        kc = j // 4
        dy = (1 - kc) * ((v + k) % 2)
        dx = (1 - kc) * (1 - (v + k) % 2)
        sh = Share()
        sh.kc = kc
        sh.p = (dy + kc) * y + dx * c
        sh.q = dy * c + (dx + kc) * x
        sh.wu, sh.w1, sh.w2 = 2 * dy + 4 * dx + kc, 4 * dy + 2 * dx + 4 * kc, dy + dx + 2 * kc
        sh.u = dy * x + dx * y + kc * c
        sh.r1 = dy * y + dx * x + kc * y
        sh.r2 = (dy + dx) * c + kc * x
        sh.partner = self.dev + sh.wu * (1 - 2 * sh.u)
        away = (1 - kc) * (sh.u * (1 - c) + c * (1 - sh.u))
        sh.away = away
        sh.dest_same = self.dev + away * sh.wu * (1 - 2 * sh.u)
        sh.dest_other = sh.dest_same + (1 - 2 * c)
        sh.slot_other = kc + away
        return sh


class Share:
    def piece(self, i):
        r1 = self.r1 + (i // 2) * (1 - 2 * self.r1)
        r2 = self.r2 + (i % 2) * (1 - 2 * self.r2)
        return self.w1 * r1 + self.w2 * r2 + self.wu * self.u

    def start(self, ff):
        return (ff // 2) * self.p + (ff // 2 - window_width(ff)) * self.q

    def base(self, ff):
        return (ff // 4 - (ff // 2 - window_width(ff))) * self.q


def layer_of(s):
    e = s // N_LAYER
    r = s - N_LAYER * e
    back = e // HALF
    return e, r + back * (N_LAYER - 1 - 2 * r)


def block_of(e):
    back = e // HALF
    first = (e - HALF * back) // N_CHUNK
    return first + back * (1 - 2 * first)


def step_kernel(n_tok, tokens, targets, wu, wd, hg, dd, upp, loss_ref, sup, kup, ub, sd, zin, lbuf, sems):
    place = Place(lax.axis_index("stage"), lax.axis_index("data"))
    stage, dev, c = place.stage, place.dev, place.c
    d, ff = wu.shape[2:]
    rows = zin.shape[1]
    tile = (rows, d)

    def remote(src, dst, send, recv, to):
        return pltpu.make_async_remote_copy(src, dst, send, recv, to, MESH)

    def at(index):
        return (stage, index)

    z_peer = (1 - stage, dev)
    local_peers = [place.flip(*f) for f in ((0, 0, 1), (0, 1, 0), (1, 0, 0), (0, 1, 1), (1, 0, 1), (1, 1, 0))]

    @pl.when(stage == 0)
    def _():
        for m in range(N_CHUNK):
            pltpu.make_async_copy(tokens.at[m], zin.at[m], sems.z_recv.at[m]).start()

    barrier = pltpu.get_barrier_semaphore()
    for peer in [z_peer] + [at(i) for i in local_peers]:
        pl.semaphore_signal(barrier, inc=1, device_id=peer, device_id_type=MESH)
    pl.semaphore_wait(barrier, 1 + len(local_peers))

    def a_copy(s):
        e, l = layer_of(s)
        one, _ = place.gather(block_of(e), l)
        return remote(hg.at[0, e, l], hg.at[1, e, l], sems.a_send, sems.a_recv.at[s], at(one))

    def c_copy(s):
        e, l = layer_of(s)
        v = block_of(e)
        _, two = place.gather(v, l)
        return remote(hg.at[0, e, l], hg.at[2, e, l], sems.c_send, sems.c_recv.at[v], at(two))

    def forward(s):
        e, l = layer_of(s)
        v = block_of(e)
        _, two = place.gather(v, l)
        a_copy(s).wait_recv()
        remote(hg.at[1, e, l], hg.at[3, e, l], sems.f_send, sems.f_recv.at[v], at(two)).start()

    def chain(wub, wdb, ring, zout, hld, tgt, acc, loss_row):
        subs = sub_blocks(ff)

        def weight_copies(v, l):
            return (
                pltpu.make_async_copy(wu.at[v, l], wub.at[l], sems.w.at[l, 0]),
                pltpu.make_async_copy(wd.at[v, l], wdb.at[l], sems.w.at[l, 1]),
            )

        def load_weights(v, l):
            for cp in weight_copies(v, l):
                cp.start()

        def wait_weights(l):
            for cp in weight_copies(0, l):
                cp.wait()

        def z_copy(m):
            return remote(zout, zin.at[m], sems.z_send, sems.z_recv.at[m], z_peer)

        def sent(e):
            fwd = (e < HALF) & ((stage == 0) | (e < N_CHUNK))
            return fwd | ((e >= HALF) & ((stage == 1) | (e < HALF + N_CHUNK)))

        def start_tile(s, e, l, first):
            @pl.when(first)
            def _():
                @pl.when(jnp.logical_not((stage == 1) & (e >= HALF) & (e < HALF + N_CHUNK)))
                def _():
                    z_copy(e % N_CHUNK).wait_recv()

                ring[s % 3] = zin[e % N_CHUNK]

            pltpu.make_async_copy(ring.at[s % 3], hg.at[0, e, l], sems.ld).start()

        def end_tile(s, e, l, last):
            pltpu.make_async_copy(ring.at[s % 3], hg.at[0, e, l], sems.ld).wait()
            a_copy(s).start()
            c_copy(s).start()

            @pl.when((s >= LONG) & (s < 2 * LONG))
            def _():
                forward(s - LONG)

            @pl.when(s >= LONG + SHORT)
            def _():
                forward(s - SHORT)

            @pl.when(last & (e >= 1))
            def _():
                @pl.when(sent(e - 1))
                def _():
                    z_copy(0).wait_send()

        for l in range(N_LAYER):
            load_weights(0, l)
        loss_row[...] = jnp.zeros_like(loss_row)

        def fwd_step(s, _):
            e, l = layer_of(s)
            v, m = e // N_CHUNK, e % N_CHUNK
            top = (stage == 1) & (v == 1)
            start_tile(s, e, l, l == 0)

            @pl.when(top & (l == 0))
            def _():
                pltpu.make_async_copy(targets.at[m], tgt, sems.t).start()

            @pl.when(m == 0)
            def _():
                wait_weights(l)

            for i, (off, w) in enumerate(subs):
                h = ring[s % 3]
                z = jnp.dot(h, wub[l, :, off : off + w], preferred_element_type=F32)
                a = gelu(z).astype(BF16)
                part = jnp.dot(a, wdb[l, off : off + w, :], preferred_element_type=F32)
                acc[...] = (h.astype(F32) if i == 0 else acc[...]) + part

            end_tile(s, e, l, l == N_LAYER - 1)

            @pl.when(e == N_CHUNK - 1)
            def _():
                load_weights(1, l)

            @pl.when(l < N_LAYER - 1)
            def _():
                ring[(s + 1) % 3] = acc[...].astype(BF16)

            @pl.when(l == N_LAYER - 1)
            def _():
                @pl.when(top)
                def _():
                    pltpu.make_async_copy(targets.at[m], tgt, sems.t).wait()
                    err = acc[...].astype(BF16).astype(F32) - tgt[...].astype(F32)
                    loss_row[...] += jnp.sum(err * err, axis=0, keepdims=True)
                    zin[m] = (err * (1.0 / n_tok)).astype(BF16)

                @pl.when(jnp.logical_not(top))
                def _():
                    zout[...] = acc[...].astype(BF16)

                @pl.when(sent(e))
                def _():
                    z_copy(m).start()

            return 0

        lax.fori_loop(0, N_TILE // 2, fwd_step, 0)

        def h_copy(s):
            e, l = layer_of(s)
            src = N_CHUNK * block_of(e) + e % N_CHUNK
            return pltpu.make_async_copy(hg.at[0, src, l], hld.at[s % 2], sems.h.at[s % 2])

        h_copy(N_TILE // 2).start()

        def bwd_step(s, _):
            e, l = layer_of(s)
            m = e % N_CHUNK

            @pl.when(s + 1 < N_TILE)
            def _():
                h_copy(s + 1).start()

            start_tile(s, e, l, l == N_LAYER - 1)
            h_copy(s).wait()

            @pl.when(e == HALF + N_CHUNK)
            def _():
                wait_weights(l)

            for i, (off, w) in enumerate(subs):
                g = ring[s % 3]
                z = jnp.dot(hld[s % 2], wub[l, :, off : off + w], preferred_element_type=F32)
                da = lax.dot_general(g, wdb[l, off : off + w, :], NT, preferred_element_type=F32)
                _, slope = gelu_and_slope(z)
                dz = (slope * da.astype(BF16).astype(F32)).astype(BF16)
                part = lax.dot_general(dz, wub[l, :, off : off + w], NT, preferred_element_type=F32)
                acc[...] = (g.astype(F32) if i == 0 else acc[...]) + part

            end_tile(s, e, l, l == 0)

            @pl.when(e == HALF + N_CHUNK - 1)
            def _():
                load_weights(0, l)

            @pl.when(l > 0)
            def _():
                ring[(s + 1) % 3] = acc[...].astype(BF16)

            @pl.when(l == 0)
            def _():
                zout[...] = acc[...].astype(BF16)

                @pl.when(sent(e))
                def _():
                    z_copy(m).start()

            return 0

        lax.fori_loop(N_TILE // 2, N_TILE, bwd_step, 0)

        @pl.when(sent(2 * HALF - 1))
        def _():
            z_copy(0).wait_send()

        loss_ref[...] = jnp.broadcast_to(jnp.sum(loss_row[...], axis=1, keepdims=True), loss_ref.shape)

    width = window_width(ff)
    seg_d, seg_u = dd.shape[2], upp.shape[2]

    def grads(wub, wdb, hb, gb, gd, gu, cb, ubb):
        def weight_copies(j):
            v, k = place.layer(j)
            start = pl.multiple_of(place.share(j).start(ff), 128)
            b = j % 2
            return (
                pltpu.make_async_copy(wu.at[v, k, :, pl.ds(start, width)], wub.at[b], sems.ww.at[b, 0]),
                pltpu.make_async_copy(wd.at[v, k, pl.ds(start, width), :], wdb.at[b], sems.ww.at[b, 1]),
            )

        def fetches(n):
            v, k = place.layer(n // N_STEP)
            t = n % N_STEP
            m, part = t // 2, 2 * (t % 2)
            h_at = N_CHUNK * v + part
            g_at = HALF + N_CHUNK * (1 - v) + part
            b = n % 2
            return (
                pltpu.make_async_copy(hg.at[m, pl.ds(h_at, 2), k], hb.at[b], sems.hb.at[b]),
                pltpu.make_async_copy(hg.at[m, pl.ds(g_at, 2), k], gb.at[b], sems.gb.at[b]),
            )

        def arrived(v):
            ref = hg.at[2, pl.ds(0, HALF)]
            remote(ref, ref, sems.c_send, sems.c_recv.at[v], z_peer).wait_recv()
            remote(ref, ref, sems.f_send, sems.f_recv.at[v], z_peer).wait_recv()

        def stage_copies(j):
            sh = place.share(j)
            b = j % 2
            up = []
            for i in range(4):
                keep = sh.piece(i)
                send = keep + sh.wu * (1 - 2 * sh.u)
                for to, row, sem in ((sup, send, 0), (kup, keep, 1)):
                    src = gu.at[b, pl.ds(pl.multiple_of(row * seg_u, 8), seg_u), :]
                    up.append(pltpu.make_async_copy(src, to.at[j, i], sems.st.at[sem]))
            base = sh.base(ff)
            part = [gd.at[b, pl.ds(pl.multiple_of(base + seg_d * i, 8), seg_d), :] for i in (c, 1 - c)]
            same = [pltpu.make_async_copy(part[0], to.at[j, 0], sems.st.at[2]) for to in (dd, sd)]
            other = pltpu.make_async_copy(part[1], sd.at[j, 1], sems.st.at[3])
            return sh, up, same, other

        def stage_out(j):
            sh, up, same, other = stage_copies(j)
            for cp in up:
                cp.start()
            other.start()
            pl.when(sh.away == 0)(same[0].start)
            pl.when(sh.away == 1)(same[1].start)

        def down_same(j, sh):
            return remote(sd.at[j, 0], dd.at[j, 1], sems.ds_send, sems.d_recv.at[j, 1], at(sh.dest_same))

        def up_exchange(j, sh):
            return remote(sup.at[j], ub.at[j], sems.u_send, sems.u_recv.at[j], at(sh.partner))

        def send_out(j):
            sh = place.share(j)
            pltpu.make_async_copy(sup.at[j], sup.at[j], sems.st.at[0]).wait()
            up_exchange(j, sh).start()
            pltpu.make_async_copy(sd.at[j, 1], sd.at[j, 1], sems.st.at[3]).wait()
            slot = sh.slot_other
            remote(
                sd.at[j, 1], dd.at[j, slot], sems.d_send, sems.d_recv.at[j, slot], at(sh.dest_other)
            ).start()

            pltpu.make_async_copy(sd.at[j, 0], sd.at[j, 0], sems.st.at[2]).wait()
            pl.when(sh.away == 1)(down_same(j, sh).start)
            pltpu.make_async_copy(kup.at[j], kup.at[j], sems.st.at[1]).wait()

        def piece_sends(j, b):
            sh = place.share(j)
            out = [pltpu.make_async_copy(cb.at[b, 0], upp.at[j, 0], sems.p_here.at[b])]
            for i in range(1, 4):
                out.append(remote(cb.at[b, i], upp.at[j, i], sems.p_send.at[b], sems.p_recv.at[j], at(sh.piece(i))))
            return out

        def wait_pieces(j, b):
            piece_sends(j, b)[0].wait()
            ref = cb.at[b, pl.ds(1, 3)]
            remote(ref, ref, sems.p_send.at[b], sems.p_recv.at[j], z_peer).wait_send()

        def sum_loads(j, b):
            return (
                pltpu.make_async_copy(kup.at[j], cb.at[b], sems.cl.at[0]),
                pltpu.make_async_copy(ub.at[j], ubb, sems.cl.at[1]),
            )

        def sum_load(j, b):
            up_exchange(j, place.share(j)).wait_recv()
            for cp in sum_loads(j, b):
                cp.start()

        def sum_add(j, b):
            for cp in sum_loads(j, b):
                cp.wait()
            cb[b] += ubb[...]
            for cp in piece_sends(j, b):
                cp.start()

        for cp in weight_copies(0) + fetches(0):
            cp.start()

        loss_peers = [at(place.flip(0, 0, 1)), at(place.flip(0, 1, 0)), at(place.flip(1, 0, 0)), z_peer]

        def loss_copy(r):
            return remote(lbuf.at[0, r], lbuf.at[1, r], sems.l_send, sems.l_recv.at[r], loss_peers[r])

        def step(n, _):
            j, t = n // N_STEP, n % N_STEP
            b, jb = n % 2, j % 2

            @pl.when((n >= SHORT) & (n < 2 * SHORT))
            def _():
                forward(n + LONG)

            for v, when in ((1, 3), (0, N_LAYER * N_STEP + 3)):
                pl.when(n == when)(lambda v=v: arrived(v))

            @pl.when(n + 1 < N_GRAD * N_STEP)
            def _():
                for cp in fetches(n + 1):
                    cp.start()

            for r in range(4):

                @pl.when(n == 2 * r)
                def _():
                    if r:
                        loss_copy(r - 1).wait()
                        loss_ref[...] += lbuf[1, r - 1]
                    lbuf[0, r] = loss_ref[...]

                @pl.when(n == 2 * r + 1)
                def _():
                    loss_copy(r).start()

            @pl.when(n == 8)
            def _():
                loss_copy(3).wait()
                loss_ref[...] += lbuf[1, 3]

            @pl.when(t == 0)
            def _():
                for cp in weight_copies(j):
                    cp.wait()

            @pl.when((t == 1) & (j + 1 < N_GRAD))
            def _():
                for cp in weight_copies(j + 1):
                    cp.start()

            @pl.when((t == 0) & (j >= 1))
            def _():
                stage_out(j - 1)

            @pl.when((t == 1) & (j >= 1))
            def _():
                send_out(j - 1)

            @pl.when((t == 4) & (j >= 3))
            def _():
                @pl.when(j == 5)
                def _():
                    wait_pieces(0, 0)

                sum_load(j - 3, (j - 3) % 2)

            @pl.when((t == 5) & (j >= 3))
            def _():
                sum_add(j - 3, (j - 3) % 2)

            @pl.when(n == N_GRAD * N_STEP - 2)
            def _():
                wait_pieces(1, 1)
                sum_load(4, 1)

            @pl.when(n == N_GRAD * N_STEP - 1)
            def _():
                sum_add(4, 1)

            for cp in fetches(n):
                cp.wait()
            h = hb[b].reshape(2 * rows, d)
            g = gb[b].reshape(2 * rows, d)
            z = jnp.dot(h, wub[jb], preferred_element_type=F32)
            da = lax.dot_general(g, wdb[jb], NT, preferred_element_type=F32).astype(BF16).astype(F32)
            a, slope = gelu_and_slope(z)
            a = a.astype(BF16)
            dz = (slope * da).astype(BF16)
            gd[jb] = jnp.where(t == 0, 0.0, gd[jb]) + lax.dot_general(a, g, TN, preferred_element_type=F32)
            gu[jb] = jnp.where(t == 0, 0.0, gu[jb]) + lax.dot_general(h, dz, TN, preferred_element_type=F32)
            return 0

        lax.fori_loop(0, N_GRAD * N_STEP, step, 0)
        stage_out(5)
        send_out(5)
        wait_pieces(4, 1)
        sum_load(5, 1)
        sum_add(5, 1)
        wait_pieces(2, 0)
        sum_load(3, 0)
        sum_add(3, 0)
        wait_pieces(5, 1)
        wait_pieces(3, 0)

    pl.run_scoped(
        chain,
        pltpu.VMEM((N_LAYER, d, ff), BF16),
        pltpu.VMEM((N_LAYER, ff, d), BF16),
        pltpu.VMEM((3, *tile), BF16),
        pltpu.VMEM(tile, BF16),
        pltpu.VMEM((2, *tile), BF16),
        pltpu.VMEM(tile, BF16),
        pltpu.VMEM(tile, F32),
        pltpu.VMEM((1, d), F32),
    )
    pl.run_scoped(
        grads,
        pltpu.VMEM((2, d, width), BF16),
        pltpu.VMEM((2, width, d), BF16),
        pltpu.VMEM((2, 2, *tile), BF16),
        pltpu.VMEM((2, 2, *tile), BF16),
        pltpu.VMEM((2, width, d), F32),
        pltpu.VMEM((2, d, width), F32),
        pltpu.VMEM((2, 4, seg_u, width), F32),
        pltpu.VMEM((4, seg_u, width), F32),
    )

    for j in range(N_GRAD):
        sh = place.share(j)
        ref = upp.at[j, pl.ds(1, 3)]
        remote(ref, ref, sems.p_send.at[0], sems.p_recv.at[j], z_peer).wait_recv()
        ref = dd.at[j, 0]
        remote(ref, ref, sems.d_send, sems.d_recv.at[j, 1], z_peer).wait_recv()

        @pl.when(sh.away == 1)
        def _():
            remote(ref, ref, sems.ds_send, sems.d_recv.at[j, 0], z_peer).wait()

    remote(sup, sup, sems.u_send, sems.u_recv.at[0], z_peer).wait_send()
    ref = sd.at[:, 1]
    remote(ref, ref, sems.d_send, sems.d_recv.at[0, 0], z_peer).wait_send()
    for sem in (sems.a_send, sems.c_send, sems.f_send):
        remote(hg.at[0], hg.at[0], sem, sems.a_recv.at[0], z_peer).wait_send()


SEMS = {
    "w": (N_LAYER, 2),
    "ld": (),
    "h": (2,),
    "t": (),
    "z_send": (),
    "z_recv": (N_CHUNK,),
    "a_send": (),
    "a_recv": (N_TILE,),
    "c_send": (),
    "c_recv": (2,),
    "f_send": (),
    "f_recv": (2,),
    "ww": (2, 2),
    "hb": (2,),
    "gb": (2,),
    "st": (4,),
    "u_send": (),
    "u_recv": (N_GRAD,),
    "d_send": (),
    "ds_send": (),
    "d_recv": (N_GRAD, 2),
    "cl": (2,),
    "p_send": (2,),
    "p_here": (2,),
    "p_recv": (N_GRAD,),
    "l_send": (),
    "l_recv": (4,),
}


class Sems:
    def __init__(self, refs):
        for name, ref in zip(SEMS, refs, strict=True):
            setattr(self, name, ref)


def step_call(tokens, targets, wu, wd, n_tok, n_data):
    n_chunk, rows, d = tokens.shape
    ff = wu.shape[-1]
    width = window_width(ff)
    pieces = jax.ShapeDtypeStruct((N_GRAD, 4, d // n_data, width), F32)
    parts = jax.ShapeDtypeStruct((N_GRAD, 2, ff // n_data, d), F32)

    def body(*refs):
        n = 12 + 2
        step_kernel(n_tok, *refs[:n], Sems(refs[n:]))

    return pl.pallas_call(
        body,
        in_specs=[ANY] * 4,
        out_specs=[ANY] * 3 + [pl.BlockSpec(memory_space=pltpu.VMEM)] + [ANY] * 4,
        out_shape=[
            jax.ShapeDtypeStruct((4, 2 * HALF, N_LAYER, rows, d), BF16),
            parts,
            pieces,
            jax.ShapeDtypeStruct((8, 128), F32),
            pieces,
            pieces,
            pieces,
            parts,
        ],
        scratch_shapes=[
            pltpu.VMEM((n_chunk, rows, d), BF16),
            pltpu.VMEM((2, 4, 8, 128), F32),
            *[pltpu.SemaphoreType.DMA(shape) for shape in SEMS.values()],
        ],
        compiler_params=pltpu.CompilerParams(collective_id=0, has_side_effects=True, vmem_limit_bytes=67043328),
        name="step",
    )(tokens, targets, wu, wd)


def final_kernel(scal, dd, upp, down_ref, up_ref):
    down_ref[0, 0] = dd[0, 0] + dd[0, 1]
    width = upp.shape[-1]
    for i in range(4):
        start = pl.multiple_of(scal[4 * pl.program_id(0) + i], 128)
        up_ref[0, 0, :, pl.ds(start, width)] = upp[0, i]


def final_call(scal, dd, upp, n_data):
    seg_d, d = dd.shape[2:]
    seg_u, width = upp.shape[2:]
    ff = seg_d * n_data
    return pl.pallas_call(
        final_kernel,
        grid_spec=pltpu.PrefetchScalarGridSpec(
            num_scalar_prefetch=1,
            grid=(N_GRAD,),
            in_specs=[
                pl.BlockSpec((1, 2, seg_d, d), lambda j, s: (j, 0, 0, 0)),
                pl.BlockSpec((1, 4, seg_u, width), lambda j, s: (j, 0, 0, 0)),
            ],
            out_specs=[
                pl.BlockSpec((1, 1, seg_d, d), lambda j, s: (1 - j // N_LAYER, N_LAYER - 1 - j % N_LAYER, 0, 0)),
                pl.BlockSpec((1, 1, seg_u, ff), lambda j, s: (1 - j // N_LAYER, N_LAYER - 1 - j % N_LAYER, 0, 0)),
            ],
        ),
        out_shape=[
            jax.ShapeDtypeStruct((2, N_LAYER, seg_d, d), F32),
            jax.ShapeDtypeStruct((2, N_LAYER, seg_u, ff), F32),
        ],
        compiler_params=pltpu.CompilerParams(dimension_semantics=("arbitrary",), vmem_limit_bytes=40 * 2**20),
        name="final",
    )(scal, dd, upp)


def window_table(n_data, ff):
    table = []
    for dev in range(n_data):
        place = Place(0, dev)
        row = []
        for j in range(N_GRAD):
            for i in range(4):
                row.append(Place(0, place.share(j).piece(i)).share(j).start(ff))
        table.append(row)
    return np.array(table, np.int32)


def solution(mesh):
    n_data = mesh.shape["data"]

    def device_fn(tokens_loc, targets_loc, wu, wd):
        n_micro, seq_len, d = tokens_loc.shape
        n_tok = n_data * n_micro * seq_len
        ff = wu.shape[-1]
        rows = n_micro * seq_len // N_CHUNK
        tokens = tokens_loc.reshape(N_CHUNK, rows, d)
        targets = targets_loc.reshape(N_CHUNK, rows, d)
        out = step_call(tokens, targets, wu, wd, n_tok, n_data)
        dd, upp, loss = out[1:4]
        starts = jnp.asarray(window_table(n_data, ff))
        scal = lax.dynamic_index_in_dim(starts, lax.axis_index("data"), 0, keepdims=False)
        down, up = final_call(scal, dd, upp, n_data)
        return loss[0, 0] / (2.0 * n_tok), up, down

    return jax.shard_map(
        device_fn,
        mesh=mesh,
        in_specs=(P("data"), P("data"), P(None, "stage"), P(None, "stage")),
        out_specs=(P(), P(None, "stage", "data"), P(None, "stage", "data")),
        check_vma=False,
    )
```

```python
import jax
import jax.numpy as jnp
import numpy as np
from jax import lax
from jax.experimental import pallas as pl
from jax.experimental.pallas import tpu as pltpu
from jax.sharding import PartitionSpec as P

F32, BF16 = jnp.float32, jnp.bfloat16
MESH = pl.DeviceIdType.MESH
N_CHUNK = 4
N_LAYER = 3
HALF = 2 * N_CHUNK
N_TILE = 2 * HALF * N_LAYER
N_GRAD = 2 * N_LAYER
N_RING = 11
BWD_BLOCK = 256
N_STEP = 8
LONG, SHORT = 8 * N_LAYER, 4 * N_LAYER
NT = (((1,), (1,)), ((), ()))
TN = (((0,), (0,)), ((), ()))
C0 = 0.7978845608028654
C1 = 0.044715
ANY = pl.BlockSpec(memory_space=pl.ANY)


def gelu(z):
    return z * (0.5 * (1.0 + jnp.tanh(C0 * (z + C1 * (z * z * z)))))


def gelu_and_slope(z):
    z2 = z * z
    t = jnp.tanh(C0 * (z + C1 * (z2 * z)))
    cdf = 0.5 * (1.0 + t)
    slope = cdf + (0.5 * z) * ((1.0 - t * t) * (C0 + (3.0 * C0 * C1) * z2))
    return cdf * z, slope


def sub_blocks(ff):
    step = 512
    return [(o, min(step, ff - o)) for o in range(0, ff, step)]


def grad_blocks(width):
    return [(o, min(768, width - o)) for o in range(0, width, 768)]


def window_width(ff):
    return (ff // 4 + 127) // 128 * 128


class Place:
    def __init__(self, stage, dev):
        self.stage, self.dev = stage, dev
        self.y, self.x, self.c = dev // 4, (dev // 2) % 2, dev % 2

    def flip(self, fy, fx, fc):
        return self.dev + fy * (4 - 8 * self.y) + fx * (2 - 4 * self.x) + fc * (1 - 2 * self.c)

    def gather(self, v, k):
        is_y = (v + k) % 2
        kind_c = (1 - v) * (1 - k // 2)
        one = self.flip(is_y, 1 - is_y, 0)
        two = self.flip(kind_c * (1 - is_y), kind_c * is_y, 1 - kind_c)
        return one, two

    def layer(self, j):
        return 1 - j // N_LAYER, N_LAYER - 1 - j % N_LAYER

    def group(self, v, k):
        return (1 - v) * (N_LAYER - k)

    def share(self, j):
        y, x, c = self.y, self.x, self.c
        v, k = self.layer(j)
        kc = j // 4
        dy = (1 - kc) * ((v + k) % 2)
        dx = (1 - kc) * (1 - (v + k) % 2)
        sh = Share()
        sh.kc = kc
        sh.p = (dy + kc) * y + dx * c
        sh.q = dy * c + (dx + kc) * x
        sh.wu, sh.w1, sh.w2 = 2 * dy + 4 * dx + kc, 4 * dy + 2 * dx + 4 * kc, dy + dx + 2 * kc
        sh.u = dy * x + dx * y + kc * c
        sh.r1 = dy * y + dx * x + kc * y
        sh.r2 = (dy + dx) * c + kc * x
        sh.partner = self.dev + sh.wu * (1 - 2 * sh.u)
        away = (1 - kc) * (sh.u * (1 - c) + c * (1 - sh.u))
        sh.away = away
        sh.dest_same = self.dev + away * sh.wu * (1 - 2 * sh.u)
        sh.dest_other = sh.dest_same + (1 - 2 * c)
        sh.slot_other = kc + away
        return sh


class Share:
    def piece(self, i):
        r1 = self.r1 + (i // 2) * (1 - 2 * self.r1)
        r2 = self.r2 + (i % 2) * (1 - 2 * self.r2)
        return self.w1 * r1 + self.w2 * r2 + self.wu * self.u

    def start(self, ff):
        return (ff // 2) * self.p + (ff // 2 - window_width(ff)) * self.q

    def base(self, ff):
        return (ff // 4 - (ff // 2 - window_width(ff))) * self.q


def layer_of(s):
    e = s // N_LAYER
    r = s - N_LAYER * e
    back = e // HALF
    return e, r + back * (N_LAYER - 1 - 2 * r)


def block_of(e):
    back = e // HALF
    first = (e - HALF * back) // N_CHUNK
    return first + back * (1 - 2 * first)


def step_kernel(n_tok, tokens, targets, wu, wd, hg, dd, upp, loss_ref, sup, kup, ub, sd, zs, zin, lbuf, sems):
    place = Place(lax.axis_index("stage"), lax.axis_index("data"))
    stage, dev, c = place.stage, place.dev, place.c
    d, ff = wu.shape[2:]
    rows = zin.shape[1]
    tile = (rows, d)

    def remote(src, dst, send, recv, to):
        return pltpu.make_async_remote_copy(src, dst, send, recv, to, MESH)

    def at(index):
        return (stage, index)

    z_peer = (1 - stage, dev)
    local_peers = [place.flip(*f) for f in ((0, 0, 1), (0, 1, 0), (1, 0, 0), (0, 1, 1), (1, 0, 1), (1, 1, 0))]

    @pl.when(stage == 0)
    def _():
        for m in range(N_CHUNK):
            pltpu.make_async_copy(tokens.at[m], zin.at[m], sems.z_recv.at[m]).start()

    barrier = pltpu.get_barrier_semaphore()
    for peer in [z_peer] + [at(i) for i in local_peers]:
        pl.semaphore_signal(barrier, inc=1, device_id=peer, device_id_type=MESH)
    pl.semaphore_wait(barrier, 1 + len(local_peers))

    def a_copy(s):
        e, l = layer_of(s)
        one, _ = place.gather(block_of(e), l)
        return remote(hg.at[0, e, l], hg.at[1, e, l], sems.a_send, sems.a_recv.at[s], at(one))

    def c_copy(s):
        e, l = layer_of(s)
        v = block_of(e)
        _, two = place.gather(v, l)
        return remote(hg.at[0, e, l], hg.at[2, e, l], sems.c_send, sems.c_recv.at[place.group(v, l)], at(two))

    def forward(s):
        e, l = layer_of(s)
        v = block_of(e)
        _, two = place.gather(v, l)
        a_copy(s).wait_recv()
        remote(hg.at[1, e, l], hg.at[3, e, l], sems.f_send, sems.f_recv.at[place.group(v, l)], at(two)).start()

    def chain(wub, wdb, ring, zout, zb, tgt, acc, loss_row):
        subs = sub_blocks(ff)
        n_sub = len(subs)
        assert n_sub < N_RING

        def weight_copies(v, l):
            return (
                pltpu.make_async_copy(wu.at[v, l], wub.at[l], sems.w.at[l, 0]),
                pltpu.make_async_copy(wd.at[v, l], wdb.at[l], sems.w.at[l, 1]),
            )

        def load_weights(v, l):
            for cp in weight_copies(v, l):
                cp.start()

        def wait_weights(l):
            for cp in weight_copies(0, l):
                cp.wait()

        def z_copy(m):
            return remote(zout, zin.at[m], sems.z_send, sems.z_recv.at[m], z_peer)

        def sent(e):
            fwd = (e < HALF) & ((stage == 0) | (e < N_CHUNK))
            return fwd | ((e >= HALF) & ((stage == 1) | (e < HALF + N_CHUNK)))

        def start_tile(s, e, l, first):
            @pl.when(first)
            def _():
                @pl.when(jnp.logical_not((stage == 1) & (e >= HALF) & (e < HALF + N_CHUNK)))
                def _():
                    z_copy(e % N_CHUNK).wait_recv()

                ring[s % 3] = zin[e % N_CHUNK]

            pltpu.make_async_copy(ring.at[s % 3], hg.at[0, e, l], sems.ld).start()

        def end_tile(s, e, l, last):
            pltpu.make_async_copy(ring.at[s % 3], hg.at[0, e, l], sems.ld).wait()
            a_copy(s).start()
            c_copy(s).start()

            @pl.when((s >= LONG) & (s < LONG + SHORT))
            def _():
                forward(s - LONG)

            @pl.when(s >= LONG)
            def _():
                forward(s - SHORT)

            @pl.when(last & (e >= 1))
            def _():
                @pl.when(sent(e - 1))
                def _():
                    z_copy(0).wait_send()

        for l in range(N_LAYER):
            load_weights(0, l)

        def z_block(s, i, forward_pass):
            e, l = layer_of(s)
            off, w = subs[i]
            q = e if forward_pass else N_CHUNK * block_of(e) + e % N_CHUNK
            b = (n_sub * s + i) % (n_sub + 1)
            return zs.at[q, l, :, pl.ds(off, w)], zb.at[b, :, pl.ds(0, w)], b

        def z_out(s, i):
            store, buf, b = z_block(s, i, True)
            return pltpu.make_async_copy(buf, store, sems.zo.at[b])

        def z_in(s, i):
            store, buf, b = z_block(s, i, False)
            return pltpu.make_async_copy(store, buf, sems.zi.at[b])

        loss_row[...] = jnp.zeros_like(loss_row)

        def fwd_step(s, _):
            e, l = layer_of(s)
            v, m = e // N_CHUNK, e % N_CHUNK
            top = (stage == 1) & (v == 1)
            with jax.named_scope("f_pre"):
                start_tile(s, e, l, l == 0)

                @pl.when(top & (l == 0))
                def _():
                    pltpu.make_async_copy(targets.at[m], tgt, sems.t).start()

                @pl.when(m == 0)
                def _():
                    wait_weights(l)

                @pl.when(s >= 1)
                def _():
                    for i in range(n_sub - 1):
                        z_out(s - 1, i).wait()

                pl.when(s >= 2)(lambda: z_out(s - 2, n_sub - 1).wait())

            with jax.named_scope("f_mm"):
                for i, (off, w) in enumerate(subs):
                    h = ring[s % 3]
                    z = jnp.dot(h, wub[l, :, off : off + w], preferred_element_type=F32)
                    zb[(n_sub * s + i) % (n_sub + 1), :, :w] = z
                    if i:
                        z_out(s, i - 1).start()
                    a = gelu(z).astype(BF16)
                    part = jnp.dot(a, wdb[l, off : off + w, :], preferred_element_type=F32)
                    acc[...] = (h.astype(F32) if i == 0 else acc[...]) + part

            z_out(s, n_sub - 1).start()
            with jax.named_scope("f_end"):
                end_tile(s, e, l, l == N_LAYER - 1)

                @pl.when(e == N_CHUNK - 1)
                def _():
                    load_weights(1, l)

                @pl.when(l < N_LAYER - 1)
                def _():
                    ring[(s + 1) % 3] = acc[...].astype(BF16)

                @pl.when(l == N_LAYER - 1)
                def _():
                    @pl.when(top)
                    def _():
                        pltpu.make_async_copy(targets.at[m], tgt, sems.t).wait()
                        err = acc[...].astype(BF16).astype(F32) - tgt[...].astype(F32)
                        loss_row[...] += jnp.sum(err * err, axis=0, keepdims=True)
                        zin[m] = (err * (1.0 / n_tok)).astype(BF16)

                    @pl.when(jnp.logical_not(top))
                    def _():
                        zout[...] = acc[...].astype(BF16)

                    @pl.when(sent(e))
                    def _():
                        z_copy(m).start()

            return 0

        n_fwd = N_TILE // 2
        lax.fori_loop(0, n_fwd, fwd_step, 0)
        z_out(n_fwd - 2, n_sub - 1).wait()
        for i in range(n_sub):
            z_out(n_fwd - 1, i).wait()
        for i in range(n_sub):
            z_in(n_fwd, i).start()

        def bwd_step(s, _):
            e, l = layer_of(s)
            m = e % N_CHUNK

            with jax.named_scope("b_pre"):
                start_tile(s, e, l, l == N_LAYER - 1)
                for i in range(n_sub):
                    z_in(s, i).wait()
            after = jnp.minimum(s + 1, N_TILE - 1)

            def z_next(i):
                store, _, _ = z_block(after, i, False)
                _, buf, b = z_block(s + 1, i, False)
                pltpu.make_async_copy(store, buf, sems.zi.at[b]).start()

            z_next(0)

            @pl.when(e == HALF + N_CHUNK)
            def _():
                wait_weights(l)

            with jax.named_scope("b_mm"):
                for i, (off, w) in enumerate(subs):
                    for o in range(0, w, BWD_BLOCK):
                        cut = slice(off + o, off + o + BWD_BLOCK)
                        g = ring[s % 3]
                        da = lax.dot_general(g, wdb[l, cut, :], NT, preferred_element_type=F32)
                        _, slope = gelu_and_slope(zb[(n_sub * s + i) % (n_sub + 1), :, o : o + BWD_BLOCK])
                        dz = (slope * da.astype(BF16).astype(F32)).astype(BF16)
                        part = lax.dot_general(dz, wub[l, :, cut], NT, preferred_element_type=F32)
                        acc[...] = (g.astype(F32) if i + o == 0 else acc[...]) + part
                    if i + 1 < n_sub:
                        z_next(i + 1)

            with jax.named_scope("b_end"):
                end_tile(s, e, l, l == 0)

                @pl.when(e == HALF + N_CHUNK - 1)
                def _():
                    load_weights(0, l)

                @pl.when(l > 0)
                def _():
                    ring[(s + 1) % 3] = acc[...].astype(BF16)

                @pl.when(l == 0)
                def _():
                    zout[...] = acc[...].astype(BF16)

                    @pl.when(sent(e))
                    def _():
                        z_copy(m).start()

            return 0

        lax.fori_loop(n_fwd, N_TILE, bwd_step, 0)
        for i in range(n_sub):
            store, _, _ = z_block(N_TILE - 1, i, False)
            _, buf, b = z_block(N_TILE, i, False)
            pltpu.make_async_copy(store, buf, sems.zi.at[b]).wait()

        @pl.when(sent(2 * HALF - 1))
        def _():
            z_copy(0).wait_send()

        loss_ref[...] = jnp.broadcast_to(jnp.sum(loss_row[...], axis=1, keepdims=True), loss_ref.shape)

    width = window_width(ff)
    seg_d, seg_u = dd.shape[2], upp.shape[2]

    def grads(wub, wdb, hb, gb, gd, gu, cb, ubb):
        def weight_copies(j):
            v, k = place.layer(j)
            start = pl.multiple_of(place.share(j).start(ff), 128)
            b = j % 2
            return (
                pltpu.make_async_copy(wu.at[v, k, :, pl.ds(start, width)], wub.at[b], sems.ww.at[b, 0]),
                pltpu.make_async_copy(wd.at[v, k, pl.ds(start, width), :], wdb.at[b], sems.ww.at[b, 1]),
            )

        def fetches(n):
            v, k = place.layer(n // N_STEP)
            t = n % N_STEP
            m, part = t // 2, 2 * (t % 2)
            h_at = N_CHUNK * v + part
            g_at = HALF + N_CHUNK * (1 - v) + part
            b = n % 2
            return (
                pltpu.make_async_copy(hg.at[m, pl.ds(h_at, 2), k], hb.at[b], sems.hb.at[b]),
                pltpu.make_async_copy(hg.at[m, pl.ds(g_at, 2), k], gb.at[b], sems.gb.at[b]),
            )

        def arrived(group):
            ref = hg.at[2, pl.ds(0, HALF), 0] if group else hg.at[2, pl.ds(0, HALF)]
            remote(ref, ref, sems.c_send, sems.c_recv.at[group], z_peer).wait_recv()
            remote(ref, ref, sems.f_send, sems.f_recv.at[group], z_peer).wait_recv()

        def stage_copies(j):
            sh = place.share(j)
            b = j % 2
            up = []
            for i in range(4):
                keep = sh.piece(i)
                send = keep + sh.wu * (1 - 2 * sh.u)
                for to, row, sem in ((sup, send, 0), (kup, keep, 1)):
                    src = gu.at[b, pl.ds(pl.multiple_of(row * seg_u, 8), seg_u), :]
                    up.append(pltpu.make_async_copy(src, to.at[j, i], sems.st.at[sem]))
            base = sh.base(ff)
            part = [gd.at[b, pl.ds(pl.multiple_of(base + seg_d * i, 8), seg_d), :] for i in (c, 1 - c)]
            same = [pltpu.make_async_copy(part[0], to.at[j, 0], sems.st.at[2]) for to in (dd, sd)]
            other = pltpu.make_async_copy(part[1], sd.at[j, 1], sems.st.at[3])
            return sh, up, same, other

        def stage_out(j):
            sh, up, same, other = stage_copies(j)
            for cp in up:
                cp.start()
            other.start()
            pl.when(sh.away == 0)(same[0].start)
            pl.when(sh.away == 1)(same[1].start)

        def down_same(j, sh):
            return remote(sd.at[j, 0], dd.at[j, 1], sems.ds_send, sems.d_recv.at[j, 1], at(sh.dest_same))

        def up_exchange(j, sh):
            return remote(sup.at[j], ub.at[j], sems.u_send, sems.u_recv.at[j], at(sh.partner))

        def send_out(j):
            sh = place.share(j)
            pltpu.make_async_copy(sup.at[j], sup.at[j], sems.st.at[0]).wait()
            up_exchange(j, sh).start()
            pltpu.make_async_copy(sd.at[j, 1], sd.at[j, 1], sems.st.at[3]).wait()
            slot = sh.slot_other
            remote(
                sd.at[j, 1], dd.at[j, slot], sems.d_send, sems.d_recv.at[j, slot], at(sh.dest_other)
            ).start()

            pltpu.make_async_copy(sd.at[j, 0], sd.at[j, 0], sems.st.at[2]).wait()
            pl.when(sh.away == 1)(down_same(j, sh).start)
            pltpu.make_async_copy(kup.at[j], kup.at[j], sems.st.at[1]).wait()

        def piece_sends(j, b):
            sh = place.share(j)
            out = [pltpu.make_async_copy(cb.at[b, 0], upp.at[j, 0], sems.p_here.at[b])]
            for i in range(1, 4):
                out.append(remote(cb.at[b, i], upp.at[j, i], sems.p_send.at[b], sems.p_recv.at[j], at(sh.piece(i))))
            return out

        def wait_pieces(j, b):
            piece_sends(j, b)[0].wait()
            ref = cb.at[b, pl.ds(1, 3)]
            remote(ref, ref, sems.p_send.at[b], sems.p_recv.at[j], z_peer).wait_send()

        def sum_loads(j, b):
            return (
                pltpu.make_async_copy(kup.at[j], cb.at[b], sems.cl.at[0]),
                pltpu.make_async_copy(ub.at[j], ubb, sems.cl.at[1]),
            )

        def sum_load(j, b):
            up_exchange(j, place.share(j)).wait_recv()
            for cp in sum_loads(j, b):
                cp.start()

        def sum_add(j, b):
            for cp in sum_loads(j, b):
                cp.wait()
            cb[b] += ubb[...]
            for cp in piece_sends(j, b):
                cp.start()

        for cp in weight_copies(0) + fetches(0):
            cp.start()

        loss_peers = [at(place.flip(0, 0, 1)), at(place.flip(0, 1, 0)), at(place.flip(1, 0, 0)), z_peer]

        def loss_copy(r):
            return remote(lbuf.at[0, r], lbuf.at[1, r], sems.l_send, sems.l_recv.at[r], loss_peers[r])

        def step(n, _):
            j, t = n // N_STEP, n % N_STEP
            b, jb = n % 2, j % 2

            with jax.named_scope("w_fwd"):
                @pl.when(n < SHORT)
                def _():
                    forward(n + N_TILE - SHORT)

            with jax.named_scope("w_arr"):
                for group, first in enumerate((0, 3, 4, 5)):
                    pl.when(n == first * N_STEP + 3)(lambda group=group: arrived(group))

            @pl.when(n + 1 < N_GRAD * N_STEP)
            def _():
                for cp in fetches(n + 1):
                    cp.start()

            with jax.named_scope("w_pre"):
                for r in range(4):

                    @pl.when(n == 2 * r)
                    def _():
                        if r:
                            loss_copy(r - 1).wait()
                            loss_ref[...] += lbuf[1, r - 1]
                        lbuf[0, r] = loss_ref[...]

                    @pl.when(n == 2 * r + 1)
                    def _():
                        loss_copy(r).start()

                @pl.when(n == 8)
                def _():
                    loss_copy(3).wait()
                    loss_ref[...] += lbuf[1, 3]

                @pl.when(t == 0)
                def _():
                    for cp in weight_copies(j):
                        cp.wait()

                @pl.when((t == 1) & (j + 1 < N_GRAD))
                def _():
                    for cp in weight_copies(j + 1):
                        cp.start()

                @pl.when((t == 0) & (j >= 1))
                def _():
                    stage_out(j - 1)

                @pl.when((t == 1) & (j >= 1))
                def _():
                    send_out(j - 1)

            with jax.named_scope("w_sum"):
                @pl.when((t == 5) & (j >= 3))
                def _():
                    sum_load(j - 3, j - 3)

                @pl.when((t == 6) & (j >= 3))
                def _():
                    sum_add(j - 3, j - 3)

                @pl.when(n == 5 * N_STEP + 3)
                def _():
                    wait_pieces(0, 0)
                    sum_load(4, 0)

                @pl.when(n == 5 * N_STEP + 4)
                def _():
                    sum_add(4, 0)

            with jax.named_scope("w_fetch"):
                for cp in fetches(n):
                    cp.wait()
            h = hb[b].reshape(2 * rows, d)
            g = gb[b].reshape(2 * rows, d)
            with jax.named_scope("w_mm"):
                for off, w in grad_blocks(width):
                    cut = slice(off, off + w)
                    z = jnp.dot(h, wub[jb, :, cut], preferred_element_type=F32)
                    da = lax.dot_general(g, wdb[jb, cut, :], NT, preferred_element_type=F32).astype(BF16).astype(F32)
                    a, slope = gelu_and_slope(z)
                    a = a.astype(BF16)
                    dz = (slope * da).astype(BF16)
                    down = lax.dot_general(a, g, TN, preferred_element_type=F32)
                    gd[jb, cut, :] = jnp.where(t == 0, 0.0, gd[jb, cut, :]) + down
                    up = lax.dot_general(h, dz, TN, preferred_element_type=F32)
                    gu[jb, :, cut] = jnp.where(t == 0, 0.0, gu[jb, :, cut]) + up
            return 0

        lax.fori_loop(0, N_GRAD * N_STEP, step, 0)
        with jax.named_scope("t_stage"):
            stage_out(5)
            send_out(5)
        with jax.named_scope("t_sum5"):
            wait_pieces(2, 2)
            sum_load(5, 2)
            sum_add(5, 2)
        with jax.named_scope("t_sum3"):
            wait_pieces(1, 1)
            sum_load(3, 1)
            sum_add(3, 1)
        with jax.named_scope("t_pieces"):
            for j, b in ((4, 0), (5, 2), (3, 1)):
                wait_pieces(j, b)

    pl.run_scoped(
        chain,
        pltpu.VMEM((N_LAYER, d, ff), BF16),
        pltpu.VMEM((N_LAYER, ff, d), BF16),
        pltpu.VMEM((3, *tile), BF16),
        pltpu.VMEM(tile, BF16),
        pltpu.VMEM((len(sub_blocks(ff)) + 1, rows, sub_blocks(ff)[0][1]), F32),
        pltpu.VMEM(tile, BF16),
        pltpu.VMEM(tile, F32),
        pltpu.VMEM((1, d), F32),
    )
    pl.run_scoped(
        grads,
        pltpu.VMEM((2, d, width), BF16),
        pltpu.VMEM((2, width, d), BF16),
        pltpu.VMEM((2, 2, *tile), BF16),
        pltpu.VMEM((2, 2, *tile), BF16),
        pltpu.VMEM((2, width, d), F32),
        pltpu.VMEM((2, d, width), F32),
        pltpu.VMEM((3, 4, seg_u, width), F32),
        pltpu.VMEM((4, seg_u, width), F32),
    )

    with jax.named_scope("t_all"):
        for j in range(N_GRAD):
            sh = place.share(j)
            ref = upp.at[j, pl.ds(1, 3)]
            remote(ref, ref, sems.p_send.at[0], sems.p_recv.at[j], z_peer).wait_recv()
            ref = dd.at[j, 0]
            remote(ref, ref, sems.d_send, sems.d_recv.at[j, 1], z_peer).wait_recv()

            @pl.when(sh.away == 1)
            def _():
                remote(ref, ref, sems.ds_send, sems.d_recv.at[j, 0], z_peer).wait()

        remote(sup, sup, sems.u_send, sems.u_recv.at[0], z_peer).wait_send()
        ref = sd.at[:, 1]
        remote(ref, ref, sems.d_send, sems.d_recv.at[0, 0], z_peer).wait_send()
        for sem in (sems.a_send, sems.c_send, sems.f_send):
            remote(hg.at[0], hg.at[0], sem, sems.a_recv.at[0], z_peer).wait_send()


SEMS = {
    "w": (N_LAYER, 2),
    "ld": (),
    "zo": (N_RING,),
    "zi": (N_RING,),
    "t": (),
    "z_send": (),
    "z_recv": (N_CHUNK,),
    "a_send": (),
    "a_recv": (N_TILE,),
    "c_send": (),
    "c_recv": (4,),
    "f_send": (),
    "f_recv": (4,),
    "ww": (2, 2),
    "hb": (2,),
    "gb": (2,),
    "st": (4,),
    "u_send": (),
    "u_recv": (N_GRAD,),
    "d_send": (),
    "ds_send": (),
    "d_recv": (N_GRAD, 2),
    "cl": (2,),
    "p_send": (3,),
    "p_here": (3,),
    "p_recv": (N_GRAD,),
    "l_send": (),
    "l_recv": (4,),
}


class Sems:
    def __init__(self, refs):
        for name, ref in zip(SEMS, refs, strict=True):
            setattr(self, name, ref)


def step_call(tokens, targets, wu, wd, n_tok, n_data):
    n_chunk, rows, d = tokens.shape
    ff = wu.shape[-1]
    width = window_width(ff)
    pieces = jax.ShapeDtypeStruct((N_GRAD, 4, d // n_data, width), F32)
    parts = jax.ShapeDtypeStruct((N_GRAD, 2, ff // n_data, d), F32)

    def body(*refs):
        n = 13 + 2
        step_kernel(n_tok, *refs[:n], Sems(refs[n:]))

    return pl.pallas_call(
        body,
        in_specs=[ANY] * 4,
        out_specs=[ANY] * 3 + [pl.BlockSpec(memory_space=pltpu.VMEM)] + [ANY] * 5,
        out_shape=[
            jax.ShapeDtypeStruct((4, 2 * HALF, N_LAYER, rows, d), BF16),
            parts,
            pieces,
            jax.ShapeDtypeStruct((8, 128), F32),
            pieces,
            pieces,
            pieces,
            parts,
            jax.ShapeDtypeStruct((HALF, N_LAYER, rows, ff), F32),
        ],
        scratch_shapes=[
            pltpu.VMEM((n_chunk, rows, d), BF16),
            pltpu.VMEM((2, 4, 8, 128), F32),
            *[pltpu.SemaphoreType.DMA(shape) for shape in SEMS.values()],
        ],
        compiler_params=pltpu.CompilerParams(collective_id=0, has_side_effects=True, vmem_limit_bytes=67043328),
        name="step",
    )(tokens, targets, wu, wd)


def final_kernel(scal, dd, upp, down_ref, up_ref):
    down_ref[0, 0] = dd[0, 0] + dd[0, 1]
    width = upp.shape[-1]
    for i in range(4):
        start = pl.multiple_of(scal[4 * pl.program_id(0) + i], 128)
        up_ref[0, 0, :, pl.ds(start, width)] = upp[0, i]


def final_call(scal, dd, upp, n_data):
    seg_d, d = dd.shape[2:]
    seg_u, width = upp.shape[2:]
    ff = seg_d * n_data
    return pl.pallas_call(
        final_kernel,
        grid_spec=pltpu.PrefetchScalarGridSpec(
            num_scalar_prefetch=1,
            grid=(N_GRAD,),
            in_specs=[
                pl.BlockSpec((1, 2, seg_d, d), lambda j, s: (j, 0, 0, 0)),
                pl.BlockSpec((1, 4, seg_u, width), lambda j, s: (j, 0, 0, 0)),
            ],
            out_specs=[
                pl.BlockSpec((1, 1, seg_d, d), lambda j, s: (1 - j // N_LAYER, N_LAYER - 1 - j % N_LAYER, 0, 0)),
                pl.BlockSpec((1, 1, seg_u, ff), lambda j, s: (1 - j // N_LAYER, N_LAYER - 1 - j % N_LAYER, 0, 0)),
            ],
        ),
        out_shape=[
            jax.ShapeDtypeStruct((2, N_LAYER, seg_d, d), F32),
            jax.ShapeDtypeStruct((2, N_LAYER, seg_u, ff), F32),
        ],
        compiler_params=pltpu.CompilerParams(dimension_semantics=("arbitrary",), vmem_limit_bytes=62 * 2**20),
        name="final",
    )(scal, dd, upp)


def window_table(n_data, ff):
    table = []
    for dev in range(n_data):
        place = Place(0, dev)
        row = []
        for j in range(N_GRAD):
            for i in range(4):
                row.append(Place(0, place.share(j).piece(i)).share(j).start(ff))
        table.append(row)
    return np.array(table, np.int32)


def solution(mesh):
    n_data = mesh.shape["data"]

    def device_fn(tokens_loc, targets_loc, wu, wd):
        n_micro, seq_len, d = tokens_loc.shape
        n_tok = n_data * n_micro * seq_len
        ff = wu.shape[-1]
        rows = n_micro * seq_len // N_CHUNK
        tokens = tokens_loc.reshape(N_CHUNK, rows, d)
        targets = targets_loc.reshape(N_CHUNK, rows, d)
        out = step_call(tokens, targets, wu, wd, n_tok, n_data)
        dd, upp, loss = out[1:4]
        starts = jnp.asarray(window_table(n_data, ff))
        scal = lax.dynamic_index_in_dim(starts, lax.axis_index("data"), 0, keepdims=False)
        down, up = final_call(scal, dd, upp, n_data)
        return loss[0, 0] / (2.0 * n_tok), up, down

    return jax.shard_map(
        device_fn,
        mesh=mesh,
        in_specs=(P("data"), P("data"), P(None, "stage"), P(None, "stage")),
        out_specs=(P(), P(None, "stage", "data"), P(None, "stage", "data")),
        check_vma=False,
    )
```

```python
import jax
import jax.numpy as jnp
import numpy as np
from jax import lax
from jax.experimental import pallas as pl
from jax.experimental.pallas import tpu as pltpu
from jax.sharding import PartitionSpec as P

F32, BF16 = jnp.float32, jnp.bfloat16
MESH = pl.DeviceIdType.MESH
N_CHUNK = 4
N_LAYER = 3
HALF = 2 * N_CHUNK
N_TILE = 2 * HALF * N_LAYER
N_GRAD = 2 * N_LAYER
N_SPARE = 2
N_RING = 12
LOSS_GAP = 10
SUM_AT = {0: (0, 29), 1: (1, 37), 2: (2, 42), 4: (0, 44)}
BWD_BLOCK = 256
N_STEP = 8
DELAY = 4 * N_LAYER
NT = (((1,), (1,)), ((), ()))
TN = (((0,), (0,)), ((), ()))
C0 = 0.7978845608028654
C1 = 0.044715
ANY = pl.BlockSpec(memory_space=pl.ANY)


def gelu(z):
    return z * (0.5 * (1.0 + jnp.tanh(C0 * (z + C1 * (z * z * z)))))


def gelu_and_slope(z):
    z2 = z * z
    t = jnp.tanh(C0 * (z + C1 * (z2 * z)))
    cdf = 0.5 * (1.0 + t)
    slope = cdf + (0.5 * z) * ((1.0 - t * t) * (C0 + (3.0 * C0 * C1) * z2))
    return cdf * z, slope


def sub_blocks(ff):
    step = 512
    return [(o, min(step, ff - o)) for o in range(0, ff, step)]


def grad_blocks(width):
    return [(o, min(768, width - o)) for o in range(0, width, 768)]


def window_width(ff):
    return (ff // 4 + 127) // 128 * 128


class Place:
    def __init__(self, stage, dev):
        self.stage, self.dev = stage, dev
        self.y, self.x, self.c = dev // 4, (dev // 2) % 2, dev % 2

    def flip(self, fy, fx, fc):
        return self.dev + fy * (4 - 8 * self.y) + fx * (2 - 4 * self.x) + fc * (1 - 2 * self.c)

    def gather(self, v, k):
        is_y = (v + k) % 2
        kind_c = (1 - v) * (1 - k // 2)
        one = self.flip(is_y, 1 - is_y, 0)
        two = self.flip(kind_c * (1 - is_y), kind_c * is_y, 1 - kind_c)
        return one, two

    def layer(self, j):
        return 1 - j // N_LAYER, N_LAYER - 1 - j % N_LAYER

    def group(self, v, k):
        return (1 - v) * (N_LAYER - k)

    def share(self, j):
        y, x, c = self.y, self.x, self.c
        v, k = self.layer(j)
        kc = j // 4
        dy = (1 - kc) * ((v + k) % 2)
        dx = (1 - kc) * (1 - (v + k) % 2)
        sh = Share()
        sh.kc = kc
        sh.p = (dy + kc) * y + dx * c
        sh.q = dy * c + (dx + kc) * x
        sh.wu, sh.w1, sh.w2 = 2 * dy + 4 * dx + kc, 4 * dy + 2 * dx + 4 * kc, dy + dx + 2 * kc
        sh.u = dy * x + dx * y + kc * c
        sh.r1 = dy * y + dx * x + kc * y
        sh.r2 = (dy + dx) * c + kc * x
        sh.partner = self.dev + sh.wu * (1 - 2 * sh.u)
        away = (1 - kc) * (sh.u * (1 - c) + c * (1 - sh.u))
        sh.away = away
        sh.dest_same = self.dev + away * sh.wu * (1 - 2 * sh.u)
        sh.dest_other = sh.dest_same + (1 - 2 * c)
        sh.slot_other = kc + away
        return sh


class Share:
    def piece(self, i):
        r1 = self.r1 + (i // 2) * (1 - 2 * self.r1)
        r2 = self.r2 + (i % 2) * (1 - 2 * self.r2)
        return self.w1 * r1 + self.w2 * r2 + self.wu * self.u

    def start(self, ff):
        return (ff // 2) * self.p + (ff // 2 - window_width(ff)) * self.q

    def base(self, ff):
        return (ff // 4 - (ff // 2 - window_width(ff))) * self.q


def layer_of(s):
    e = s // N_LAYER
    r = s - N_LAYER * e
    back = e // HALF
    return e, r + back * (N_LAYER - 1 - 2 * r)


def block_of(e):
    back = e // HALF
    first = (e - HALF * back) // N_CHUNK
    return first + back * (1 - 2 * first)


def step_kernel(n_tok, tokens, targets, wu, wd, hg, dd, upp, loss_ref, sup, kup, ub, sd, zs, zin, lbuf, sems):
    place = Place(lax.axis_index("stage"), lax.axis_index("data"))
    stage, dev, c = place.stage, place.dev, place.c
    d, ff = wu.shape[2:]
    rows = zin.shape[1]
    tile = (rows, d)

    def remote(src, dst, send, recv, to):
        return pltpu.make_async_remote_copy(src, dst, send, recv, to, MESH)

    def at(index):
        return (stage, index)

    z_peer = (1 - stage, dev)
    local_peers = [place.flip(*f) for f in ((0, 0, 1), (0, 1, 0), (1, 0, 0), (0, 1, 1), (1, 0, 1), (1, 1, 0))]

    @pl.when(stage == 0)
    def _():
        for m in range(N_CHUNK):
            pltpu.make_async_copy(tokens.at[m], zin.at[m], sems.z_recv.at[m]).start()

    barrier = pltpu.get_barrier_semaphore()
    for peer in [z_peer] + [at(i) for i in local_peers]:
        pl.semaphore_signal(barrier, inc=1, device_id=peer, device_id_type=MESH)
    pl.semaphore_wait(barrier, 1 + len(local_peers))

    def a_copy(s):
        e, l = layer_of(s)
        one, _ = place.gather(block_of(e), l)
        return remote(hg.at[0, e, l], hg.at[1, e, l], sems.a_send, sems.a_recv.at[s], at(one))

    def c_copy(s):
        e, l = layer_of(s)
        v = block_of(e)
        _, two = place.gather(v, l)
        return remote(hg.at[0, e, l], hg.at[2, e, l], sems.c_send, sems.c_recv.at[place.group(v, l)], at(two))

    def forward(s):
        e, l = layer_of(s)
        v = block_of(e)
        _, two = place.gather(v, l)
        a_copy(s).wait_recv()
        remote(hg.at[1, e, l], hg.at[3, e, l], sems.f_send, sems.f_recv.at[place.group(v, l)], at(two)).start()

    def chain(wub, wdb, ring, zout, zb, tgt, acc, loss_row):
        subs = sub_blocks(ff)
        n_sub = len(subs)
        n_ring = n_sub + N_SPARE
        assert n_ring <= N_RING

        def weight_copies(v, l):
            return (
                pltpu.make_async_copy(wu.at[v, l], wub.at[l], sems.w.at[l, 0]),
                pltpu.make_async_copy(wd.at[v, l], wdb.at[l], sems.w.at[l, 1]),
            )

        def load_weights(v, l):
            for cp in weight_copies(v, l):
                cp.start()

        def wait_weights(l):
            for cp in weight_copies(0, l):
                cp.wait()

        def z_copy(m):
            return remote(zout, zin.at[m], sems.z_send, sems.z_recv.at[m], z_peer)

        def sent(e):
            fwd = (e < HALF) & ((stage == 0) | (e < N_CHUNK))
            return fwd | ((e >= HALF) & ((stage == 1) | (e < HALF + N_CHUNK)))

        def start_tile(s, e, l, first):
            @pl.when(first)
            def _():
                @pl.when(jnp.logical_not((stage == 1) & (e >= HALF) & (e < HALF + N_CHUNK)))
                def _():
                    z_copy(e % N_CHUNK).wait_recv()

                ring[s % 3] = zin[e % N_CHUNK]

            pltpu.make_async_copy(ring.at[s % 3], hg.at[0, e, l], sems.ld).start()

        def end_tile(s, e, l, last):
            pltpu.make_async_copy(ring.at[s % 3], hg.at[0, e, l], sems.ld).wait()
            a_copy(s).start()
            c_copy(s).start()

            @pl.when(s >= DELAY)
            def _():
                forward(s - DELAY)

            @pl.when(last & (e >= 1))
            def _():
                @pl.when(sent(e - 1))
                def _():
                    z_copy(0).wait_send()

        for l in range(N_LAYER):
            load_weights(0, l)

        def z_block(s, i, forward_pass):
            e, l = layer_of(s)
            off, w = subs[i]
            q = e if forward_pass else N_CHUNK * block_of(e) + e % N_CHUNK
            b = (n_sub * s + i) % n_ring
            return zs.at[q, l, i, :, pl.ds(0, w)], zb.at[b, :, pl.ds(0, w)], b

        def z_out(s, i):
            store, buf, b = z_block(s, i, True)
            return pltpu.make_async_copy(buf, store, sems.zo.at[b])

        def z_in(s, i):
            store, buf, b = z_block(s, i, False)
            return pltpu.make_async_copy(store, buf, sems.zi.at[b])

        loss_row[...] = jnp.zeros_like(loss_row)

        def fwd_step(s, _):
            e, l = layer_of(s)
            v, m = e // N_CHUNK, e % N_CHUNK
            top = (stage == 1) & (v == 1)
            with jax.named_scope("f_pre"):
                start_tile(s, e, l, l == 0)

                @pl.when(top & (l == 0))
                def _():
                    pltpu.make_async_copy(targets.at[m], tgt, sems.t).start()

                @pl.when(m == 0)
                def _():
                    wait_weights(l)

                @pl.when(s >= 1)
                def _():
                    for i in range(n_sub - N_SPARE):
                        z_out(s - 1, i).wait()

                @pl.when(s >= 2)
                def _():
                    for i in range(n_sub - N_SPARE, n_sub):
                        z_out(s - 2, i).wait()

            with jax.named_scope("f_mm"):
                for i, (off, w) in enumerate(subs):
                    h = ring[s % 3]
                    z = jnp.dot(h, wub[l, :, off : off + w], preferred_element_type=F32)
                    zb[(n_sub * s + i) % n_ring, :, :w] = z
                    if i:
                        z_out(s, i - 1).start()
                    a = gelu(z).astype(BF16)
                    part = jnp.dot(a, wdb[l, off : off + w, :], preferred_element_type=F32)
                    acc[...] = (h.astype(F32) if i == 0 else acc[...]) + part

            z_out(s, n_sub - 1).start()
            with jax.named_scope("f_end"):
                end_tile(s, e, l, l == N_LAYER - 1)

                @pl.when(e == N_CHUNK - 1)
                def _():
                    load_weights(1, l)

                @pl.when(l < N_LAYER - 1)
                def _():
                    ring[(s + 1) % 3] = acc[...].astype(BF16)

                @pl.when(l == N_LAYER - 1)
                def _():
                    @pl.when(top)
                    def _():
                        pltpu.make_async_copy(targets.at[m], tgt, sems.t).wait()
                        err = acc[...].astype(BF16).astype(F32) - tgt[...].astype(F32)
                        loss_row[...] += jnp.sum(err * err, axis=0, keepdims=True)
                        zin[m] = (err * (1.0 / n_tok)).astype(BF16)

                    @pl.when(jnp.logical_not(top))
                    def _():
                        zout[...] = acc[...].astype(BF16)

                    @pl.when(sent(e))
                    def _():
                        z_copy(m).start()

            return 0

        n_fwd = N_TILE // 2
        lax.fori_loop(0, n_fwd, fwd_step, 0)
        for i in range(n_sub - N_SPARE, n_sub):
            z_out(n_fwd - 2, i).wait()
        for i in range(n_sub):
            z_out(n_fwd - 1, i).wait()
        for i in range(n_sub):
            z_in(n_fwd, i).start()

        def bwd_step(s, _):
            e, l = layer_of(s)
            m = e % N_CHUNK

            with jax.named_scope("b_pre"):
                start_tile(s, e, l, l == N_LAYER - 1)
                for i in range(n_sub):
                    z_in(s, i).wait()
            after = jnp.minimum(s + 1, N_TILE - 1)

            def z_next(i):
                store, _, _ = z_block(after, i, False)
                _, buf, b = z_block(s + 1, i, False)
                pltpu.make_async_copy(store, buf, sems.zi.at[b]).start()

            for i in range(N_SPARE):
                z_next(i)

            @pl.when(e == HALF + N_CHUNK)
            def _():
                wait_weights(l)

            with jax.named_scope("b_mm"):
                for i, (off, w) in enumerate(subs):
                    for o in range(0, w, BWD_BLOCK):
                        cut = slice(off + o, off + o + BWD_BLOCK)
                        g = ring[s % 3]
                        da = lax.dot_general(g, wdb[l, cut, :], NT, preferred_element_type=F32)
                        _, slope = gelu_and_slope(zb[(n_sub * s + i) % n_ring, :, o : o + BWD_BLOCK])
                        dz = (slope * da.astype(BF16).astype(F32)).astype(BF16)
                        part = lax.dot_general(dz, wub[l, :, cut], NT, preferred_element_type=F32)
                        acc[...] = (g.astype(F32) if i + o == 0 else acc[...]) + part
                    if i + N_SPARE < n_sub:
                        z_next(i + N_SPARE)

            with jax.named_scope("b_end"):
                end_tile(s, e, l, l == 0)

                @pl.when(e == HALF + N_CHUNK - 1)
                def _():
                    load_weights(0, l)

                @pl.when(l > 0)
                def _():
                    ring[(s + 1) % 3] = acc[...].astype(BF16)

                @pl.when(l == 0)
                def _():
                    zout[...] = acc[...].astype(BF16)

                    @pl.when(sent(e))
                    def _():
                        z_copy(m).start()

            return 0

        lax.fori_loop(n_fwd, N_TILE, bwd_step, 0)
        for i in range(n_sub):
            store, _, _ = z_block(N_TILE - 1, i, False)
            _, buf, b = z_block(N_TILE, i, False)
            pltpu.make_async_copy(store, buf, sems.zi.at[b]).wait()

        @pl.when(sent(2 * HALF - 1))
        def _():
            z_copy(0).wait_send()

        loss_ref[...] = jnp.broadcast_to(jnp.sum(loss_row[...], axis=1, keepdims=True), loss_ref.shape)

    width = window_width(ff)
    seg_d, seg_u = dd.shape[2], upp.shape[2]

    def grads(wub, wdb, hb, gb, gd, gu, cb, ubb):
        def weight_copies(j):
            v, k = place.layer(j)
            start = pl.multiple_of(place.share(j).start(ff), 128)
            b = j % 2
            return (
                pltpu.make_async_copy(wu.at[v, k, :, pl.ds(start, width)], wub.at[b], sems.ww.at[b, 0]),
                pltpu.make_async_copy(wd.at[v, k, pl.ds(start, width), :], wdb.at[b], sems.ww.at[b, 1]),
            )

        def fetches(n):
            v, k = place.layer(n // N_STEP)
            t = n % N_STEP
            m, part = t // 2, 2 * (t % 2)
            h_at = N_CHUNK * v + part
            g_at = HALF + N_CHUNK * (1 - v) + part
            b = n % 2
            return (
                pltpu.make_async_copy(hg.at[m, pl.ds(h_at, 2), k], hb.at[b], sems.hb.at[b]),
                pltpu.make_async_copy(hg.at[m, pl.ds(g_at, 2), k], gb.at[b], sems.gb.at[b]),
            )

        def arrived(group):
            ref = hg.at[2, pl.ds(0, HALF), 0] if group else hg.at[2, pl.ds(0, HALF)]
            remote(ref, ref, sems.c_send, sems.c_recv.at[group], z_peer).wait_recv()
            remote(ref, ref, sems.f_send, sems.f_recv.at[group], z_peer).wait_recv()

        def stage_copies(j):
            sh = place.share(j)
            b = j % 2
            up = []
            for i in range(4):
                keep = sh.piece(i)
                send = keep + sh.wu * (1 - 2 * sh.u)
                for to, row, sem in ((sup, send, 0), (kup, keep, 1)):
                    src = gu.at[b, pl.ds(pl.multiple_of(row * seg_u, 8), seg_u), :]
                    up.append(pltpu.make_async_copy(src, to.at[j, i], sems.st.at[sem]))
            base = sh.base(ff)
            part = [gd.at[b, pl.ds(pl.multiple_of(base + seg_d * i, 8), seg_d), :] for i in (c, 1 - c)]
            same = [pltpu.make_async_copy(part[0], to.at[j, 0], sems.st.at[2]) for to in (dd, sd)]
            other = pltpu.make_async_copy(part[1], sd.at[j, 1], sems.st.at[3])
            return sh, up, same, other

        def stage_out(j):
            sh, up, same, other = stage_copies(j)
            for cp in up:
                cp.start()
            other.start()
            pl.when(sh.away == 0)(same[0].start)
            pl.when(sh.away == 1)(same[1].start)

        def down_same(j, sh):
            return remote(sd.at[j, 0], dd.at[j, 1], sems.ds_send, sems.d_recv.at[j, 1], at(sh.dest_same))

        def up_exchange(j, sh):
            return remote(sup.at[j], ub.at[j], sems.u_send, sems.u_recv.at[j], at(sh.partner))

        def send_out(j):
            sh = place.share(j)
            pltpu.make_async_copy(sup.at[j], sup.at[j], sems.st.at[0]).wait()
            up_exchange(j, sh).start()
            pltpu.make_async_copy(sd.at[j, 1], sd.at[j, 1], sems.st.at[3]).wait()
            slot = sh.slot_other
            remote(
                sd.at[j, 1], dd.at[j, slot], sems.d_send, sems.d_recv.at[j, slot], at(sh.dest_other)
            ).start()

            pltpu.make_async_copy(sd.at[j, 0], sd.at[j, 0], sems.st.at[2]).wait()
            pl.when(sh.away == 1)(down_same(j, sh).start)
            pltpu.make_async_copy(kup.at[j], kup.at[j], sems.st.at[1]).wait()

        def piece_sends(j, b):
            sh = place.share(j)
            out = [pltpu.make_async_copy(cb.at[b, 0], upp.at[j, 0], sems.p_here.at[b])]
            for i in range(1, 4):
                out.append(remote(cb.at[b, i], upp.at[j, i], sems.p_send.at[b], sems.p_recv.at[j], at(sh.piece(i))))
            return out

        def wait_pieces(j, b):
            piece_sends(j, b)[0].wait()
            ref = cb.at[b, pl.ds(1, 3)]
            remote(ref, ref, sems.p_send.at[b], sems.p_recv.at[j], z_peer).wait_send()

        def sum_loads(j, b):
            return (
                pltpu.make_async_copy(kup.at[j], cb.at[b], sems.cl.at[0]),
                pltpu.make_async_copy(ub.at[j], ubb, sems.cl.at[1]),
            )

        def sum_load(j, b):
            up_exchange(j, place.share(j)).wait_recv()
            for cp in sum_loads(j, b):
                cp.start()

        def sum_add(j, b):
            for cp in sum_loads(j, b):
                cp.wait()
            cb[b] += ubb[...]
            for cp in piece_sends(j, b):
                cp.start()

        for cp in weight_copies(0) + fetches(0):
            cp.start()

        loss_peers = [at(place.flip(0, 0, 1)), at(place.flip(0, 1, 0)), at(place.flip(1, 0, 0)), z_peer]

        def loss_copy(r):
            return remote(lbuf.at[0, r], lbuf.at[1, r], sems.l_send, sems.l_recv.at[r], loss_peers[r])

        def step(n, _):
            j, t = n // N_STEP, n % N_STEP
            b, jb = n % 2, j % 2

            with jax.named_scope("w_fwd"):
                @pl.when(n < DELAY)
                def _():
                    forward(n + N_TILE - DELAY)

            with jax.named_scope("w_arr"):
                for group, first in enumerate((0, 3, 4, 5)):
                    pl.when(n == first * N_STEP + 3)(lambda group=group: arrived(group))

            @pl.when(n + 1 < N_GRAD * N_STEP)
            def _():
                for cp in fetches(n + 1):
                    cp.start()

            with jax.named_scope("w_pre"):
                for r in range(4):

                    @pl.when(n == LOSS_GAP * r)
                    def _():
                        if r:
                            loss_copy(r - 1).wait()
                            loss_ref[...] += lbuf[1, r - 1]
                        lbuf[0, r] = loss_ref[...]

                    @pl.when(n == LOSS_GAP * r + 1)
                    def _():
                        loss_copy(r).start()

                @pl.when(n == LOSS_GAP * 4)
                def _():
                    loss_copy(3).wait()
                    loss_ref[...] += lbuf[1, 3]

                @pl.when(t == 0)
                def _():
                    for cp in weight_copies(j):
                        cp.wait()

                @pl.when((t == 1) & (j + 1 < N_GRAD))
                def _():
                    for cp in weight_copies(j + 1):
                        cp.start()

                @pl.when((t == 0) & (j >= 1))
                def _():
                    stage_out(j - 1)

                @pl.when((t == 1) & (j >= 1))
                def _():
                    send_out(j - 1)

            with jax.named_scope("w_sum"):
                for i, (b_, when) in SUM_AT.items():

                    @pl.when(n == when)
                    def _():
                        if i == 4:
                            wait_pieces(0, 0)
                        sum_load(i, b_)

                    @pl.when(n == when + 1)
                    def _():
                        sum_add(i, b_)

            with jax.named_scope("w_fetch"):
                for cp in fetches(n):
                    cp.wait()
            h = hb[b].reshape(2 * rows, d)
            g = gb[b].reshape(2 * rows, d)
            with jax.named_scope("w_mm"):
                for off, w in grad_blocks(width):
                    cut = slice(off, off + w)
                    z = jnp.dot(h, wub[jb, :, cut], preferred_element_type=F32)
                    da = lax.dot_general(g, wdb[jb, cut, :], NT, preferred_element_type=F32).astype(BF16).astype(F32)
                    a, slope = gelu_and_slope(z)
                    a = a.astype(BF16)
                    dz = (slope * da).astype(BF16)
                    down = lax.dot_general(a, g, TN, preferred_element_type=F32)
                    gd[jb, cut, :] = jnp.where(t == 0, 0.0, gd[jb, cut, :]) + down
                    up = lax.dot_general(h, dz, TN, preferred_element_type=F32)
                    gu[jb, :, cut] = jnp.where(t == 0, 0.0, gu[jb, :, cut]) + up
            return 0

        lax.fori_loop(0, N_GRAD * N_STEP, step, 0)
        with jax.named_scope("t_stage"):
            stage_out(5)
            send_out(5)
        with jax.named_scope("t_sum5"):
            wait_pieces(2, 2)
            sum_load(5, 2)
            sum_add(5, 2)
        with jax.named_scope("t_sum3"):
            wait_pieces(1, 1)
            sum_load(3, 1)
            sum_add(3, 1)
        with jax.named_scope("t_pieces"):
            for j, b in ((4, 0), (5, 2), (3, 1)):
                wait_pieces(j, b)

    pl.run_scoped(
        chain,
        pltpu.VMEM((N_LAYER, d, ff), BF16),
        pltpu.VMEM((N_LAYER, ff, d), BF16),
        pltpu.VMEM((3, *tile), BF16),
        pltpu.VMEM(tile, BF16),
        pltpu.VMEM((len(sub_blocks(ff)) + N_SPARE, rows, sub_blocks(ff)[0][1]), F32),
        pltpu.VMEM(tile, BF16),
        pltpu.VMEM(tile, F32),
        pltpu.VMEM((1, d), F32),
    )
    pl.run_scoped(
        grads,
        pltpu.VMEM((2, d, width), BF16),
        pltpu.VMEM((2, width, d), BF16),
        pltpu.VMEM((2, 2, *tile), BF16),
        pltpu.VMEM((2, 2, *tile), BF16),
        pltpu.VMEM((2, width, d), F32),
        pltpu.VMEM((2, d, width), F32),
        pltpu.VMEM((3, 4, seg_u, width), F32),
        pltpu.VMEM((4, seg_u, width), F32),
    )

    with jax.named_scope("t_all"):
        for j in range(N_GRAD):
            sh = place.share(j)
            ref = upp.at[j, pl.ds(1, 3)]
            remote(ref, ref, sems.p_send.at[0], sems.p_recv.at[j], z_peer).wait_recv()
            ref = dd.at[j, 0]
            remote(ref, ref, sems.d_send, sems.d_recv.at[j, 1], z_peer).wait_recv()

            @pl.when(sh.away == 1)
            def _():
                remote(ref, ref, sems.ds_send, sems.d_recv.at[j, 0], z_peer).wait()

        remote(sup, sup, sems.u_send, sems.u_recv.at[0], z_peer).wait_send()
        ref = sd.at[:, 1]
        remote(ref, ref, sems.d_send, sems.d_recv.at[0, 0], z_peer).wait_send()
        for sem in (sems.a_send, sems.c_send, sems.f_send):
            remote(hg.at[0], hg.at[0], sem, sems.a_recv.at[0], z_peer).wait_send()


SEMS = {
    "w": (N_LAYER, 2),
    "ld": (),
    "zo": (N_RING,),
    "zi": (N_RING,),
    "t": (),
    "z_send": (),
    "z_recv": (N_CHUNK,),
    "a_send": (),
    "a_recv": (N_TILE,),
    "c_send": (),
    "c_recv": (4,),
    "f_send": (),
    "f_recv": (4,),
    "ww": (2, 2),
    "hb": (2,),
    "gb": (2,),
    "st": (4,),
    "u_send": (),
    "u_recv": (N_GRAD,),
    "d_send": (),
    "ds_send": (),
    "d_recv": (N_GRAD, 2),
    "cl": (2,),
    "p_send": (3,),
    "p_here": (3,),
    "p_recv": (N_GRAD,),
    "l_send": (),
    "l_recv": (4,),
}


class Sems:
    def __init__(self, refs):
        for name, ref in zip(SEMS, refs, strict=True):
            setattr(self, name, ref)


def step_call(tokens, targets, wu, wd, n_tok, n_data):
    n_chunk, rows, d = tokens.shape
    ff = wu.shape[-1]
    width = window_width(ff)
    pieces = jax.ShapeDtypeStruct((N_GRAD, 4, d // n_data, width), F32)
    parts = jax.ShapeDtypeStruct((N_GRAD, 2, ff // n_data, d), F32)

    def body(*refs):
        n = 13 + 2
        step_kernel(n_tok, *refs[:n], Sems(refs[n:]))

    return pl.pallas_call(
        body,
        in_specs=[ANY] * 4,
        out_specs=[ANY] * 3 + [pl.BlockSpec(memory_space=pltpu.VMEM)] + [ANY] * 5,
        out_shape=[
            jax.ShapeDtypeStruct((4, 2 * HALF, N_LAYER, rows, d), BF16),
            parts,
            pieces,
            jax.ShapeDtypeStruct((8, 128), F32),
            pieces,
            pieces,
            pieces,
            parts,
            jax.ShapeDtypeStruct((HALF, N_LAYER, len(sub_blocks(ff)), rows, sub_blocks(ff)[0][1]), F32),
        ],
        scratch_shapes=[
            pltpu.VMEM((n_chunk, rows, d), BF16),
            pltpu.VMEM((2, 4, 8, 128), F32),
            *[pltpu.SemaphoreType.DMA(shape) for shape in SEMS.values()],
        ],
        compiler_params=pltpu.CompilerParams(collective_id=0, has_side_effects=True, vmem_limit_bytes=67043328),
        name="step",
    )(tokens, targets, wu, wd)


def final_kernel(scal, dd, upp, down_ref, up_ref):
    down_ref[0, 0] = dd[0, 0] + dd[0, 1]
    width = upp.shape[-1]
    for i in range(4):
        start = pl.multiple_of(scal[4 * pl.program_id(0) + i], 128)
        up_ref[0, 0, :, pl.ds(start, width)] = upp[0, i]


def final_call(scal, dd, upp, n_data):
    seg_d, d = dd.shape[2:]
    seg_u, width = upp.shape[2:]
    ff = seg_d * n_data
    return pl.pallas_call(
        final_kernel,
        grid_spec=pltpu.PrefetchScalarGridSpec(
            num_scalar_prefetch=1,
            grid=(N_GRAD,),
            in_specs=[
                pl.BlockSpec((1, 2, seg_d, d), lambda j, s: (j, 0, 0, 0)),
                pl.BlockSpec((1, 4, seg_u, width), lambda j, s: (j, 0, 0, 0)),
            ],
            out_specs=[
                pl.BlockSpec((1, 1, seg_d, d), lambda j, s: (1 - j // N_LAYER, N_LAYER - 1 - j % N_LAYER, 0, 0)),
                pl.BlockSpec((1, 1, seg_u, ff), lambda j, s: (1 - j // N_LAYER, N_LAYER - 1 - j % N_LAYER, 0, 0)),
            ],
        ),
        out_shape=[
            jax.ShapeDtypeStruct((2, N_LAYER, seg_d, d), F32),
            jax.ShapeDtypeStruct((2, N_LAYER, seg_u, ff), F32),
        ],
        compiler_params=pltpu.CompilerParams(dimension_semantics=("arbitrary",), vmem_limit_bytes=62 * 2**20),
        name="final",
    )(scal, dd, upp)


def window_table(n_data, ff):
    table = []
    for dev in range(n_data):
        place = Place(0, dev)
        row = []
        for j in range(N_GRAD):
            for i in range(4):
                row.append(Place(0, place.share(j).piece(i)).share(j).start(ff))
        table.append(row)
    return np.array(table, np.int32)


def solution(mesh):
    n_data = mesh.shape["data"]

    def device_fn(tokens_loc, targets_loc, wu, wd):
        n_micro, seq_len, d = tokens_loc.shape
        n_tok = n_data * n_micro * seq_len
        ff = wu.shape[-1]
        rows = n_micro * seq_len // N_CHUNK
        tokens = tokens_loc.reshape(N_CHUNK, rows, d)
        targets = targets_loc.reshape(N_CHUNK, rows, d)
        out = step_call(tokens, targets, wu, wd, n_tok, n_data)
        dd, upp, loss = out[1:4]
        starts = jnp.asarray(window_table(n_data, ff))
        scal = lax.dynamic_index_in_dim(starts, lax.axis_index("data"), 0, keepdims=False)
        down, up = final_call(scal, dd, upp, n_data)
        return loss[0, 0] / (2.0 * n_tok), up, down

    return jax.shard_map(
        device_fn,
        mesh=mesh,
        in_specs=(P("data"), P("data"), P(None, "stage"), P(None, "stage")),
        out_specs=(P(), P(None, "stage", "data"), P(None, "stage", "data")),
        check_vma=False,
    )
```

```python
import jax
import jax.numpy as jnp
import numpy as np
from jax import lax
from jax.experimental import pallas as pl
from jax.experimental.pallas import tpu as pltpu
from jax.sharding import PartitionSpec as P

F32, BF16 = jnp.float32, jnp.bfloat16
MESH = pl.DeviceIdType.MESH
N_CHUNK = 4
N_LAYER = 3
HALF = 2 * N_CHUNK
N_TILE = 2 * HALF * N_LAYER
N_GRAD = 2 * N_LAYER
N_SPARE = 2
N_RING = 12
LOSS_AT = (0, 6, 15, 23, 30)
SUM_AT = {0: (0, 29), 1: (1, 37), 2: (2, 42), 4: (0, 44)}
BWD_BLOCK = 256
N_STEP = 8
DELAY = 4 * N_LAYER
NT = (((1,), (1,)), ((), ()))
TN = (((0,), (0,)), ((), ()))
C0 = 0.7978845608028654
C1 = 0.044715
ANY = pl.BlockSpec(memory_space=pl.ANY)


def gelu(z):
    return z * (0.5 * (1.0 + jnp.tanh(C0 * (z + C1 * (z * z * z)))))


def gelu_and_slope(z):
    z2 = z * z
    t = jnp.tanh(C0 * (z + C1 * (z2 * z)))
    cdf = 0.5 * (1.0 + t)
    slope = cdf + (0.5 * z) * ((1.0 - t * t) * (C0 + (3.0 * C0 * C1) * z2))
    return cdf * z, slope


def sub_blocks(ff):
    step = 512
    return [(o, min(step, ff - o)) for o in range(0, ff, step)]


def grad_blocks(width):
    return [(o, min(768, width - o)) for o in range(0, width, 768)]


def window_width(ff):
    return (ff // 4 + 127) // 128 * 128


class Place:
    def __init__(self, stage, dev):
        self.stage, self.dev = stage, dev
        self.y, self.x, self.c = dev // 4, (dev // 2) % 2, dev % 2

    def flip(self, fy, fx, fc):
        return self.dev + fy * (4 - 8 * self.y) + fx * (2 - 4 * self.x) + fc * (1 - 2 * self.c)

    def gather(self, v, k):
        is_y = (v + k) % 2
        kind_c = (1 - v) * (1 - k // 2)
        one = self.flip(is_y, 1 - is_y, 0)
        two = self.flip(kind_c * (1 - is_y), kind_c * is_y, 1 - kind_c)
        return one, two

    def layer(self, j):
        return 1 - j // N_LAYER, N_LAYER - 1 - j % N_LAYER

    def group(self, v, k):
        return (1 - v) * (N_LAYER - k)

    def share(self, j):
        y, x, c = self.y, self.x, self.c
        v, k = self.layer(j)
        kc = j // 4
        dy = (1 - kc) * ((v + k) % 2)
        dx = (1 - kc) * (1 - (v + k) % 2)
        sh = Share()
        sh.kc = kc
        sh.p = (dy + kc) * y + dx * c
        sh.q = dy * c + (dx + kc) * x
        sh.wu, sh.w1, sh.w2 = 2 * dy + 4 * dx + kc, 4 * dy + 2 * dx + 4 * kc, dy + dx + 2 * kc
        sh.u = dy * x + dx * y + kc * c
        sh.r1 = dy * y + dx * x + kc * y
        sh.r2 = (dy + dx) * c + kc * x
        sh.partner = self.dev + sh.wu * (1 - 2 * sh.u)
        away = (1 - kc) * (sh.u * (1 - c) + c * (1 - sh.u))
        sh.away = away
        sh.dest_same = self.dev + away * sh.wu * (1 - 2 * sh.u)
        sh.core_peer = self.dev + (1 - 2 * c)
        return sh


class Share:
    def piece(self, i):
        r1 = self.r1 + (i // 2) * (1 - 2 * self.r1)
        r2 = self.r2 + (i % 2) * (1 - 2 * self.r2)
        return self.w1 * r1 + self.w2 * r2 + self.wu * self.u

    def start(self, ff):
        return (ff // 2) * self.p + (ff // 2 - window_width(ff)) * self.q

    def base(self, ff):
        return (ff // 4 - (ff // 2 - window_width(ff))) * self.q


def layer_of(s):
    e = s // N_LAYER
    r = s - N_LAYER * e
    back = e // HALF
    return e, r + back * (N_LAYER - 1 - 2 * r)


def block_of(e):
    back = e // HALF
    first = (e - HALF * back) // N_CHUNK
    return first + back * (1 - 2 * first)


def step_kernel(n_tok, tokens, targets, wu, wd, hg, dd, upp, loss_ref, sup, kup, ub, sd, rb, zs, zin, lbuf, sems):
    place = Place(lax.axis_index("stage"), lax.axis_index("data"))
    stage, dev, c = place.stage, place.dev, place.c
    d, ff = wu.shape[2:]
    rows = zin.shape[1]
    tile = (rows, d)

    def remote(src, dst, send, recv, to):
        return pltpu.make_async_remote_copy(src, dst, send, recv, to, MESH)

    def at(index):
        return (stage, index)

    z_peer = (1 - stage, dev)
    local_peers = [place.flip(*f) for f in ((0, 0, 1), (0, 1, 0), (1, 0, 0), (0, 1, 1), (1, 0, 1), (1, 1, 0))]

    @pl.when(stage == 0)
    def _():
        for m in range(N_CHUNK):
            pltpu.make_async_copy(tokens.at[m], zin.at[m], sems.z_recv.at[m]).start()

    barrier = pltpu.get_barrier_semaphore()
    for peer in [z_peer] + [at(i) for i in local_peers]:
        pl.semaphore_signal(barrier, inc=1, device_id=peer, device_id_type=MESH)
    pl.semaphore_wait(barrier, 1 + len(local_peers))

    def a_copy(s):
        e, l = layer_of(s)
        one, _ = place.gather(block_of(e), l)
        return remote(hg.at[0, e, l], hg.at[1, e, l], sems.a_send, sems.a_recv.at[s], at(one))

    def c_copy(s):
        e, l = layer_of(s)
        v = block_of(e)
        _, two = place.gather(v, l)
        return remote(hg.at[0, e, l], hg.at[2, e, l], sems.c_send, sems.c_recv.at[place.group(v, l)], at(two))

    def forward(s):
        e, l = layer_of(s)
        v = block_of(e)
        _, two = place.gather(v, l)
        a_copy(s).wait_recv()
        remote(hg.at[1, e, l], hg.at[3, e, l], sems.f_send, sems.f_recv.at[place.group(v, l)], at(two)).start()

    def chain(wub, wdb, ring, zout, zb, tgt, acc, loss_row):
        subs = sub_blocks(ff)
        n_sub = len(subs)
        n_ring = n_sub + N_SPARE
        assert n_ring <= N_RING

        def weight_copies(v, l):
            return (
                pltpu.make_async_copy(wu.at[v, l], wub.at[l], sems.w.at[l, 0]),
                pltpu.make_async_copy(wd.at[v, l], wdb.at[l], sems.w.at[l, 1]),
            )

        def load_weights(v, l):
            for cp in weight_copies(v, l):
                cp.start()

        def wait_weights(l):
            for cp in weight_copies(0, l):
                cp.wait()

        def z_copy(m):
            return remote(zout, zin.at[m], sems.z_send, sems.z_recv.at[m], z_peer)

        def sent(e):
            fwd = (e < HALF) & ((stage == 0) | (e < N_CHUNK))
            return fwd | ((e >= HALF) & ((stage == 1) | (e < HALF + N_CHUNK)))

        def start_tile(s, e, l, first):
            @pl.when(first)
            def _():
                @pl.when(jnp.logical_not((stage == 1) & (e >= HALF) & (e < HALF + N_CHUNK)))
                def _():
                    z_copy(e % N_CHUNK).wait_recv()

                ring[s % 3] = zin[e % N_CHUNK]

            pltpu.make_async_copy(ring.at[s % 3], hg.at[0, e, l], sems.ld).start()

        def end_tile(s, e, l, last):
            pltpu.make_async_copy(ring.at[s % 3], hg.at[0, e, l], sems.ld).wait()
            a_copy(s).start()
            c_copy(s).start()

            @pl.when(s >= DELAY)
            def _():
                forward(s - DELAY)

            @pl.when(last & (e >= 1))
            def _():
                @pl.when(sent(e - 1))
                def _():
                    z_copy(0).wait_send()

        for l in range(N_LAYER):
            load_weights(0, l)

        def z_block(s, i, forward_pass):
            e, l = layer_of(s)
            off, w = subs[i]
            q = e if forward_pass else N_CHUNK * block_of(e) + e % N_CHUNK
            b = (n_sub * s + i) % n_ring
            return zs.at[q, l, i, :, pl.ds(0, w)], zb.at[b, :, pl.ds(0, w)], b

        def z_out(s, i):
            store, buf, b = z_block(s, i, True)
            return pltpu.make_async_copy(buf, store, sems.zo.at[b])

        def z_in(s, i):
            store, buf, b = z_block(s, i, False)
            return pltpu.make_async_copy(store, buf, sems.zi.at[b])

        loss_row[...] = jnp.zeros_like(loss_row)

        def fwd_step(s, _):
            e, l = layer_of(s)
            v, m = e // N_CHUNK, e % N_CHUNK
            top = (stage == 1) & (v == 1)
            with jax.named_scope("f_pre"):
                start_tile(s, e, l, l == 0)

                @pl.when(top & (l == 0))
                def _():
                    pltpu.make_async_copy(targets.at[m], tgt, sems.t).start()

                @pl.when(m == 0)
                def _():
                    wait_weights(l)

                @pl.when(s >= 1)
                def _():
                    for i in range(n_sub - N_SPARE):
                        z_out(s - 1, i).wait()

                @pl.when(s >= 2)
                def _():
                    for i in range(n_sub - N_SPARE, n_sub):
                        z_out(s - 2, i).wait()

            with jax.named_scope("f_mm"):
                for i, (off, w) in enumerate(subs):
                    h = ring[s % 3]
                    z = jnp.dot(h, wub[l, :, off : off + w], preferred_element_type=F32)
                    zb[(n_sub * s + i) % n_ring, :, :w] = z
                    if i:
                        z_out(s, i - 1).start()
                    a = gelu(z).astype(BF16)
                    part = jnp.dot(a, wdb[l, off : off + w, :], preferred_element_type=F32)
                    acc[...] = (h.astype(F32) if i == 0 else acc[...]) + part

            z_out(s, n_sub - 1).start()
            with jax.named_scope("f_end"):
                end_tile(s, e, l, l == N_LAYER - 1)

                @pl.when(e == N_CHUNK - 1)
                def _():
                    load_weights(1, l)

                @pl.when(l < N_LAYER - 1)
                def _():
                    ring[(s + 1) % 3] = acc[...].astype(BF16)

                @pl.when(l == N_LAYER - 1)
                def _():
                    @pl.when(top)
                    def _():
                        pltpu.make_async_copy(targets.at[m], tgt, sems.t).wait()
                        err = acc[...].astype(BF16).astype(F32) - tgt[...].astype(F32)
                        loss_row[...] += jnp.sum(err * err, axis=0, keepdims=True)
                        zin[m] = (err * (1.0 / n_tok)).astype(BF16)

                    @pl.when(jnp.logical_not(top))
                    def _():
                        zout[...] = acc[...].astype(BF16)

                    @pl.when(sent(e))
                    def _():
                        z_copy(m).start()

            return 0

        n_fwd = N_TILE // 2
        lax.fori_loop(0, n_fwd, fwd_step, 0)
        for i in range(n_sub - N_SPARE, n_sub):
            z_out(n_fwd - 2, i).wait()
        for i in range(n_sub):
            z_out(n_fwd - 1, i).wait()
        for i in range(n_sub):
            z_in(n_fwd, i).start()

        def bwd_step(s, _):
            e, l = layer_of(s)
            m = e % N_CHUNK

            with jax.named_scope("b_pre"):
                start_tile(s, e, l, l == N_LAYER - 1)
                for i in range(n_sub):
                    z_in(s, i).wait()
            after = jnp.minimum(s + 1, N_TILE - 1)

            def z_next(i):
                store, _, _ = z_block(after, i, False)
                _, buf, b = z_block(s + 1, i, False)
                pltpu.make_async_copy(store, buf, sems.zi.at[b]).start()

            for i in range(N_SPARE):
                z_next(i)

            @pl.when(e == HALF + N_CHUNK)
            def _():
                wait_weights(l)

            with jax.named_scope("b_mm"):
                for i, (off, w) in enumerate(subs):
                    for o in range(0, w, BWD_BLOCK):
                        cut = slice(off + o, off + o + BWD_BLOCK)
                        g = ring[s % 3]
                        da = lax.dot_general(g, wdb[l, cut, :], NT, preferred_element_type=F32)
                        _, slope = gelu_and_slope(zb[(n_sub * s + i) % n_ring, :, o : o + BWD_BLOCK])
                        dz = (slope * da.astype(BF16).astype(F32)).astype(BF16)
                        part = lax.dot_general(dz, wub[l, :, cut], NT, preferred_element_type=F32)
                        acc[...] = (g.astype(F32) if i + o == 0 else acc[...]) + part
                    if i + N_SPARE < n_sub:
                        z_next(i + N_SPARE)

            with jax.named_scope("b_end"):
                end_tile(s, e, l, l == 0)

                @pl.when(e == HALF + N_CHUNK - 1)
                def _():
                    load_weights(0, l)

                @pl.when(l > 0)
                def _():
                    ring[(s + 1) % 3] = acc[...].astype(BF16)

                @pl.when(l == 0)
                def _():
                    zout[...] = acc[...].astype(BF16)

                    @pl.when(sent(e))
                    def _():
                        z_copy(m).start()

            return 0

        lax.fori_loop(n_fwd, N_TILE, bwd_step, 0)
        for i in range(n_sub):
            store, _, _ = z_block(N_TILE - 1, i, False)
            _, buf, b = z_block(N_TILE, i, False)
            pltpu.make_async_copy(store, buf, sems.zi.at[b]).wait()

        @pl.when(sent(2 * HALF - 1))
        def _():
            z_copy(0).wait_send()

        loss_ref[...] = jnp.broadcast_to(jnp.sum(loss_row[...], axis=1, keepdims=True), loss_ref.shape)

    width = window_width(ff)
    seg_d, seg_u = dd.shape[2], upp.shape[2]

    def grads(wub, wdb, hb, gb, gd, gu, cb, ubb):
        def weight_copies(j):
            v, k = place.layer(j)
            start = pl.multiple_of(place.share(j).start(ff), 128)
            b = j % 2
            return (
                pltpu.make_async_copy(wu.at[v, k, :, pl.ds(start, width)], wub.at[b], sems.ww.at[b, 0]),
                pltpu.make_async_copy(wd.at[v, k, pl.ds(start, width), :], wdb.at[b], sems.ww.at[b, 1]),
            )

        def fetches(n):
            v, k = place.layer(n // N_STEP)
            t = n % N_STEP
            m, part = t // 2, 2 * (t % 2)
            h_at = N_CHUNK * v + part
            g_at = HALF + N_CHUNK * (1 - v) + part
            b = n % 2
            return (
                pltpu.make_async_copy(hg.at[m, pl.ds(h_at, 2), k], hb.at[b], sems.hb.at[b]),
                pltpu.make_async_copy(hg.at[m, pl.ds(g_at, 2), k], gb.at[b], sems.gb.at[b]),
            )

        def arrived(group):
            ref = hg.at[2, pl.ds(0, HALF), 0] if group else hg.at[2, pl.ds(0, HALF)]
            remote(ref, ref, sems.c_send, sems.c_recv.at[group], z_peer).wait_recv()
            remote(ref, ref, sems.f_send, sems.f_recv.at[group], z_peer).wait_recv()

        def stage_copies(j):
            sh = place.share(j)
            b = j % 2
            up = []
            for i in range(4):
                keep = sh.piece(i)
                send = keep + sh.wu * (1 - 2 * sh.u)
                for to, row, sem in ((sup, send, 0), (kup, keep, 1)):
                    src = gu.at[b, pl.ds(pl.multiple_of(row * seg_u, 8), seg_u), :]
                    up.append(pltpu.make_async_copy(src, to.at[j, i], sems.st.at[sem]))
            base = sh.base(ff)
            part = [gd.at[b, pl.ds(pl.multiple_of(base + seg_d * i, 8), seg_d), :] for i in (c, 1 - c)]
            same = [pltpu.make_async_copy(part[0], to.at[j, 0], sems.st.at[2]) for to in (dd, sd)]
            other = pltpu.make_async_copy(part[1], sd.at[j, 1], sems.st.at[3])
            return sh, up, same, other

        def stage_out(j):
            sh, up, same, other = stage_copies(j)
            for cp in up:
                cp.start()
            other.start()
            pl.when(sh.away == 0)(same[0].start)
            pl.when(sh.away == 1)(same[1].start)

        def down_same(j, sh):
            return remote(sd.at[j, 0], dd.at[j, 1], sems.ds_send, sems.d_recv.at[j, 1], at(sh.dest_same))

        def up_exchange(j, sh):
            return remote(sup.at[j], ub.at[j], sems.u_send, sems.u_recv.at[j], at(sh.partner))

        def send_out(j):
            sh = place.share(j)
            pltpu.make_async_copy(sup.at[j], sup.at[j], sems.st.at[0]).wait()
            up_exchange(j, sh).start()
            pltpu.make_async_copy(sd.at[j, 1], sd.at[j, 1], sems.st.at[3]).wait()
            pltpu.make_async_copy(sd.at[j, 0], sd.at[j, 0], sems.st.at[2]).wait()

            @pl.when(sh.away == 0)
            def _():
                slot = sh.kc
                remote(
                    sd.at[j, 1], dd.at[j, slot], sems.d_send, sems.d_recv.at[j, slot], at(sh.core_peer)
                ).start()

            @pl.when(sh.away == 1)
            def _():
                remote(sd.at[j, 1], rb.at[j], sems.d_send, sems.r_recv.at[j], at(sh.core_peer)).start()
                down_same(j, sh).start()

            pltpu.make_async_copy(kup.at[j], kup.at[j], sems.st.at[1]).wait()

        def relay(j):
            sh = place.share(j)

            @pl.when((sh.away == 0) & (sh.kc == 0))
            def _():
                cp = remote(rb.at[j], rb.at[j], sems.r_send, sems.r_recv.at[j], z_peer)
                cp.wait_recv()
                remote(rb.at[j], dd.at[j, 1], sems.r_send, sems.d_recv.at[j, 1], at(sh.partner)).start()

        def tail_sends(j):
            sh = place.share(j)
            b = j % 2
            out = []
            for i in range(4):
                row = sh.piece(i) + sh.wu * (1 - 2 * sh.u)
                src = gu.at[b, pl.ds(pl.multiple_of(row * seg_u, 8), seg_u), :]
                out.append(remote(src, ub.at[j, i], sems.t_send, sems.u_recv.at[j], at(sh.partner)))
            base = sh.base(ff)
            same, other = [gd.at[b, pl.ds(pl.multiple_of(base + seg_d * i, 8), seg_d), :] for i in (c, 1 - c)]
            out.append(remote(other, dd.at[j, 1], sems.td_send, sems.d_recv.at[j, 1], at(sh.core_peer)))
            out.append(pltpu.make_async_copy(same, dd.at[j, 0], sems.st.at[2]))
            return out

        def piece_sends(j, b):
            sh = place.share(j)
            out = [pltpu.make_async_copy(cb.at[b, 0], upp.at[j, 0], sems.p_here.at[b])]
            for i in range(1, 4):
                out.append(remote(cb.at[b, i], upp.at[j, i], sems.p_send.at[b], sems.p_recv.at[j], at(sh.piece(i))))
            return out

        def wait_pieces(j, b):
            piece_sends(j, b)[0].wait()
            ref = cb.at[b, pl.ds(1, 3)]
            remote(ref, ref, sems.p_send.at[b], sems.p_recv.at[j], z_peer).wait_send()

        def sum_loads(j, b):
            return (
                pltpu.make_async_copy(kup.at[j], cb.at[b], sems.cl.at[0]),
                pltpu.make_async_copy(ub.at[j], ubb, sems.cl.at[1]),
            )

        def sum_load(j, b):
            up_exchange(j, place.share(j)).wait_recv()
            for cp in sum_loads(j, b):
                cp.start()

        def sum_add(j, b):
            for cp in sum_loads(j, b):
                cp.wait()
            cb[b] += ubb[...]
            for cp in piece_sends(j, b):
                cp.start()

        for cp in weight_copies(0) + fetches(0):
            cp.start()

        loss_peers = [at(place.flip(0, 0, 1)), at(place.flip(0, 1, 0)), at(place.flip(1, 0, 0)), z_peer]

        def loss_copy(r):
            return remote(lbuf.at[0, r], lbuf.at[1, r], sems.l_send, sems.l_recv.at[r], loss_peers[r])

        def step(n, _):
            j, t = n // N_STEP, n % N_STEP
            b, jb = n % 2, j % 2

            with jax.named_scope("w_fwd"):
                @pl.when(n < DELAY)
                def _():
                    forward(n + N_TILE - DELAY)

            with jax.named_scope("w_arr"):
                for group, first in enumerate((0, 3, 4, 5)):
                    pl.when(n == first * N_STEP + 3)(lambda group=group: arrived(group))

            @pl.when(n + 1 < N_GRAD * N_STEP)
            def _():
                for cp in fetches(n + 1):
                    cp.start()

            with jax.named_scope("w_pre"):
                for r in range(5):

                    @pl.when(n == LOSS_AT[r])
                    def _():
                        if r:
                            loss_copy(r - 1).wait()
                            loss_ref[...] += lbuf[1, r - 1]
                        if r < 4:
                            lbuf[0, r] = loss_ref[...]

                    if r < 4:

                        @pl.when(n == LOSS_AT[r] + 1)
                        def _():
                            loss_copy(r).start()

                @pl.when(t == 0)
                def _():
                    for cp in weight_copies(j):
                        cp.wait()

                @pl.when((t == 1) & (j + 1 < N_GRAD))
                def _():
                    for cp in weight_copies(j + 1):
                        cp.start()

                @pl.when((t == 0) & (j >= 1))
                def _():
                    stage_out(j - 1)

                @pl.when((t == 1) & (j >= 1))
                def _():
                    send_out(j - 1)

                @pl.when((t == 2) & (j >= 1) & (j < 5))
                def _():
                    relay(j - 1)

            with jax.named_scope("w_sum"):
                for i, (b_, when) in SUM_AT.items():

                    @pl.when(n == when)
                    def _():
                        if i == 4:
                            wait_pieces(0, 0)
                        sum_load(i, b_)

                    @pl.when(n == when + 1)
                    def _():
                        sum_add(i, b_)

            with jax.named_scope("w_fetch"):
                for cp in fetches(n):
                    cp.wait()
            h = hb[b].reshape(2 * rows, d)
            g = gb[b].reshape(2 * rows, d)
            with jax.named_scope("w_mm"):
                for off, w in grad_blocks(width):
                    cut = slice(off, off + w)
                    z = jnp.dot(h, wub[jb, :, cut], preferred_element_type=F32)
                    da = lax.dot_general(g, wdb[jb, cut, :], NT, preferred_element_type=F32).astype(BF16).astype(F32)
                    a, slope = gelu_and_slope(z)
                    a = a.astype(BF16)
                    dz = (slope * da).astype(BF16)
                    down = lax.dot_general(a, g, TN, preferred_element_type=F32)
                    gd[jb, cut, :] = jnp.where(t == 0, 0.0, gd[jb, cut, :]) + down
                    up = lax.dot_general(h, dz, TN, preferred_element_type=F32)
                    gu[jb, :, cut] = jnp.where(t == 0, 0.0, gu[jb, :, cut]) + up
            return 0

        lax.fori_loop(0, N_GRAD * N_STEP, step, 0)
        with jax.named_scope("t_stage"):
            last = N_GRAD - 1
            for cp in tail_sends(last):
                cp.start()
        with jax.named_scope("t_sum5"):
            wait_pieces(2, 2)
            up_exchange(last, place.share(last)).wait_recv()
            load = sum_loads(last, 2)[1]
            load.start()
            load.wait()
            for i in range(4):
                row = pl.multiple_of(place.share(last).piece(i) * seg_u, 8)
                cb[2, i] = gu[last % 2, pl.ds(row, seg_u), :] + ubb[i]
            for cp in piece_sends(last, 2):
                cp.start()
        with jax.named_scope("t_sum3"):
            wait_pieces(1, 1)
            sum_load(3, 1)
            sum_add(3, 1)
        with jax.named_scope("t_pieces"):
            for j, b in ((4, 0), (5, 2), (3, 1)):
                wait_pieces(j, b)
            tail_sends(last)[-1].wait()
            remote(ub.at[last], ub.at[last], sems.t_send, sems.u_recv.at[last], z_peer).wait_send()
            tail_sends(last)[4].wait_send()

    pl.run_scoped(
        chain,
        pltpu.VMEM((N_LAYER, d, ff), BF16),
        pltpu.VMEM((N_LAYER, ff, d), BF16),
        pltpu.VMEM((3, *tile), BF16),
        pltpu.VMEM(tile, BF16),
        pltpu.VMEM((len(sub_blocks(ff)) + N_SPARE, rows, sub_blocks(ff)[0][1]), F32),
        pltpu.VMEM(tile, BF16),
        pltpu.VMEM(tile, F32),
        pltpu.VMEM((1, d), F32),
    )
    pl.run_scoped(
        grads,
        pltpu.VMEM((2, d, width), BF16),
        pltpu.VMEM((2, width, d), BF16),
        pltpu.VMEM((2, 2, *tile), BF16),
        pltpu.VMEM((2, 2, *tile), BF16),
        pltpu.VMEM((2, width, d), F32),
        pltpu.VMEM((2, d, width), F32),
        pltpu.VMEM((3, 4, seg_u, width), F32),
        pltpu.VMEM((4, seg_u, width), F32),
    )

    with jax.named_scope("t_all"):
        for j in range(N_GRAD):
            sh = place.share(j)
            ref = upp.at[j, pl.ds(1, 3)]
            remote(ref, ref, sems.p_send.at[0], sems.p_recv.at[j], z_peer).wait_recv()
            ref = dd.at[j, 0]
            remote(ref, ref, sems.d_send, sems.d_recv.at[j, 1], z_peer).wait_recv()

            @pl.when(sh.away == 1)
            def _():
                remote(ref, ref, sems.ds_send, sems.d_recv.at[j, 0], z_peer).wait()

            @pl.when((sh.away == 0) & (sh.kc == 0))
            def _():
                remote(ref, ref, sems.r_send, sems.d_recv.at[j, 0], z_peer).wait_send()

        ref = sup.at[pl.ds(0, N_GRAD - 1)]
        remote(ref, ref, sems.u_send, sems.u_recv.at[0], z_peer).wait_send()
        ref = sd.at[pl.ds(0, N_GRAD - 1), 1]
        remote(ref, ref, sems.d_send, sems.d_recv.at[0, 0], z_peer).wait_send()
        for sem in (sems.a_send, sems.c_send, sems.f_send):
            remote(hg.at[0], hg.at[0], sem, sems.a_recv.at[0], z_peer).wait_send()


SEMS = {
    "w": (N_LAYER, 2),
    "ld": (),
    "zo": (N_RING,),
    "zi": (N_RING,),
    "t": (),
    "z_send": (),
    "z_recv": (N_CHUNK,),
    "a_send": (),
    "a_recv": (N_TILE,),
    "c_send": (),
    "c_recv": (4,),
    "f_send": (),
    "f_recv": (4,),
    "ww": (2, 2),
    "hb": (2,),
    "gb": (2,),
    "st": (4,),
    "u_send": (),
    "u_recv": (N_GRAD,),
    "d_send": (),
    "ds_send": (),
    "d_recv": (N_GRAD, 2),
    "r_send": (),
    "t_send": (),
    "td_send": (),
    "r_recv": (N_GRAD,),
    "cl": (2,),
    "p_send": (3,),
    "p_here": (3,),
    "p_recv": (N_GRAD,),
    "l_send": (),
    "l_recv": (4,),
}


class Sems:
    def __init__(self, refs):
        for name, ref in zip(SEMS, refs, strict=True):
            setattr(self, name, ref)


def step_call(tokens, targets, wu, wd, n_tok, n_data):
    n_chunk, rows, d = tokens.shape
    ff = wu.shape[-1]
    width = window_width(ff)
    pieces = jax.ShapeDtypeStruct((N_GRAD, 4, d // n_data, width), F32)
    parts = jax.ShapeDtypeStruct((N_GRAD, 2, ff // n_data, d), F32)

    def body(*refs):
        n = 14 + 2
        step_kernel(n_tok, *refs[:n], Sems(refs[n:]))

    return pl.pallas_call(
        body,
        in_specs=[ANY] * 4,
        out_specs=[ANY] * 3 + [pl.BlockSpec(memory_space=pltpu.VMEM)] + [ANY] * 6,
        out_shape=[
            jax.ShapeDtypeStruct((4, 2 * HALF, N_LAYER, rows, d), BF16),
            parts,
            pieces,
            jax.ShapeDtypeStruct((8, 128), F32),
            pieces,
            pieces,
            pieces,
            parts,
            jax.ShapeDtypeStruct((N_GRAD, ff // n_data, d), F32),
            jax.ShapeDtypeStruct((HALF, N_LAYER, len(sub_blocks(ff)), rows, sub_blocks(ff)[0][1]), F32),
        ],
        scratch_shapes=[
            pltpu.VMEM((n_chunk, rows, d), BF16),
            pltpu.VMEM((2, 4, 8, 128), F32),
            *[pltpu.SemaphoreType.DMA(shape) for shape in SEMS.values()],
        ],
        compiler_params=pltpu.CompilerParams(collective_id=0, has_side_effects=True, vmem_limit_bytes=67043328),
        name="step",
    )(tokens, targets, wu, wd)


def final_kernel(scal, dd, upp, down_ref, up_ref):
    down_ref[0, 0] = dd[0, 0] + dd[0, 1]
    width = upp.shape[-1]
    for i in range(4):
        start = pl.multiple_of(scal[4 * pl.program_id(0) + i], 128)
        up_ref[0, 0, :, pl.ds(start, width)] = upp[0, i]


def final_call(scal, dd, upp, n_data):
    seg_d, d = dd.shape[2:]
    seg_u, width = upp.shape[2:]
    ff = seg_d * n_data
    return pl.pallas_call(
        final_kernel,
        grid_spec=pltpu.PrefetchScalarGridSpec(
            num_scalar_prefetch=1,
            grid=(N_GRAD,),
            in_specs=[
                pl.BlockSpec((1, 2, seg_d, d), lambda j, s: (j, 0, 0, 0)),
                pl.BlockSpec((1, 4, seg_u, width), lambda j, s: (j, 0, 0, 0)),
            ],
            out_specs=[
                pl.BlockSpec((1, 1, seg_d, d), lambda j, s: (1 - j // N_LAYER, N_LAYER - 1 - j % N_LAYER, 0, 0)),
                pl.BlockSpec((1, 1, seg_u, ff), lambda j, s: (1 - j // N_LAYER, N_LAYER - 1 - j % N_LAYER, 0, 0)),
            ],
        ),
        out_shape=[
            jax.ShapeDtypeStruct((2, N_LAYER, seg_d, d), F32),
            jax.ShapeDtypeStruct((2, N_LAYER, seg_u, ff), F32),
        ],
        compiler_params=pltpu.CompilerParams(dimension_semantics=("arbitrary",), vmem_limit_bytes=62 * 2**20),
        name="final",
    )(scal, dd, upp)


def window_table(n_data, ff):
    table = []
    for dev in range(n_data):
        place = Place(0, dev)
        row = []
        for j in range(N_GRAD):
            for i in range(4):
                row.append(Place(0, place.share(j).piece(i)).share(j).start(ff))
        table.append(row)
    return np.array(table, np.int32)


def solution(mesh):
    n_data = mesh.shape["data"]

    def device_fn(tokens_loc, targets_loc, wu, wd):
        n_micro, seq_len, d = tokens_loc.shape
        n_tok = n_data * n_micro * seq_len
        ff = wu.shape[-1]
        rows = n_micro * seq_len // N_CHUNK
        tokens = tokens_loc.reshape(N_CHUNK, rows, d)
        targets = targets_loc.reshape(N_CHUNK, rows, d)
        out = step_call(tokens, targets, wu, wd, n_tok, n_data)
        dd, upp, loss = out[1:4]
        starts = jnp.asarray(window_table(n_data, ff))
        scal = lax.dynamic_index_in_dim(starts, lax.axis_index("data"), 0, keepdims=False)
        down, up = final_call(scal, dd, upp, n_data)
        return loss[0, 0] / (2.0 * n_tok), up, down

    return jax.shard_map(
        device_fn,
        mesh=mesh,
        in_specs=(P("data"), P("data"), P(None, "stage"), P(None, "stage")),
        out_specs=(P(), P(None, "stage", "data"), P(None, "stage", "data")),
        check_vma=False,
    )
```

```python
import jax
import jax.numpy as jnp
import numpy as np
from jax import lax
from jax.experimental import pallas as pl
from jax.experimental.pallas import tpu as pltpu
from jax.sharding import PartitionSpec as P

F32, BF16 = jnp.float32, jnp.bfloat16
MESH = pl.DeviceIdType.MESH
N_CHUNK = 4
N_LAYER = 3
HALF = 2 * N_CHUNK
N_TILE = 2 * HALF * N_LAYER
N_GRAD = 2 * N_LAYER
N_SPARE = 2
N_RING = 12
LOSS_AT = (0, 6, 15, 23, 30)
SUM_AT = {0: (0, 29), 3: (1, 35), 1: (2, 37), 2: (0, 42), 4: (1, 44)}
BWD_BLOCK = 256
N_STEP = 8
DELAY = 4 * N_LAYER
NT = (((1,), (1,)), ((), ()))
TN = (((0,), (0,)), ((), ()))
C0 = 0.7978845608028654
C1 = 0.044715
ANY = pl.BlockSpec(memory_space=pl.ANY)


def gelu(z):
    return z * (0.5 * (1.0 + jnp.tanh(C0 * (z + C1 * (z * z * z)))))


def gelu_and_slope(z):
    z2 = z * z
    t = jnp.tanh(C0 * (z + C1 * (z2 * z)))
    cdf = 0.5 * (1.0 + t)
    slope = cdf + (0.5 * z) * ((1.0 - t * t) * (C0 + (3.0 * C0 * C1) * z2))
    return cdf * z, slope


def sub_blocks(ff):
    step = 512
    return [(o, min(step, ff - o)) for o in range(0, ff, step)]


def grad_blocks(width):
    return [(o, min(768, width - o)) for o in range(0, width, 768)]


def window_width(ff):
    return (ff // 4 + 127) // 128 * 128


class Place:
    def __init__(self, stage, dev):
        self.stage, self.dev = stage, dev
        self.y, self.x, self.c = dev // 4, (dev // 2) % 2, dev % 2

    def flip(self, fy, fx, fc):
        return self.dev + fy * (4 - 8 * self.y) + fx * (2 - 4 * self.x) + fc * (1 - 2 * self.c)

    def gather(self, v, k, m):
        kind_c = 1 - v
        is_y = v * ((1 + k) % 2) + kind_c * (k % 2) * (m % 2)
        one = self.flip(is_y, 1 - is_y, 0)
        two = self.flip(kind_c * (1 - is_y), kind_c * is_y, 1 - kind_c)
        return one, two

    def layer(self, j):
        return 1 - j // N_LAYER, N_LAYER - 1 - j % N_LAYER

    def group(self, v, k):
        return (1 - v) * (N_LAYER - k)

    def share(self, j):
        y, x, c = self.y, self.x, self.c
        v, k = self.layer(j)
        kc = j // N_LAYER
        dy = (1 - kc) * ((v + k) % 2)
        dx = (1 - kc) * (1 - (v + k) % 2)
        sh = Share()
        sh.kc = kc
        sh.p = (dy + kc) * y + dx * c
        sh.q = dy * c + (dx + kc) * x
        sh.wu, sh.w1, sh.w2 = 2 * dy + 4 * dx + kc, 4 * dy + 2 * dx + 4 * kc, dy + dx + 2 * kc
        sh.u = dy * x + dx * y + kc * c
        sh.r1 = dy * y + dx * x + kc * y
        sh.r2 = (dy + dx) * c + kc * x
        sh.partner = self.dev + sh.wu * (1 - 2 * sh.u)
        away = (1 - kc) * (sh.u * (1 - c) + c * (1 - sh.u))
        sh.away = away
        sh.dest_same = self.dev + away * sh.wu * (1 - 2 * sh.u)
        sh.core_peer = self.dev + (1 - 2 * c)
        return sh


class Share:
    def piece(self, i):
        r1 = self.r1 + (i // 2) * (1 - 2 * self.r1)
        r2 = self.r2 + (i % 2) * (1 - 2 * self.r2)
        return self.w1 * r1 + self.w2 * r2 + self.wu * self.u

    def start(self, ff):
        return (ff // 2) * self.p + (ff // 2 - window_width(ff)) * self.q

    def base(self, ff):
        return (ff // 4 - (ff // 2 - window_width(ff))) * self.q


def layer_of(s):
    e = s // N_LAYER
    r = s - N_LAYER * e
    back = e // HALF
    return e, r + back * (N_LAYER - 1 - 2 * r)


def block_of(e):
    back = e // HALF
    first = (e - HALF * back) // N_CHUNK
    return first + back * (1 - 2 * first)


def step_kernel(n_tok, tokens, targets, wu, wd, hg, dd, upp, loss_ref, sup, kup, ub, sd, rb, zs, zin, lbuf, sems):
    place = Place(lax.axis_index("stage"), lax.axis_index("data"))
    stage, dev, c = place.stage, place.dev, place.c
    d, ff = wu.shape[2:]
    rows = zin.shape[1]
    tile = (rows, d)

    def remote(src, dst, send, recv, to):
        return pltpu.make_async_remote_copy(src, dst, send, recv, to, MESH)

    def at(index):
        return (stage, index)

    z_peer = (1 - stage, dev)
    local_peers = [place.flip(i // 4, i // 2 % 2, i % 2) for i in range(1, 7)]

    @pl.when(stage == 0)
    def _():
        for m in range(N_CHUNK):
            pltpu.make_async_copy(tokens.at[m], zin.at[m], sems.z_recv.at[m]).start()

    barrier = pltpu.get_barrier_semaphore()
    for peer in [z_peer] + [at(i) for i in local_peers]:
        pl.semaphore_signal(barrier, inc=1, device_id=peer, device_id_type=MESH)
    pl.semaphore_wait(barrier, 1 + len(local_peers))

    def a_copy(s):
        e, l = layer_of(s)
        one, _ = place.gather(block_of(e), l, e % N_CHUNK)
        return remote(hg.at[0, e, l], hg.at[1, e, l], sems.a_send, sems.a_recv.at[s], at(one))

    def c_copy(s):
        e, l = layer_of(s)
        v = block_of(e)
        _, two = place.gather(v, l, e % N_CHUNK)
        return remote(hg.at[0, e, l], hg.at[2, e, l], sems.c_send, sems.c_recv.at[place.group(v, l)], at(two))

    def forward(s):
        e, l = layer_of(s)
        v = block_of(e)
        _, two = place.gather(v, l, e % N_CHUNK)
        a_copy(s).wait_recv()
        remote(hg.at[1, e, l], hg.at[3, e, l], sems.f_send, sems.f_recv.at[place.group(v, l)], at(two)).start()

    def chain(wub, wdb, ring, zout, zb, tgt, acc, loss_row):
        subs = sub_blocks(ff)
        n_sub = len(subs)
        n_ring = n_sub + N_SPARE
        assert n_ring <= N_RING

        def weight_copies(v, l):
            return (
                pltpu.make_async_copy(wu.at[v, l], wub.at[l], sems.w.at[l, 0]),
                pltpu.make_async_copy(wd.at[v, l], wdb.at[l], sems.w.at[l, 1]),
            )

        def load_weights(v, l):
            for cp in weight_copies(v, l):
                cp.start()

        def wait_weights(l):
            for cp in weight_copies(0, l):
                cp.wait()

        def z_copy(m):
            return remote(zout, zin.at[m], sems.z_send, sems.z_recv.at[m], z_peer)

        def sent(e):
            fwd = (e < HALF) & ((stage == 0) | (e < N_CHUNK))
            return fwd | ((e >= HALF) & ((stage == 1) | (e < HALF + N_CHUNK)))

        def start_tile(s, e, l, first):
            @pl.when(first)
            def _():
                @pl.when(jnp.logical_not((stage == 1) & (e >= HALF) & (e < HALF + N_CHUNK)))
                def _():
                    z_copy(e % N_CHUNK).wait_recv()

                ring[s % 3] = zin[e % N_CHUNK]

            pltpu.make_async_copy(ring.at[s % 3], hg.at[0, e, l], sems.ld).start()

        def end_tile(s, e, l, last):
            pltpu.make_async_copy(ring.at[s % 3], hg.at[0, e, l], sems.ld).wait()
            a_copy(s).start()
            c_copy(s).start()

            @pl.when(s >= DELAY)
            def _():
                forward(s - DELAY)

            @pl.when(last & (e >= 1))
            def _():
                @pl.when(sent(e - 1))
                def _():
                    z_copy(0).wait_send()

        for l in range(N_LAYER):
            load_weights(0, l)

        def z_block(s, i, forward_pass):
            e, l = layer_of(s)
            off, w = subs[i]
            q = e if forward_pass else N_CHUNK * block_of(e) + e % N_CHUNK
            b = (n_sub * s + i) % n_ring
            return zs.at[q, l, i, :, pl.ds(0, w)], zb.at[b, :, pl.ds(0, w)], b

        def z_out(s, i):
            store, buf, b = z_block(s, i, True)
            return pltpu.make_async_copy(buf, store, sems.zo.at[b])

        def z_in(s, i):
            store, buf, b = z_block(s, i, False)
            return pltpu.make_async_copy(store, buf, sems.zi.at[b])

        loss_row[:] = jnp.zeros_like(loss_row)

        def fwd_step(s, _):
            e, l = layer_of(s)
            v, m = e // N_CHUNK, e % N_CHUNK
            top = (stage == 1) & (v == 1)
            with jax.named_scope("f_pre"):
                start_tile(s, e, l, l == 0)

                @pl.when(top & (l == 0))
                def _():
                    pltpu.make_async_copy(targets.at[m], tgt, sems.t).start()

                @pl.when(m == 0)
                def _():
                    wait_weights(l)

                @pl.when(s >= 1)
                def _():
                    for i in range(n_sub - N_SPARE):
                        z_out(s - 1, i).wait()

                @pl.when(s >= 2)
                def _():
                    for i in range(n_sub - N_SPARE, n_sub):
                        z_out(s - 2, i).wait()

            with jax.named_scope("f_mm"):
                for i, (off, w) in enumerate(subs):
                    h = ring[s % 3]
                    z = jnp.dot(h, wub[l, :, off : off + w], preferred_element_type=F32)
                    zb[(n_sub * s + i) % n_ring, :, :w] = z
                    if i:
                        z_out(s, i - 1).start()
                    a = gelu(z).astype(BF16)
                    part = jnp.dot(a, wdb[l, off : off + w, :], preferred_element_type=F32)
                    acc[:] = (h.astype(F32) if i == 0 else acc[:]) + part

            z_out(s, n_sub - 1).start()
            with jax.named_scope("f_end"):
                end_tile(s, e, l, l == N_LAYER - 1)

                @pl.when(e == N_CHUNK - 1)
                def _():
                    load_weights(1, l)

                @pl.when(l < N_LAYER - 1)
                def _():
                    ring[(s + 1) % 3] = acc[:].astype(BF16)

                @pl.when(l == N_LAYER - 1)
                def _():
                    @pl.when(top)
                    def _():
                        pltpu.make_async_copy(targets.at[m], tgt, sems.t).wait()
                        err = acc[:].astype(BF16).astype(F32) - tgt[:].astype(F32)
                        loss_row[:] += jnp.sum(err * err, axis=0, keepdims=True)
                        zin[m] = (err * (1.0 / n_tok)).astype(BF16)

                    @pl.when(jnp.logical_not(top))
                    def _():
                        zout[:] = acc[:].astype(BF16)

                    @pl.when(sent(e))
                    def _():
                        z_copy(m).start()

            return 0

        n_fwd = N_TILE // 2
        lax.fori_loop(0, n_fwd, fwd_step, 0)
        for i in range(n_sub - N_SPARE, n_sub):
            z_out(n_fwd - 2, i).wait()
        for i in range(n_sub):
            z_out(n_fwd - 1, i).wait()
        for i in range(n_sub):
            z_in(n_fwd, i).start()

        def bwd_step(s, _):
            e, l = layer_of(s)
            m = e % N_CHUNK

            with jax.named_scope("b_pre"):
                start_tile(s, e, l, l == N_LAYER - 1)
                for i in range(n_sub):
                    z_in(s, i).wait()
            after = jnp.minimum(s + 1, N_TILE - 1)

            def z_next(i):
                store, _, _ = z_block(after, i, False)
                _, buf, b = z_block(s + 1, i, False)
                pltpu.make_async_copy(store, buf, sems.zi.at[b]).start()

            for i in range(N_SPARE):
                z_next(i)

            @pl.when(e == HALF + N_CHUNK)
            def _():
                wait_weights(l)

            with jax.named_scope("b_mm"):
                for i, (off, w) in enumerate(subs):
                    for o in range(0, w, BWD_BLOCK):
                        cut = slice(off + o, off + o + BWD_BLOCK)
                        g = ring[s % 3]
                        da = lax.dot_general(g, wdb[l, cut, :], NT, preferred_element_type=F32)
                        _, slope = gelu_and_slope(zb[(n_sub * s + i) % n_ring, :, o : o + BWD_BLOCK])
                        dz = (slope * da.astype(BF16).astype(F32)).astype(BF16)
                        part = lax.dot_general(dz, wub[l, :, cut], NT, preferred_element_type=F32)
                        acc[:] = (g.astype(F32) if i + o == 0 else acc[:]) + part
                    if i + N_SPARE < n_sub:
                        z_next(i + N_SPARE)

            with jax.named_scope("b_end"):
                end_tile(s, e, l, l == 0)

                @pl.when(e == HALF + N_CHUNK - 1)
                def _():
                    load_weights(0, l)

                @pl.when(l > 0)
                def _():
                    ring[(s + 1) % 3] = acc[:].astype(BF16)

                @pl.when(l == 0)
                def _():
                    zout[:] = acc[:].astype(BF16)

                    @pl.when(sent(e))
                    def _():
                        z_copy(m).start()

            return 0

        lax.fori_loop(n_fwd, N_TILE, bwd_step, 0)
        for i in range(n_sub):
            store, _, _ = z_block(N_TILE - 1, i, False)
            _, buf, b = z_block(N_TILE, i, False)
            pltpu.make_async_copy(store, buf, sems.zi.at[b]).wait()

        @pl.when(sent(2 * HALF - 1))
        def _():
            z_copy(0).wait_send()

        loss_ref[:] = jnp.broadcast_to(jnp.sum(loss_row[:], axis=1, keepdims=True), loss_ref.shape)

    width = window_width(ff)
    seg_d, seg_u = dd.shape[2], upp.shape[2]

    def grads(wub, wdb, hb, gb, gd, gu, cb, ubb):
        def weight_copies(j):
            v, k = place.layer(j)
            start = pl.multiple_of(place.share(j).start(ff), 128)
            b = j % 2
            return (
                pltpu.make_async_copy(wu.at[v, k, :, pl.ds(start, width)], wub.at[b], sems.ww.at[b, 0]),
                pltpu.make_async_copy(wd.at[v, k, pl.ds(start, width), :], wdb.at[b], sems.ww.at[b, 1]),
            )

        def fetches(n):
            v, k = place.layer(n // N_STEP)
            t = n % N_STEP
            m, part = t // 2, 2 * (t % 2)
            h_at = N_CHUNK * v + part
            g_at = HALF + N_CHUNK * (1 - v) + part
            b = n % 2
            return (
                pltpu.make_async_copy(hg.at[m, pl.ds(h_at, 2), k], hb.at[b], sems.hb.at[b]),
                pltpu.make_async_copy(hg.at[m, pl.ds(g_at, 2), k], gb.at[b], sems.gb.at[b]),
            )

        def arrived(group):
            ref = hg.at[2, pl.ds(0, HALF), 0] if group else hg.at[2, pl.ds(0, HALF)]
            remote(ref, ref, sems.c_send, sems.c_recv.at[group], z_peer).wait_recv()
            remote(ref, ref, sems.f_send, sems.f_recv.at[group], z_peer).wait_recv()

        def stage_copies(j):
            sh = place.share(j)
            b = j % 2
            up = []
            for i in range(4):
                keep = sh.piece(i)
                send = keep + sh.wu * (1 - 2 * sh.u)
                for to, row, sem in ((sup, send, 0), (kup, keep, 1)):
                    src = gu.at[b, pl.ds(pl.multiple_of(row * seg_u, 8), seg_u), :]
                    up.append(pltpu.make_async_copy(src, to.at[j, i], sems.st.at[sem]))
            base = sh.base(ff)
            part = [gd.at[b, pl.ds(pl.multiple_of(base + seg_d * i, 8), seg_d), :] for i in (c, 1 - c)]
            same = [pltpu.make_async_copy(part[0], to.at[j, 0], sems.st.at[2]) for to in (dd, sd)]
            other = pltpu.make_async_copy(part[1], sd.at[j, 1], sems.st.at[3])
            return sh, up, same, other

        def stage_out(j):
            sh, up, same, other = stage_copies(j)
            for cp in up:
                cp.start()
            other.start()
            pl.when(sh.away == 0)(same[0].start)
            pl.when(sh.away == 1)(same[1].start)

        def down_same(j, sh):
            return remote(sd.at[j, 0], dd.at[j, 1], sems.ds_send, sems.d_recv.at[j, 1], at(sh.dest_same))

        def up_exchange(j, sh):
            return remote(sup.at[j], ub.at[j], sems.u_send, sems.u_recv.at[j], at(sh.partner))

        def send_out(j):
            sh = place.share(j)
            pltpu.make_async_copy(sup.at[j], sup.at[j], sems.st.at[0]).wait()
            up_exchange(j, sh).start()
            pltpu.make_async_copy(sd.at[j, 1], sd.at[j, 1], sems.st.at[3]).wait()
            pltpu.make_async_copy(sd.at[j, 0], sd.at[j, 0], sems.st.at[2]).wait()

            @pl.when(sh.away == 0)
            def _():
                slot = sh.kc
                remote(
                    sd.at[j, 1], dd.at[j, slot], sems.d_send, sems.d_recv.at[j, slot], at(sh.core_peer)
                ).start()

            @pl.when(sh.away == 1)
            def _():
                remote(sd.at[j, 1], rb.at[j], sems.d_send, sems.r_recv.at[j], at(sh.core_peer)).start()
                down_same(j, sh).start()

            pltpu.make_async_copy(kup.at[j], kup.at[j], sems.st.at[1]).wait()

        def relay(j):
            sh = place.share(j)

            @pl.when((sh.away == 0) & (sh.kc == 0))
            def _():
                cp = remote(rb.at[j], rb.at[j], sems.r_send, sems.r_recv.at[j], z_peer)
                cp.wait_recv()
                remote(rb.at[j], dd.at[j, 1], sems.r_send, sems.d_recv.at[j, 1], at(sh.partner)).start()

        def tail_sends(j):
            sh = place.share(j)
            b = j % 2
            out = []
            for i in range(4):
                row = sh.piece(i) + sh.wu * (1 - 2 * sh.u)
                src = gu.at[b, pl.ds(pl.multiple_of(row * seg_u, 8), seg_u), :]
                out.append(remote(src, ub.at[j, i], sems.t_send, sems.u_recv.at[j], at(sh.partner)))
            base = sh.base(ff)
            same, other = [gd.at[b, pl.ds(pl.multiple_of(base + seg_d * i, 8), seg_d), :] for i in (c, 1 - c)]
            out.append(remote(other, dd.at[j, 1], sems.td_send, sems.d_recv.at[j, 1], at(sh.core_peer)))
            out.append(pltpu.make_async_copy(same, dd.at[j, 0], sems.st.at[2]))
            return out

        def piece_sends(j, b):
            sh = place.share(j)
            out = [pltpu.make_async_copy(cb.at[b, 0], upp.at[j, 0], sems.p_here.at[b])]
            for i in range(1, 4):
                out.append(remote(cb.at[b, i], upp.at[j, i], sems.p_send.at[b], sems.p_recv.at[j], at(sh.piece(i))))
            return out

        def wait_pieces(j, b):
            piece_sends(j, b)[0].wait()
            ref = cb.at[b, pl.ds(1, 3)]
            remote(ref, ref, sems.p_send.at[b], sems.p_recv.at[j], z_peer).wait_send()

        def sum_loads(j, b):
            return (
                pltpu.make_async_copy(kup.at[j], cb.at[b], sems.cl.at[0]),
                pltpu.make_async_copy(ub.at[j], ubb, sems.cl.at[1]),
            )

        def sum_load(j, b):
            up_exchange(j, place.share(j)).wait_recv()
            for cp in sum_loads(j, b):
                cp.start()

        def sum_add(j, b):
            for cp in sum_loads(j, b):
                cp.wait()
            cb[b] += ubb[:]
            for cp in piece_sends(j, b):
                cp.start()

        for cp in weight_copies(0) + fetches(0):
            cp.start()

        loss_peers = [at(local_peers[i]) for i in (0, 1, 3)] + [z_peer]

        def loss_copy(r):
            return remote(lbuf.at[0, r], lbuf.at[1, r], sems.l_send, sems.l_recv.at[r], loss_peers[r])

        def step(n, _):
            j, t = n // N_STEP, n % N_STEP
            b, jb = n % 2, j % 2

            with jax.named_scope("w_fwd"):
                @pl.when(n < DELAY)
                def _():
                    forward(n + N_TILE - DELAY)

            with jax.named_scope("w_arr"):
                for group, first in enumerate((0, 3, 4, 5)):
                    pl.when(n == first * N_STEP + 3)(lambda group=group: arrived(group))

            @pl.when(n + 1 < N_GRAD * N_STEP)
            def _():
                for cp in fetches(n + 1):
                    cp.start()

            with jax.named_scope("w_pre"):
                for r in range(5):

                    @pl.when(n == LOSS_AT[r])
                    def _():
                        if r:
                            loss_copy(r - 1).wait()
                            loss_ref[:] += lbuf[1, r - 1]
                        if r < 4:
                            lbuf[0, r] = loss_ref[:]

                    if r < 4:

                        @pl.when(n == LOSS_AT[r] + 1)
                        def _():
                            loss_copy(r).start()

                @pl.when(t == 0)
                def _():
                    for cp in weight_copies(j):
                        cp.wait()

                @pl.when((t == 1) & (j + 1 < N_GRAD))
                def _():
                    for cp in weight_copies(j + 1):
                        cp.start()

                @pl.when((t == 0) & (j >= 1))
                def _():
                    stage_out(j - 1)

                @pl.when((t == 1) & (j >= 1))
                def _():
                    send_out(j - 1)

                @pl.when((t == 2) & (j >= 1) & (j <= N_LAYER))
                def _():
                    relay(j - 1)

            with jax.named_scope("w_sum"):
                for i, (b_, when) in SUM_AT.items():

                    @pl.when(n == when)
                    def _():
                        if i in (2, 4):
                            wait_pieces(*{2: (0, 0), 4: (3, 1)}[i])
                        sum_load(i, b_)

                    @pl.when(n == when + 1)
                    def _():
                        sum_add(i, b_)

            with jax.named_scope("w_fetch"):
                for cp in fetches(n):
                    cp.wait()
            h = hb[b].reshape(2 * rows, d)
            g = gb[b].reshape(2 * rows, d)
            with jax.named_scope("w_mm"):
                for off, w in grad_blocks(width):
                    cut = slice(off, off + w)
                    z = jnp.dot(h, wub[jb, :, cut], preferred_element_type=F32)
                    da = lax.dot_general(g, wdb[jb, cut, :], NT, preferred_element_type=F32).astype(BF16).astype(F32)
                    a, slope = gelu_and_slope(z)
                    a = a.astype(BF16)
                    dz = (slope * da).astype(BF16)
                    down = lax.dot_general(a, g, TN, preferred_element_type=F32)
                    gd[jb, cut, :] = jnp.where(t == 0, 0.0, gd[jb, cut, :]) + down
                    up = lax.dot_general(h, dz, TN, preferred_element_type=F32)
                    gu[jb, :, cut] = jnp.where(t == 0, 0.0, gu[jb, :, cut]) + up
            return 0

        lax.fori_loop(0, N_GRAD * N_STEP, step, 0)
        with jax.named_scope("t_stage"):
            last = N_GRAD - 1
            for cp in tail_sends(last):
                cp.start()
        with jax.named_scope("t_sum5"):
            wait_pieces(1, 2)
            up_exchange(last, place.share(last)).wait_recv()
            load = sum_loads(last, 2)[1]
            load.start()
            load.wait()
            for i in range(4):
                row = pl.multiple_of(place.share(last).piece(i) * seg_u, 8)
                cb[2, i] = gu[last % 2, pl.ds(row, seg_u), :] + ubb[i]
            for cp in piece_sends(last, 2):
                cp.start()
        with jax.named_scope("t_pieces"):
            for j, b in ((2, 0), (4, 1), (last, 2)):
                wait_pieces(j, b)
            tail_sends(last)[-1].wait()
            remote(ub.at[last], ub.at[last], sems.t_send, sems.u_recv.at[last], z_peer).wait_send()
            tail_sends(last)[4].wait_send()

    pl.run_scoped(
        chain,
        pltpu.VMEM((N_LAYER, d, ff), BF16),
        pltpu.VMEM((N_LAYER, ff, d), BF16),
        pltpu.VMEM((3, *tile), BF16),
        pltpu.VMEM(tile, BF16),
        pltpu.VMEM((len(sub_blocks(ff)) + N_SPARE, rows, sub_blocks(ff)[0][1]), F32),
        pltpu.VMEM(tile, BF16),
        pltpu.VMEM(tile, F32),
        pltpu.VMEM((1, d), F32),
    )
    pl.run_scoped(
        grads,
        pltpu.VMEM((2, d, width), BF16),
        pltpu.VMEM((2, width, d), BF16),
        pltpu.VMEM((2, 2, *tile), BF16),
        pltpu.VMEM((2, 2, *tile), BF16),
        pltpu.VMEM((2, width, d), F32),
        pltpu.VMEM((2, d, width), F32),
        pltpu.VMEM((3, 4, seg_u, width), F32),
        pltpu.VMEM((4, seg_u, width), F32),
    )

    with jax.named_scope("t_all"):
        for j in range(N_GRAD):
            sh = place.share(j)
            ref = upp.at[j, pl.ds(1, 3)]
            remote(ref, ref, sems.p_send.at[0], sems.p_recv.at[j], z_peer).wait_recv()
            ref = dd.at[j, 0]
            remote(ref, ref, sems.d_send, sems.d_recv.at[j, 1], z_peer).wait_recv()

            @pl.when(sh.away == 1)
            def _():
                remote(ref, ref, sems.ds_send, sems.d_recv.at[j, 0], z_peer).wait()

            @pl.when((sh.away == 0) & (sh.kc == 0))
            def _():
                remote(ref, ref, sems.r_send, sems.d_recv.at[j, 0], z_peer).wait_send()

        ref = sup.at[pl.ds(0, N_GRAD - 1)]
        remote(ref, ref, sems.u_send, sems.u_recv.at[0], z_peer).wait_send()
        ref = sd.at[pl.ds(0, N_GRAD - 1), 1]
        remote(ref, ref, sems.d_send, sems.d_recv.at[0, 0], z_peer).wait_send()
        for sem in (sems.a_send, sems.c_send, sems.f_send):
            remote(hg.at[0], hg.at[0], sem, sems.a_recv.at[0], z_peer).wait_send()


SEMS = {
    "w": (N_LAYER, 2),
    "zo": (N_RING,),
    "zi": (N_RING,),
    "z_recv": (N_CHUNK,),
    "a_recv": (N_TILE,),
    "c_recv": (N_CHUNK,),
    "f_recv": (N_CHUNK,),
    "ww": (2, 2),
    "hb": (2,),
    "gb": (2,),
    "st": (N_CHUNK,),
    "u_recv": (N_GRAD,),
    "d_recv": (N_GRAD, 2),
    "r_recv": (N_GRAD,),
    "cl": (2,),
    "p_send": (N_LAYER,),
    "p_here": (N_LAYER,),
    "p_recv": (N_GRAD,),
    "l_recv": (N_CHUNK,),
}
SEMS |= dict.fromkeys(("ld", "t", "z_send", "a_send", "c_send", "f_send", "u_send", "d_send"), ())
SEMS |= dict.fromkeys(("ds_send", "r_send", "t_send", "td_send", "l_send"), ())


class Sems:
    def __init__(self, refs):
        for name, ref in zip(SEMS, refs, strict=True):
            setattr(self, name, ref)


def step_call(tokens, targets, wu, wd, n_tok, n_data):
    n_chunk, rows, d = tokens.shape
    ff = wu.shape[-1]
    width = window_width(ff)
    pieces = jax.ShapeDtypeStruct((N_GRAD, 4, d // n_data, width), F32)
    parts = jax.ShapeDtypeStruct((N_GRAD, 2, ff // n_data, d), F32)

    def body(*refs):
        n = 14 + 2
        step_kernel(n_tok, *refs[:n], Sems(refs[n:]))

    return pl.pallas_call(
        body,
        in_specs=[ANY] * 4,
        out_specs=[ANY] * 3 + [pl.BlockSpec(memory_space=pltpu.VMEM)] + [ANY] * 6,
        out_shape=[
            jax.ShapeDtypeStruct((4, 2 * HALF, N_LAYER, rows, d), BF16),
            parts,
            pieces,
            jax.ShapeDtypeStruct((8, 128), F32),
            pieces,
            pieces,
            pieces,
            parts,
            jax.ShapeDtypeStruct((N_GRAD, ff // n_data, d), F32),
            jax.ShapeDtypeStruct((HALF, N_LAYER, len(sub_blocks(ff)), rows, sub_blocks(ff)[0][1]), F32),
        ],
        scratch_shapes=[
            pltpu.VMEM((n_chunk, rows, d), BF16),
            pltpu.VMEM((2, 4, 8, 128), F32),
            *[pltpu.SemaphoreType.DMA(shape) for shape in SEMS.values()],
        ],
        compiler_params=pltpu.CompilerParams(collective_id=0, has_side_effects=True, vmem_limit_bytes=67043328),
        name="step",
    )(tokens, targets, wu, wd)


def final_kernel(scal, dd, upp, down_ref, up_ref):
    down_ref[0, 0] = dd[0, 0] + dd[0, 1]
    width = upp.shape[-1]
    for i in range(4):
        start = pl.multiple_of(scal[4 * pl.program_id(0) + i], 128)
        up_ref[0, 0, :, pl.ds(start, width)] = upp[0, i]


def final_call(scal, dd, upp, n_data):
    seg_d, d = dd.shape[2:]
    seg_u, width = upp.shape[2:]
    ff = seg_d * n_data
    return pl.pallas_call(
        final_kernel,
        grid_spec=pltpu.PrefetchScalarGridSpec(
            num_scalar_prefetch=1,
            grid=(N_GRAD,),
            in_specs=[
                pl.BlockSpec((1, 2, seg_d, d), lambda j, s: (j, 0, 0, 0)),
                pl.BlockSpec((1, 4, seg_u, width), lambda j, s: (j, 0, 0, 0)),
            ],
            out_specs=[
                pl.BlockSpec((1, 1, seg_d, d), lambda j, s: (1 - j // N_LAYER, N_LAYER - 1 - j % N_LAYER, 0, 0)),
                pl.BlockSpec((1, 1, seg_u, ff), lambda j, s: (1 - j // N_LAYER, N_LAYER - 1 - j % N_LAYER, 0, 0)),
            ],
        ),
        out_shape=[
            jax.ShapeDtypeStruct((2, N_LAYER, seg_d, d), F32),
            jax.ShapeDtypeStruct((2, N_LAYER, seg_u, ff), F32),
        ],
        compiler_params=pltpu.CompilerParams(dimension_semantics=("arbitrary",), vmem_limit_bytes=62 * 2**20),
        name="final",
    )(scal, dd, upp)


def window_table(n_data, ff):
    table = []
    for dev in range(n_data):
        place = Place(0, dev)
        row = []
        for j in range(N_GRAD):
            for i in range(4):
                row.append(Place(0, place.share(j).piece(i)).share(j).start(ff))
        table.append(row)
    return np.array(table, np.int32)


def solution(mesh):
    n_data = mesh.shape["data"]

    def device_fn(tokens_loc, targets_loc, wu, wd):
        n_micro, seq_len, d = tokens_loc.shape
        n_tok = n_data * n_micro * seq_len
        ff = wu.shape[-1]
        rows = n_micro * seq_len // N_CHUNK
        tokens = tokens_loc.reshape(N_CHUNK, rows, d)
        targets = targets_loc.reshape(N_CHUNK, rows, d)
        out = step_call(tokens, targets, wu, wd, n_tok, n_data)
        dd, upp, loss = out[1:4]
        starts = jnp.asarray(window_table(n_data, ff))
        scal = lax.dynamic_index_in_dim(starts, lax.axis_index("data"), 0, keepdims=False)
        down, up = final_call(scal, dd, upp, n_data)
        return loss[0, 0] / (2.0 * n_tok), up, down

    return jax.shard_map(
        device_fn,
        mesh=mesh,
        in_specs=(P("data"), P("data"), P(None, "stage"), P(None, "stage")),
        out_specs=(P(), P(None, "stage", "data"), P(None, "stage", "data")),
        check_vma=False,
    )
```

```python
import jax
import jax.numpy as jnp
import numpy as np
from jax import lax
from jax.experimental import pallas as pl
from jax.experimental.pallas import tpu as pltpu
from jax.sharding import PartitionSpec as P

F32, BF16 = jnp.float32, jnp.bfloat16
MESH = pl.DeviceIdType.MESH
N_CHUNK = 4
N_LAYER = 3
HALF = 2 * N_CHUNK
N_TILE = 2 * HALF * N_LAYER
N_GRAD = 2 * N_LAYER
N_SPARE = 2
N_RING = 12
LOSS_AT = (0, 6, 15, 23, 30)
SUM_AT = {0: (0, 29), 1: (1, 37), 2: (2, 42), 4: (0, 44)}
BWD_BLOCK = 256
N_STEP = 8
DELAY = 4 * N_LAYER
NT = (((1,), (1,)), ((), ()))
TN = (((0,), (0,)), ((), ()))
C0 = 0.7978845608028654
C1 = 0.044715
ANY = pl.BlockSpec(memory_space=pl.ANY)


def gelu(z):
    return z * (0.5 * (1.0 + jnp.tanh(C0 * (z + C1 * (z * z * z)))))


def gelu_and_slope(z):
    z2 = z * z
    t = jnp.tanh(C0 * (z + C1 * (z2 * z)))
    cdf = 0.5 * (1.0 + t)
    slope = cdf + (0.5 * z) * ((1.0 - t * t) * (C0 + (3.0 * C0 * C1) * z2))
    return cdf * z, slope


def sub_blocks(ff):
    step = 512
    return [(o, min(step, ff - o)) for o in range(0, ff, step)]


def grad_blocks(width):
    return [(o, min(768, width - o)) for o in range(0, width, 768)]


def window_width(ff):
    return (ff // 4 + 127) // 128 * 128


class Place:
    def __init__(self, stage, dev):
        self.stage, self.dev = stage, dev
        self.y, self.x, self.c = dev // 4, (dev // 2) % 2, dev % 2

    def flip(self, fy, fx, fc):
        return self.dev + fy * (4 - 8 * self.y) + fx * (2 - 4 * self.x) + fc * (1 - 2 * self.c)

    def gather(self, v, k):
        is_y = (v + k) % 2
        kind_c = (1 - v) * (1 - k // 2)
        one = self.flip(is_y, 1 - is_y, 0)
        two = self.flip(kind_c * (1 - is_y), kind_c * is_y, 1 - kind_c)
        return one, two

    def layer(self, j):
        return 1 - j // N_LAYER, N_LAYER - 1 - j % N_LAYER

    def group(self, v, k):
        return (1 - v) * (N_LAYER - k)

    def share(self, j):
        y, x, c = self.y, self.x, self.c
        v, k = self.layer(j)
        kc = j // N_CHUNK
        dy = (1 - kc) * ((v + k) % 2)
        dx = (1 - kc) * (1 - (v + k) % 2)
        sh = Share()
        sh.kc = kc
        sh.p = (dy + kc) * y + dx * c
        sh.q = dy * c + (dx + kc) * x
        sh.wu, sh.w1, sh.w2 = 2 * dy + 4 * dx + kc, 4 * dy + 2 * dx + 4 * kc, dy + dx + 2 * kc
        sh.u = dy * x + dx * y + kc * c
        sh.r1 = dy * y + dx * x + kc * y
        sh.r2 = (dy + dx) * c + kc * x
        sh.partner = self.dev + sh.wu * (1 - 2 * sh.u)
        away = (1 - kc) * (sh.u * (1 - c) + c * (1 - sh.u))
        sh.away = away
        sh.dest_same = self.dev + away * sh.wu * (1 - 2 * sh.u)
        sh.core_peer = self.dev + (1 - 2 * c)
        return sh


class Share:
    def piece(self, i):
        r1 = self.r1 + (i // 2) * (1 - 2 * self.r1)
        r2 = self.r2 + (i % 2) * (1 - 2 * self.r2)
        return self.w1 * r1 + self.w2 * r2 + self.wu * self.u

    def start(self, ff):
        return (ff // 2) * self.p + (ff // 2 - window_width(ff)) * self.q

    def base(self, ff):
        return (ff // 4 - (ff // 2 - window_width(ff))) * self.q


def layer_of(s):
    e = s // N_LAYER
    r = s - N_LAYER * e
    back = e // HALF
    return e, r + back * (N_LAYER - 1 - 2 * r)


def block_of(e):
    back = e // HALF
    first = (e - HALF * back) // N_CHUNK
    return first + back * (1 - 2 * first)


def step_kernel(n_tok, tokens, targets, wu, wd, hg, dd, upp, loss_ref, sup, kup, ub, sd, rb, zs, zin, lbuf, sems):
    place = Place(lax.axis_index("stage"), lax.axis_index("data"))
    stage, dev, c = place.stage, place.dev, place.c
    d, ff = wu.shape[2:]
    rows = zin.shape[1]
    tile = (rows, d)

    def remote(src, dst, send, recv, to):
        return pltpu.make_async_remote_copy(src, dst, send, recv, to, MESH)

    def at(index):
        return (stage, index)

    z_peer = (1 - stage, dev)
    local_peers = [place.flip(i // 4, i // 2 % 2, i % 2) for i in range(1, 7)]

    @pl.when(stage == 0)
    def _():
        for m in range(N_CHUNK):
            pltpu.make_async_copy(tokens.at[m], zin.at[m], sems.z_recv.at[m]).start()

    barrier = pltpu.get_barrier_semaphore()
    for peer in [z_peer] + [at(i) for i in local_peers]:
        pl.semaphore_signal(barrier, inc=1, device_id=peer, device_id_type=MESH)
    pl.semaphore_wait(barrier, 1 + len(local_peers))

    def a_copy(s):
        e, l = layer_of(s)
        one, _ = place.gather(block_of(e), l)
        return remote(hg.at[0, e, l], hg.at[1, e, l], sems.a_send, sems.a_recv.at[s], at(one))

    def c_copy(s):
        e, l = layer_of(s)
        v = block_of(e)
        _, two = place.gather(v, l)
        return remote(hg.at[0, e, l], hg.at[2, e, l], sems.c_send, sems.c_recv.at[place.group(v, l)], at(two))

    def forward(s):
        e, l = layer_of(s)
        v = block_of(e)
        _, two = place.gather(v, l)
        a_copy(s).wait_recv()
        remote(hg.at[1, e, l], hg.at[3, e, l], sems.f_send, sems.f_recv.at[place.group(v, l)], at(two)).start()

    def chain(wub, wdb, ring, zout, zb, tgt, acc, loss_row):
        subs = sub_blocks(ff)
        n_sub = len(subs)
        n_ring = n_sub + N_SPARE
        assert n_ring <= N_RING

        def weight_copies(v, l):
            return (
                pltpu.make_async_copy(wu.at[v, l], wub.at[l], sems.w.at[l, 0]),
                pltpu.make_async_copy(wd.at[v, l], wdb.at[l], sems.w.at[l, 1]),
            )

        def load_weights(v, l):
            for cp in weight_copies(v, l):
                cp.start()

        def wait_weights(l):
            for cp in weight_copies(0, l):
                cp.wait()

        def z_copy(m):
            return remote(zout, zin.at[m], sems.z_send, sems.z_recv.at[m], z_peer)

        def sent(e):
            fwd = (e < HALF) & ((stage == 0) | (e < N_CHUNK))
            return fwd | ((e >= HALF) & ((stage == 1) | (e < HALF + N_CHUNK)))

        def start_tile(s, e, l, first):
            @pl.when(first)
            def _():
                @pl.when(jnp.logical_not((stage == 1) & (e >= HALF) & (e < HALF + N_CHUNK)))
                def _():
                    z_copy(e % N_CHUNK).wait_recv()

                ring[s % 3] = zin[e % N_CHUNK]

            pltpu.make_async_copy(ring.at[s % 3], hg.at[0, e, l], sems.ld).start()

        def end_tile(s, e, l, last):
            pltpu.make_async_copy(ring.at[s % 3], hg.at[0, e, l], sems.ld).wait()
            a_copy(s).start()
            c_copy(s).start()

            @pl.when(s >= DELAY)
            def _():
                forward(s - DELAY)

            @pl.when(last & (e >= 1))
            def _():
                @pl.when(sent(e - 1))
                def _():
                    z_copy(0).wait_send()

        for l in range(N_LAYER):
            load_weights(0, l)

        def z_block(s, i, forward_pass):
            e, l = layer_of(s)
            off, w = subs[i]
            q = e if forward_pass else N_CHUNK * block_of(e) + e % N_CHUNK
            b = (n_sub * s + i) % n_ring
            return zs.at[q, l, :, pl.ds(off, w)], zb.at[b, :, pl.ds(0, w)], b

        def z_out(s, i):
            store, buf, b = z_block(s, i, True)
            return pltpu.make_async_copy(buf, store, sems.zo.at[b])

        def z_in(s, i):
            store, buf, b = z_block(s, i, False)
            return pltpu.make_async_copy(store, buf, sems.zi.at[b])

        loss_row[:] = jnp.zeros_like(loss_row)

        def fwd_step(s, _):
            e, l = layer_of(s)
            v, m = e // N_CHUNK, e % N_CHUNK
            top = (stage == 1) & (v == 1)
            with jax.named_scope("f_pre"):
                start_tile(s, e, l, l == 0)

                @pl.when(top & (l == 0))
                def _():
                    pltpu.make_async_copy(targets.at[m], tgt, sems.t).start()

                @pl.when(m == 0)
                def _():
                    wait_weights(l)

                @pl.when(s >= 1)
                def _():
                    for i in range(n_sub - N_SPARE):
                        z_out(s - 1, i).wait()

                @pl.when(s >= 2)
                def _():
                    for i in range(n_sub - N_SPARE, n_sub):
                        z_out(s - 2, i).wait()

            with jax.named_scope("f_mm"):
                for i, (off, w) in enumerate(subs):
                    h = ring[s % 3]
                    z = jnp.dot(h, wub[l, :, off : off + w], preferred_element_type=F32)
                    zb[(n_sub * s + i) % n_ring, :, :w] = z
                    if i:
                        z_out(s, i - 1).start()
                    a = gelu(z).astype(BF16)
                    part = jnp.dot(a, wdb[l, off : off + w, :], preferred_element_type=F32)
                    acc[:] = (h.astype(F32) if i == 0 else acc[:]) + part

            z_out(s, n_sub - 1).start()
            with jax.named_scope("f_end"):
                end_tile(s, e, l, l == N_LAYER - 1)

                @pl.when(e == N_CHUNK - 1)
                def _():
                    load_weights(1, l)

                @pl.when(l < N_LAYER - 1)
                def _():
                    ring[(s + 1) % 3] = acc[:].astype(BF16)

                @pl.when(l == N_LAYER - 1)
                def _():
                    @pl.when(top)
                    def _():
                        pltpu.make_async_copy(targets.at[m], tgt, sems.t).wait()
                        err = acc[:].astype(BF16).astype(F32) - tgt[:].astype(F32)
                        loss_row[:] += jnp.sum(err * err, axis=0, keepdims=True)
                        zin[m] = (err * (1.0 / n_tok)).astype(BF16)

                    @pl.when(jnp.logical_not(top))
                    def _():
                        zout[:] = acc[:].astype(BF16)

                    @pl.when(sent(e))
                    def _():
                        z_copy(m).start()

            return 0

        n_fwd = N_TILE // 2
        lax.fori_loop(0, n_fwd, fwd_step, 0)
        for i in range(n_sub - N_SPARE, n_sub):
            z_out(n_fwd - 2, i).wait()
        for i in range(n_sub):
            z_out(n_fwd - 1, i).wait()
        for i in range(n_sub):
            z_in(n_fwd, i).start()

        def bwd_step(s, _):
            e, l = layer_of(s)
            m = e % N_CHUNK

            with jax.named_scope("b_pre"):
                start_tile(s, e, l, l == N_LAYER - 1)
                for i in range(n_sub):
                    z_in(s, i).wait()
            after = jnp.minimum(s + 1, N_TILE - 1)

            def z_next(i):
                store, _, _ = z_block(after, i, False)
                _, buf, b = z_block(s + 1, i, False)
                pltpu.make_async_copy(store, buf, sems.zi.at[b]).start()

            for i in range(N_SPARE):
                z_next(i)

            @pl.when(e == HALF + N_CHUNK)
            def _():
                wait_weights(l)

            with jax.named_scope("b_mm"):
                for i, (off, w) in enumerate(subs):
                    for o in range(0, w, BWD_BLOCK):
                        cut = slice(off + o, off + o + BWD_BLOCK)
                        g = ring[s % 3]
                        da = lax.dot_general(g, wdb[l, cut, :], NT, preferred_element_type=F32)
                        _, slope = gelu_and_slope(zb[(n_sub * s + i) % n_ring, :, o : o + BWD_BLOCK])
                        dz = (slope * da.astype(BF16).astype(F32)).astype(BF16)
                        part = lax.dot_general(dz, wub[l, :, cut], NT, preferred_element_type=F32)
                        acc[:] = (g.astype(F32) if i + o == 0 else acc[:]) + part
                    if i + N_SPARE < n_sub:
                        z_next(i + N_SPARE)

            with jax.named_scope("b_end"):
                end_tile(s, e, l, l == 0)

                @pl.when(e == HALF + N_CHUNK - 1)
                def _():
                    load_weights(0, l)

                @pl.when(l > 0)
                def _():
                    ring[(s + 1) % 3] = acc[:].astype(BF16)

                @pl.when(l == 0)
                def _():
                    zout[:] = acc[:].astype(BF16)

                    @pl.when(sent(e))
                    def _():
                        z_copy(m).start()

            return 0

        lax.fori_loop(n_fwd, N_TILE, bwd_step, 0)
        for i in range(n_sub):
            store, _, _ = z_block(N_TILE - 1, i, False)
            _, buf, b = z_block(N_TILE, i, False)
            pltpu.make_async_copy(store, buf, sems.zi.at[b]).wait()

        @pl.when(sent(2 * HALF - 1))
        def _():
            z_copy(0).wait_send()

        loss_ref[:] = jnp.broadcast_to(jnp.sum(loss_row[:], axis=1, keepdims=True), loss_ref.shape)

    width = window_width(ff)
    seg_d, seg_u = dd.shape[2], upp.shape[2]

    def grads(wub, wdb, hb, gb, gd, gu, cb, zw, ubb):
        def weight_copies(j):
            v, k = place.layer(j)
            start = pl.multiple_of(place.share(j).start(ff), 128)
            b = j % 2
            return (
                pltpu.make_async_copy(wu.at[v, k, :, pl.ds(start, width)], wub.at[b], sems.ww.at[b, 0]),
                pltpu.make_async_copy(wd.at[v, k, pl.ds(start, width), :], wdb.at[b], sems.ww.at[b, 1]),
            )

        def fetches(n):
            v, k = place.layer(n // N_STEP)
            t = n % N_STEP
            m, part = t // 2, 2 * (t % 2)
            h_at = N_CHUNK * v + part
            g_at = HALF + N_CHUNK * (1 - v) + part
            b = n % 2
            return (
                pltpu.make_async_copy(hg.at[m, pl.ds(h_at, 2), k], hb.at[b], sems.hb.at[b]),
                pltpu.make_async_copy(hg.at[m, pl.ds(g_at, 2), k], gb.at[b], sems.gb.at[b]),
            )

        def z_fetch(n):
            v, k = place.layer(n // N_STEP)
            start = pl.multiple_of(place.share(n // N_STEP).start(ff), 128)
            src = zs.at[pl.ds(N_CHUNK * v + 2 * (n % N_STEP), 2), k, :, pl.ds(start, width)]
            return pltpu.make_async_copy(src, zw.at[n % 2], sems.zw.at[n % 2])

        def arrived(group):
            ref = hg.at[2, pl.ds(0, HALF), 0] if group else hg.at[2, pl.ds(0, HALF)]
            remote(ref, ref, sems.c_send, sems.c_recv.at[group], z_peer).wait_recv()
            remote(ref, ref, sems.f_send, sems.f_recv.at[group], z_peer).wait_recv()

        def stage_copies(j):
            sh = place.share(j)
            b = j % 2
            up = []
            for i in range(4):
                keep = sh.piece(i)
                send = keep + sh.wu * (1 - 2 * sh.u)
                for to, row, sem in ((sup, send, 0), (kup, keep, 1)):
                    src = gu.at[b, pl.ds(pl.multiple_of(row * seg_u, 8), seg_u), :]
                    up.append(pltpu.make_async_copy(src, to.at[j, i], sems.st.at[sem]))
            base = sh.base(ff)
            part = [gd.at[b, pl.ds(pl.multiple_of(base + seg_d * i, 8), seg_d), :] for i in (c, 1 - c)]
            same = [pltpu.make_async_copy(part[0], to.at[j, 0], sems.st.at[2]) for to in (dd, sd)]
            other = pltpu.make_async_copy(part[1], sd.at[j, 1], sems.st.at[3])
            return sh, up, same, other

        def stage_out(j):
            sh, up, same, other = stage_copies(j)
            for cp in up:
                cp.start()
            other.start()
            pl.when(sh.away == 0)(same[0].start)
            pl.when(sh.away == 1)(same[1].start)

        def down_same(j, sh):
            return remote(sd.at[j, 0], dd.at[j, 1], sems.ds_send, sems.d_recv.at[j, 1], at(sh.dest_same))

        def up_exchange(j, sh):
            return remote(sup.at[j], ub.at[j], sems.u_send, sems.u_recv.at[j], at(sh.partner))

        def send_out(j):
            sh = place.share(j)
            pltpu.make_async_copy(sup.at[j], sup.at[j], sems.st.at[0]).wait()
            up_exchange(j, sh).start()
            pltpu.make_async_copy(sd.at[j, 1], sd.at[j, 1], sems.st.at[3]).wait()
            pltpu.make_async_copy(sd.at[j, 0], sd.at[j, 0], sems.st.at[2]).wait()

            @pl.when(sh.away == 0)
            def _():
                slot = sh.kc
                remote(
                    sd.at[j, 1], dd.at[j, slot], sems.d_send, sems.d_recv.at[j, slot], at(sh.core_peer)
                ).start()

            @pl.when(sh.away == 1)
            def _():
                remote(sd.at[j, 1], rb.at[j], sems.d_send, sems.r_recv.at[j], at(sh.core_peer)).start()
                down_same(j, sh).start()

            pltpu.make_async_copy(kup.at[j], kup.at[j], sems.st.at[1]).wait()

        def relay(j):
            sh = place.share(j)

            @pl.when((sh.away == 0) & (sh.kc == 0))
            def _():
                cp = remote(rb.at[j], rb.at[j], sems.r_send, sems.r_recv.at[j], z_peer)
                cp.wait_recv()
                remote(rb.at[j], dd.at[j, 1], sems.r_send, sems.d_recv.at[j, 1], at(sh.partner)).start()

        def tail_sends(j):
            sh = place.share(j)
            b = j % 2
            out = []
            for i in range(4):
                row = sh.piece(i) + sh.wu * (1 - 2 * sh.u)
                src = gu.at[b, pl.ds(pl.multiple_of(row * seg_u, 8), seg_u), :]
                out.append(remote(src, ub.at[j, i], sems.t_send, sems.u_recv.at[j], at(sh.partner)))
            base = sh.base(ff)
            same, other = [gd.at[b, pl.ds(pl.multiple_of(base + seg_d * i, 8), seg_d), :] for i in (c, 1 - c)]
            out.append(remote(other, dd.at[j, 1], sems.td_send, sems.d_recv.at[j, 1], at(sh.core_peer)))
            out.append(pltpu.make_async_copy(same, dd.at[j, 0], sems.st.at[2]))
            return out

        def piece_sends(j, b):
            sh = place.share(j)
            out = [pltpu.make_async_copy(cb.at[b, 0], upp.at[j, 0], sems.p_here.at[b])]
            for i in range(1, 4):
                out.append(remote(cb.at[b, i], upp.at[j, i], sems.p_send.at[b], sems.p_recv.at[j], at(sh.piece(i))))
            return out

        def wait_pieces(j, b):
            piece_sends(j, b)[0].wait()
            ref = cb.at[b, pl.ds(1, 3)]
            remote(ref, ref, sems.p_send.at[b], sems.p_recv.at[j], z_peer).wait_send()

        def sum_loads(j, b):
            return (
                pltpu.make_async_copy(kup.at[j], cb.at[b], sems.cl.at[0]),
                pltpu.make_async_copy(ub.at[j], ubb, sems.cl.at[1]),
            )

        def sum_load(j, b):
            up_exchange(j, place.share(j)).wait_recv()
            for cp in sum_loads(j, b):
                cp.start()

        def sum_add(j, b):
            for cp in sum_loads(j, b):
                cp.wait()
            cb[b] += ubb[:]
            for cp in piece_sends(j, b):
                cp.start()

        for cp in (*weight_copies(0), *fetches(0), z_fetch(0)):
            cp.start()

        loss_peers = [at(local_peers[i]) for i in (0, 1, 3)] + [z_peer]

        def loss_copy(r):
            return remote(lbuf.at[0, r], lbuf.at[1, r], sems.l_send, sems.l_recv.at[r], loss_peers[r])

        def step(n, _):
            j, t = n // N_STEP, n % N_STEP
            b, jb = n % 2, j % 2

            with jax.named_scope("w_fwd"):
                @pl.when(n < DELAY)
                def _():
                    forward(n + N_TILE - DELAY)

            with jax.named_scope("w_arr"):
                for group, first in enumerate((0, 3, 4, 5)):
                    pl.when(n == first * N_STEP + 3)(lambda group=group: arrived(group))

            @pl.when(n + 1 < N_GRAD * N_STEP)
            def _():
                for cp in fetches(n + 1):
                    cp.start()

                pl.when((n + 1) % N_STEP < 2)(lambda: z_fetch(n + 1).start())

            with jax.named_scope("w_pre"):
                for r in range(5):

                    @pl.when(n == LOSS_AT[r])
                    def _():
                        if r:
                            loss_copy(r - 1).wait()
                            loss_ref[:] += lbuf[1, r - 1]
                        if r < 4:
                            lbuf[0, r] = loss_ref[:]

                    if r < 4:

                        @pl.when(n == LOSS_AT[r] + 1)
                        def _():
                            loss_copy(r).start()

                @pl.when(t == 0)
                def _():
                    for cp in weight_copies(j):
                        cp.wait()

                @pl.when((t == 1) & (j + 1 < N_GRAD))
                def _():
                    for cp in weight_copies(j + 1):
                        cp.start()

                @pl.when((t == 0) & (j >= 1))
                def _():
                    stage_out(j - 1)

                @pl.when((t == 1) & (j >= 1))
                def _():
                    send_out(j - 1)

                @pl.when((t == 2) & (j >= 1) & (j <= N_CHUNK))
                def _():
                    relay(j - 1)

            with jax.named_scope("w_sum"):
                for i, (b_, when) in SUM_AT.items():

                    @pl.when(n == when)
                    def _():
                        if i == 4:
                            wait_pieces(0, 0)
                        sum_load(i, b_)

                    @pl.when(n == when + 1)
                    def _():
                        sum_add(i, b_)

            with jax.named_scope("w_fetch"):
                for cp in fetches(n):
                    cp.wait()
            h = hb[b].reshape(2 * rows, d)
            g = gb[b].reshape(2 * rows, d)

            def accumulate(own):
                for off, w in grad_blocks(width):
                    cut = slice(off, off + w)
                    if own:
                        z = zw[b, :, :, cut].reshape(2 * rows, w)
                    else:
                        z = jnp.dot(h, wub[jb, :, cut], preferred_element_type=F32)
                    da = lax.dot_general(g, wdb[jb, cut, :], NT, preferred_element_type=F32).astype(BF16).astype(F32)
                    a, slope = gelu_and_slope(z)
                    a = a.astype(BF16)
                    dz = (slope * da).astype(BF16)
                    down = lax.dot_general(a, g, TN, preferred_element_type=F32)
                    up = lax.dot_general(h, dz, TN, preferred_element_type=F32)
                    if own:
                        gd[jb, cut, :] = jnp.where(t == 0, 0.0, gd[jb, cut, :]) + down
                        gu[jb, :, cut] = jnp.where(t == 0, 0.0, gu[jb, :, cut]) + up
                    else:
                        gd[jb, cut, :] += down
                        gu[jb, :, cut] += up

            with jax.named_scope("w_mm"):
                @pl.when(t < 2)
                def _():
                    z_fetch(n).wait()
                    accumulate(True)

                pl.when(t >= 2)(lambda: accumulate(False))
            return 0

        lax.fori_loop(0, N_GRAD * N_STEP, step, 0)
        with jax.named_scope("t_stage"):
            last = N_GRAD - 1
            for cp in tail_sends(last):
                cp.start()
        with jax.named_scope("t_sum5"):
            wait_pieces(1, 1)
            up_exchange(last, place.share(last)).wait_recv()
            load = sum_loads(last, 1)[1]
            load.start()
            load.wait()
            for i in range(4):
                row = pl.multiple_of(place.share(last).piece(i) * seg_u, 8)
                cb[1, i] = gu[last % 2, pl.ds(row, seg_u), :] + ubb[i]
            for cp in piece_sends(last, 1):
                cp.start()
        with jax.named_scope("t_sum3"):
            sum_load(3, 3)
            sum_add(3, 3)
        with jax.named_scope("t_pieces"):
            for j, b in ((2, 2), (4, 0), (last, 1), (3, 3)):
                wait_pieces(j, b)
            tail_sends(last)[-1].wait()
            remote(ub.at[last], ub.at[last], sems.t_send, sems.u_recv.at[last], z_peer).wait_send()
            tail_sends(last)[4].wait_send()

    pl.run_scoped(
        chain,
        pltpu.VMEM((N_LAYER, d, ff), BF16),
        pltpu.VMEM((N_LAYER, ff, d), BF16),
        pltpu.VMEM((3, *tile), BF16),
        pltpu.VMEM(tile, BF16),
        pltpu.VMEM((len(sub_blocks(ff)) + N_SPARE, rows, sub_blocks(ff)[0][1]), F32),
        pltpu.VMEM(tile, BF16),
        pltpu.VMEM(tile, F32),
        pltpu.VMEM((1, d), F32),
    )
    pl.run_scoped(
        grads,
        pltpu.VMEM((2, d, width), BF16),
        pltpu.VMEM((2, width, d), BF16),
        pltpu.VMEM((2, 2, *tile), BF16),
        pltpu.VMEM((2, 2, *tile), BF16),
        pltpu.VMEM((2, width, d), F32),
        pltpu.VMEM((2, d, width), F32),
        pltpu.VMEM((4, 4, seg_u, width), F32),
        pltpu.VMEM((2, 2, rows, width), F32),
        pltpu.VMEM((4, seg_u, width), F32),
    )

    with jax.named_scope("t_all"):
        for j in range(N_GRAD):
            sh = place.share(j)
            ref = upp.at[j, pl.ds(1, 3)]
            remote(ref, ref, sems.p_send.at[0], sems.p_recv.at[j], z_peer).wait_recv()
            ref = dd.at[j, 0]
            remote(ref, ref, sems.d_send, sems.d_recv.at[j, 1], z_peer).wait_recv()

            @pl.when(sh.away == 1)
            def _():
                remote(ref, ref, sems.ds_send, sems.d_recv.at[j, 0], z_peer).wait()

            @pl.when((sh.away == 0) & (sh.kc == 0))
            def _():
                remote(ref, ref, sems.r_send, sems.d_recv.at[j, 0], z_peer).wait_send()

        ref = sup.at[pl.ds(0, N_GRAD - 1)]
        remote(ref, ref, sems.u_send, sems.u_recv.at[0], z_peer).wait_send()
        ref = sd.at[pl.ds(0, N_GRAD - 1), 1]
        remote(ref, ref, sems.d_send, sems.d_recv.at[0, 0], z_peer).wait_send()
        for sem in (sems.a_send, sems.c_send, sems.f_send):
            remote(hg.at[0], hg.at[0], sem, sems.a_recv.at[0], z_peer).wait_send()


SEMS = {
    "w": (N_LAYER, 2),
    "zo": (N_RING,),
    "zi": (N_RING,),
    "z_recv": (N_CHUNK,),
    "a_recv": (N_TILE,),
    "c_recv": (N_CHUNK,),
    "f_recv": (N_CHUNK,),
    "ww": (2, 2),
    "hb": (2,),
    "gb": (2,),
    "zw": (2,),
    "st": (N_CHUNK,),
    "u_recv": (N_GRAD,),
    "d_recv": (N_GRAD, 2),
    "r_recv": (N_GRAD,),
    "cl": (2,),
    "p_send": (N_CHUNK,),
    "p_here": (N_CHUNK,),
    "p_recv": (N_GRAD,),
    "l_recv": (N_CHUNK,),
}
SEMS |= dict.fromkeys(("ld", "t", "z_send", "a_send", "c_send", "f_send", "u_send", "d_send"), ())
SEMS |= dict.fromkeys(("ds_send", "r_send", "t_send", "td_send", "l_send"), ())


class Sems:
    def __init__(self, refs):
        for name, ref in zip(SEMS, refs, strict=True):
            setattr(self, name, ref)


def step_call(tokens, targets, wu, wd, n_tok, n_data):
    n_chunk, rows, d = tokens.shape
    ff = wu.shape[-1]
    width = window_width(ff)
    pieces = jax.ShapeDtypeStruct((N_GRAD, 4, d // n_data, width), F32)
    parts = jax.ShapeDtypeStruct((N_GRAD, 2, ff // n_data, d), F32)

    def body(*refs):
        n = 14 + 2
        step_kernel(n_tok, *refs[:n], Sems(refs[n:]))

    return pl.pallas_call(
        body,
        in_specs=[ANY] * 4,
        out_specs=[ANY] * 3 + [pl.BlockSpec(memory_space=pltpu.VMEM)] + [ANY] * 6,
        out_shape=[
            jax.ShapeDtypeStruct((4, 2 * HALF, N_LAYER, rows, d), BF16),
            parts,
            pieces,
            jax.ShapeDtypeStruct((8, 128), F32),
            pieces,
            pieces,
            pieces,
            parts,
            jax.ShapeDtypeStruct((N_GRAD, ff // n_data, d), F32),
            jax.ShapeDtypeStruct((HALF, N_LAYER, rows, ff), F32),
        ],
        scratch_shapes=[
            pltpu.VMEM((n_chunk, rows, d), BF16),
            pltpu.VMEM((2, 4, 8, 128), F32),
            *[pltpu.SemaphoreType.DMA(shape) for shape in SEMS.values()],
        ],
        compiler_params=pltpu.CompilerParams(collective_id=0, has_side_effects=True, vmem_limit_bytes=67043328),
        name="step",
    )(tokens, targets, wu, wd)


def final_kernel(scal, dd, upp, down_ref, up_ref):
    down_ref[0, 0] = dd[0, 0] + dd[0, 1]
    width = upp.shape[-1]
    for i in range(4):
        start = pl.multiple_of(scal[4 * pl.program_id(0) + i], 128)
        up_ref[0, 0, :, pl.ds(start, width)] = upp[0, i]


def final_call(scal, dd, upp, n_data):
    seg_d, d = dd.shape[2:]
    seg_u, width = upp.shape[2:]
    ff = seg_d * n_data
    return pl.pallas_call(
        final_kernel,
        grid_spec=pltpu.PrefetchScalarGridSpec(
            num_scalar_prefetch=1,
            grid=(N_GRAD,),
            in_specs=[
                pl.BlockSpec((1, 2, seg_d, d), lambda j, s: (j, 0, 0, 0)),
                pl.BlockSpec((1, 4, seg_u, width), lambda j, s: (j, 0, 0, 0)),
            ],
            out_specs=[
                pl.BlockSpec((1, 1, seg_d, d), lambda j, s: (1 - j // N_LAYER, N_LAYER - 1 - j % N_LAYER, 0, 0)),
                pl.BlockSpec((1, 1, seg_u, ff), lambda j, s: (1 - j // N_LAYER, N_LAYER - 1 - j % N_LAYER, 0, 0)),
            ],
        ),
        out_shape=[
            jax.ShapeDtypeStruct((2, N_LAYER, seg_d, d), F32),
            jax.ShapeDtypeStruct((2, N_LAYER, seg_u, ff), F32),
        ],
        compiler_params=pltpu.CompilerParams(dimension_semantics=("arbitrary",), vmem_limit_bytes=62 * 2**20),
        name="final",
    )(scal, dd, upp)


def window_table(n_data, ff):
    table = []
    for dev in range(n_data):
        place = Place(0, dev)
        row = []
        for j in range(N_GRAD):
            for i in range(4):
                row.append(Place(0, place.share(j).piece(i)).share(j).start(ff))
        table.append(row)
    return np.array(table, np.int32)


def solution(mesh):
    n_data = mesh.shape["data"]

    def device_fn(tokens_loc, targets_loc, wu, wd):
        n_micro, seq_len, d = tokens_loc.shape
        n_tok = n_data * n_micro * seq_len
        ff = wu.shape[-1]
        rows = n_micro * seq_len // N_CHUNK
        tokens = tokens_loc.reshape(N_CHUNK, rows, d)
        targets = targets_loc.reshape(N_CHUNK, rows, d)
        out = step_call(tokens, targets, wu, wd, n_tok, n_data)
        dd, upp, loss = out[1:4]
        starts = jnp.asarray(window_table(n_data, ff))
        scal = lax.dynamic_index_in_dim(starts, lax.axis_index("data"), 0, keepdims=False)
        down, up = final_call(scal, dd, upp, n_data)
        return loss[0, 0] / (2.0 * n_tok), up, down

    return jax.shard_map(
        device_fn,
        mesh=mesh,
        in_specs=(P("data"), P("data"), P(None, "stage"), P(None, "stage")),
        out_specs=(P(), P(None, "stage", "data"), P(None, "stage", "data")),
        check_vma=False,
    )
```

```python
import jax
import jax.numpy as jnp
import numpy as np
from jax import lax
from jax.experimental import pallas as pl
from jax.experimental.pallas import tpu as pltpu
from jax.sharding import PartitionSpec as P

F32, BF16 = jnp.float32, jnp.bfloat16
MESH = pl.DeviceIdType.MESH
N_CHUNK = 4
N_LAYER = 3
HALF = 2 * N_CHUNK
N_TILE = 2 * HALF * N_LAYER
N_GRAD = 2 * N_LAYER
N_SPARE = 2
N_RING = 12
LOSS_AT = (0, 6, 15, 23, 30)
SUM_AT = {0: (0, 29), 3: (3, 35), 1: (1, 37), 2: (2, 42), 4: (0, 44)}
BWD_BLOCK = 256
N_STEP = 8
DELAY = 4 * N_LAYER
NT = (((1,), (1,)), ((), ()))
TN = (((0,), (0,)), ((), ()))
C0 = 0.7978845608028654
C1 = 0.044715
ANY = pl.BlockSpec(memory_space=pl.ANY)


def gelu(z):
    return z * (0.5 * (1.0 + jnp.tanh(C0 * (z + C1 * (z * z * z)))))


def gelu_and_slope(z):
    z2 = z * z
    t = jnp.tanh(C0 * (z + C1 * (z2 * z)))
    cdf = 0.5 * (1.0 + t)
    slope = cdf + (0.5 * z) * ((1.0 - t * t) * (C0 + (3.0 * C0 * C1) * z2))
    return cdf * z, slope


def sub_blocks(ff):
    step = 512
    return [(o, min(step, ff - o)) for o in range(0, ff, step)]


def grad_blocks(width):
    return [(o, min(768, width - o)) for o in range(0, width, 768)]


def window_width(ff):
    return (ff // 4 + 127) // 128 * 128


class Place:
    def __init__(self, stage, dev):
        self.stage, self.dev = stage, dev
        self.y, self.x, self.c = dev // 4, (dev // 2) % 2, dev % 2

    def flip(self, fy, fx, fc):
        return self.dev + fy * (4 - 8 * self.y) + fx * (2 - 4 * self.x) + fc * (1 - 2 * self.c)

    def gather(self, v, k):
        is_y = (v + k) % 2
        kind_c = (1 - v) * (1 - k // 2 * self.stage)
        one = self.flip(is_y, 1 - is_y, 0)
        two = self.flip(kind_c * (1 - is_y), kind_c * is_y, 1 - kind_c)
        return one, two

    def layer(self, j):
        return 1 - j // N_LAYER, N_LAYER - 1 - j % N_LAYER

    def group(self, v, k):
        return (1 - v) * (N_LAYER - k)

    def share(self, j):
        y, x, c = self.y, self.x, self.c
        v, k = self.layer(j)
        kc = (j + 1 - self.stage) // N_CHUNK
        dy = (1 - kc) * ((v + k) % 2)
        dx = (1 - kc) * (1 - (v + k) % 2)
        sh = Share()
        sh.kc = kc
        sh.p = (dy + kc) * y + dx * c
        sh.q = dy * c + (dx + kc) * x
        sh.wu, sh.w1, sh.w2 = 2 * dy + 4 * dx + kc, 4 * dy + 2 * dx + 4 * kc, dy + dx + 2 * kc
        sh.u = dy * x + dx * y + kc * c
        sh.r1 = dy * y + dx * x + kc * y
        sh.r2 = (dy + dx) * c + kc * x
        sh.partner = self.dev + sh.wu * (1 - 2 * sh.u)
        away = (1 - kc) * (sh.u * (1 - c) + c * (1 - sh.u))
        sh.away = away
        sh.dest_same = self.dev + away * sh.wu * (1 - 2 * sh.u)
        sh.core_peer = self.dev + (1 - 2 * c)
        return sh


class Share:
    def piece(self, i):
        r1 = self.r1 + (i // 2) * (1 - 2 * self.r1)
        r2 = self.r2 + (i % 2) * (1 - 2 * self.r2)
        return self.w1 * r1 + self.w2 * r2 + self.wu * self.u

    def start(self, ff):
        return (ff // 2) * self.p + (ff // 2 - window_width(ff)) * self.q

    def base(self, ff):
        return (ff // 4 - (ff // 2 - window_width(ff))) * self.q


def layer_of(s):
    e = s // N_LAYER
    r = s - N_LAYER * e
    back = e // HALF
    return e, r + back * (N_LAYER - 1 - 2 * r)


def block_of(e):
    back = e // HALF
    first = (e - HALF * back) // N_CHUNK
    return first + back * (1 - 2 * first)


def step_kernel(n_tok, tokens, targets, wu, wd, hg, dd, upp, loss_ref, sup, kup, ub, sd, rb, zs, zin, lbuf, sems):
    place = Place(lax.axis_index("stage"), lax.axis_index("data"))
    stage, dev, c = place.stage, place.dev, place.c
    d, ff = wu.shape[2:]
    rows = zin.shape[1]
    tile = (rows, d)

    def remote(src, dst, send, recv, to):
        return pltpu.make_async_remote_copy(src, dst, send, recv, to, MESH)

    def at(index):
        return (stage, index)

    z_peer = (1 - stage, dev)
    local_peers = [place.flip(i // 4, i // 2 % 2, i % 2) for i in range(1, 7)]

    @pl.when(stage == 0)
    def _():
        for m in range(N_CHUNK):
            pltpu.make_async_copy(tokens.at[m], zin.at[m], sems.z_recv.at[m]).start()

    barrier = pltpu.get_barrier_semaphore()
    for peer in [z_peer] + [at(i) for i in local_peers]:
        pl.semaphore_signal(barrier, inc=1, device_id=peer, device_id_type=MESH)
    pl.semaphore_wait(barrier, 1 + len(local_peers))

    def a_copy(s):
        e, l = layer_of(s)
        one, _ = place.gather(block_of(e), l)
        return remote(hg.at[0, e, l], hg.at[1, e, l], sems.a_send, sems.a_recv.at[s], at(one))

    def c_copy(s):
        e, l = layer_of(s)
        v = block_of(e)
        _, two = place.gather(v, l)
        return remote(hg.at[0, e, l], hg.at[2, e, l], sems.c_send, sems.c_recv.at[place.group(v, l)], at(two))

    def forward(s):
        e, l = layer_of(s)
        v = block_of(e)
        _, two = place.gather(v, l)
        a_copy(s).wait_recv()
        remote(hg.at[1, e, l], hg.at[3, e, l], sems.f_send, sems.f_recv.at[place.group(v, l)], at(two)).start()

    def chain(wub, wdb, ring, zout, zb, tgt, acc, loss_row):
        subs = sub_blocks(ff)
        n_sub = len(subs)
        n_ring = n_sub + N_SPARE
        assert n_ring <= N_RING

        def weight_copies(v, l):
            return (
                pltpu.make_async_copy(wu.at[v, l], wub.at[l], sems.w.at[l, 0]),
                pltpu.make_async_copy(wd.at[v, l], wdb.at[l], sems.w.at[l, 1]),
            )

        def load_weights(v, l):
            for cp in weight_copies(v, l):
                cp.start()

        def wait_weights(l):
            for cp in weight_copies(0, l):
                cp.wait()

        def z_copy(m):
            return remote(zout, zin.at[m], sems.z_send, sems.z_recv.at[m], z_peer)

        def sent(e):
            fwd = (e < HALF) & ((stage == 0) | (e < N_CHUNK))
            return fwd | ((e >= HALF) & ((stage == 1) | (e < HALF + N_CHUNK)))

        def start_tile(s, e, l, first):
            @pl.when(first)
            def _():
                @pl.when(jnp.logical_not((stage == 1) & (e >= HALF) & (e < HALF + N_CHUNK)))
                def _():
                    z_copy(e % N_CHUNK).wait_recv()

                ring[s % 3] = zin[e % N_CHUNK]

            pltpu.make_async_copy(ring.at[s % 3], hg.at[0, e, l], sems.ld).start()

        def end_tile(s, e, l, last):
            pltpu.make_async_copy(ring.at[s % 3], hg.at[0, e, l], sems.ld).wait()
            a_copy(s).start()
            c_copy(s).start()

            @pl.when(s >= DELAY)
            def _():
                forward(s - DELAY)

            @pl.when(last & (e >= 1))
            def _():
                @pl.when(sent(e - 1))
                def _():
                    z_copy(0).wait_send()

        for l in range(N_LAYER):
            load_weights(0, l)

        def z_block(s, i, forward_pass):
            e, l = layer_of(s)
            off, w = subs[i]
            q = e if forward_pass else N_CHUNK * block_of(e) + e % N_CHUNK
            b = (n_sub * s + i) % n_ring
            return zs.at[q, l, :, pl.ds(off, w)], zb.at[b, :, pl.ds(0, w)], b

        def z_out(s, i):
            store, buf, b = z_block(s, i, True)
            return pltpu.make_async_copy(buf, store, sems.zo.at[b])

        def z_in(s, i):
            store, buf, b = z_block(s, i, False)
            return pltpu.make_async_copy(store, buf, sems.zi.at[b])

        loss_row[:] = jnp.zeros_like(loss_row)

        def fwd_step(s, _):
            e, l = layer_of(s)
            v, m = e // N_CHUNK, e % N_CHUNK
            top = (stage == 1) & (v == 1)
            with jax.named_scope("f_pre"):
                start_tile(s, e, l, l == 0)

                @pl.when(top & (l == 0))
                def _():
                    pltpu.make_async_copy(targets.at[m], tgt, sems.t).start()

                @pl.when(m == 0)
                def _():
                    wait_weights(l)

                @pl.when(s >= 1)
                def _():
                    for i in range(n_sub - N_SPARE):
                        z_out(s - 1, i).wait()

                @pl.when(s >= 2)
                def _():
                    for i in range(n_sub - N_SPARE, n_sub):
                        z_out(s - 2, i).wait()

            with jax.named_scope("f_mm"):
                for i, (off, w) in enumerate(subs):
                    h = ring[s % 3]
                    z = jnp.dot(h, wub[l, :, off : off + w], preferred_element_type=F32)
                    zb[(n_sub * s + i) % n_ring, :, :w] = z
                    if i:
                        z_out(s, i - 1).start()
                    a = gelu(z).astype(BF16)
                    part = jnp.dot(a, wdb[l, off : off + w, :], preferred_element_type=F32)
                    acc[:] = (h.astype(F32) if i == 0 else acc[:]) + part

            z_out(s, n_sub - 1).start()
            with jax.named_scope("f_end"):
                end_tile(s, e, l, l == N_LAYER - 1)

                @pl.when(e == N_CHUNK - 1)
                def _():
                    load_weights(1, l)

                @pl.when(l < N_LAYER - 1)
                def _():
                    ring[(s + 1) % 3] = acc[:].astype(BF16)

                @pl.when(l == N_LAYER - 1)
                def _():
                    @pl.when(top)
                    def _():
                        pltpu.make_async_copy(targets.at[m], tgt, sems.t).wait()
                        err = acc[:].astype(BF16).astype(F32) - tgt[:].astype(F32)
                        loss_row[:] += jnp.sum(err * err, axis=0, keepdims=True)
                        zin[m] = (err * (1.0 / n_tok)).astype(BF16)

                    @pl.when(jnp.logical_not(top))
                    def _():
                        zout[:] = acc[:].astype(BF16)

                    @pl.when(sent(e))
                    def _():
                        z_copy(m).start()

            return 0

        n_fwd = N_TILE // 2
        lax.fori_loop(0, n_fwd, fwd_step, 0)
        for i in range(n_sub - N_SPARE, n_sub):
            z_out(n_fwd - 2, i).wait()
        for i in range(n_sub):
            z_out(n_fwd - 1, i).wait()
        for i in range(n_sub):
            z_in(n_fwd, i).start()

        def bwd_step(s, _):
            e, l = layer_of(s)
            m = e % N_CHUNK

            with jax.named_scope("b_pre"):
                start_tile(s, e, l, l == N_LAYER - 1)
                for i in range(n_sub):
                    z_in(s, i).wait()
            after = jnp.minimum(s + 1, N_TILE - 1)

            def z_next(i):
                store, _, _ = z_block(after, i, False)
                _, buf, b = z_block(s + 1, i, False)
                pltpu.make_async_copy(store, buf, sems.zi.at[b]).start()

            for i in range(N_SPARE):
                z_next(i)

            @pl.when(e == HALF + N_CHUNK)
            def _():
                wait_weights(l)

            with jax.named_scope("b_mm"):
                for i, (off, w) in enumerate(subs):
                    for o in range(0, w, BWD_BLOCK):
                        cut = slice(off + o, off + o + BWD_BLOCK)
                        g = ring[s % 3]
                        da = lax.dot_general(g, wdb[l, cut, :], NT, preferred_element_type=F32)
                        _, slope = gelu_and_slope(zb[(n_sub * s + i) % n_ring, :, o : o + BWD_BLOCK])
                        dz = (slope * da.astype(BF16).astype(F32)).astype(BF16)
                        part = lax.dot_general(dz, wub[l, :, cut], NT, preferred_element_type=F32)
                        acc[:] = (g.astype(F32) if i + o == 0 else acc[:]) + part
                    if i + N_SPARE < n_sub:
                        z_next(i + N_SPARE)

            with jax.named_scope("b_end"):
                end_tile(s, e, l, l == 0)

                @pl.when(e == HALF + N_CHUNK - 1)
                def _():
                    load_weights(0, l)

                @pl.when(l > 0)
                def _():
                    ring[(s + 1) % 3] = acc[:].astype(BF16)

                @pl.when(l == 0)
                def _():
                    zout[:] = acc[:].astype(BF16)

                    @pl.when(sent(e))
                    def _():
                        z_copy(m).start()

            return 0

        lax.fori_loop(n_fwd, N_TILE, bwd_step, 0)
        for i in range(n_sub):
            store, _, _ = z_block(N_TILE - 1, i, False)
            _, buf, b = z_block(N_TILE, i, False)
            pltpu.make_async_copy(store, buf, sems.zi.at[b]).wait()

        @pl.when(sent(2 * HALF - 1))
        def _():
            z_copy(0).wait_send()

        loss_ref[:] = jnp.broadcast_to(jnp.sum(loss_row[:], axis=1, keepdims=True), loss_ref.shape)

    width = window_width(ff)
    seg_d, seg_u = dd.shape[2], upp.shape[2]

    def grads(wub, wdb, hb, gb, gd, gu, cb, zw, ubb):
        def weight_copies(j):
            v, k = place.layer(j)
            start = pl.multiple_of(place.share(j).start(ff), 128)
            b = j % 2
            return (
                pltpu.make_async_copy(wu.at[v, k, :, pl.ds(start, width)], wub.at[b], sems.ww.at[b, 0]),
                pltpu.make_async_copy(wd.at[v, k, pl.ds(start, width), :], wdb.at[b], sems.ww.at[b, 1]),
            )

        def fetches(n):
            v, k = place.layer(n // N_STEP)
            t = n % N_STEP
            m, part = t // 2, 2 * (t % 2)
            h_at = N_CHUNK * v + part
            g_at = HALF + N_CHUNK * (1 - v) + part
            b = n % 2
            return (
                pltpu.make_async_copy(hg.at[m, pl.ds(h_at, 2), k], hb.at[b], sems.hb.at[b]),
                pltpu.make_async_copy(hg.at[m, pl.ds(g_at, 2), k], gb.at[b], sems.gb.at[b]),
            )

        def z_fetch(n):
            v, k = place.layer(n // N_STEP)
            start = pl.multiple_of(place.share(n // N_STEP).start(ff), 128)
            src = zs.at[pl.ds(N_CHUNK * v + 2 * (n % N_STEP), 2), k, :, pl.ds(start, width)]
            return pltpu.make_async_copy(src, zw.at[n % 2], sems.zw.at[n % 2])

        def arrived(group):
            ref = hg.at[2, pl.ds(0, HALF), 0] if group else hg.at[2, pl.ds(0, HALF)]
            remote(ref, ref, sems.c_send, sems.c_recv.at[group], z_peer).wait_recv()
            remote(ref, ref, sems.f_send, sems.f_recv.at[group], z_peer).wait_recv()

        def stage_copies(j):
            sh = place.share(j)
            b = j % 2
            up = []
            for i in range(4):
                keep = sh.piece(i)
                send = keep + sh.wu * (1 - 2 * sh.u)
                for to, row, sem in ((sup, send, 0), (kup, keep, 1)):
                    src = gu.at[b, pl.ds(pl.multiple_of(row * seg_u, 8), seg_u), :]
                    up.append(pltpu.make_async_copy(src, to.at[j, i], sems.st.at[sem]))
            base = sh.base(ff)
            part = [gd.at[b, pl.ds(pl.multiple_of(base + seg_d * i, 8), seg_d), :] for i in (c, 1 - c)]
            same = [pltpu.make_async_copy(part[0], to.at[j, 0], sems.st.at[2]) for to in (dd, sd)]
            other = pltpu.make_async_copy(part[1], sd.at[j, 1], sems.st.at[3])
            return sh, up, same, other

        def stage_out(j):
            sh, up, same, other = stage_copies(j)
            for cp in up:
                cp.start()
            other.start()
            pl.when(sh.away == 0)(same[0].start)
            pl.when(sh.away == 1)(same[1].start)

        def down_same(j, sh):
            return remote(sd.at[j, 0], dd.at[j, 1], sems.ds_send, sems.d_recv.at[j, 1], at(sh.dest_same))

        def up_exchange(j, sh):
            return remote(sup.at[j], ub.at[j], sems.u_send, sems.u_recv.at[j], at(sh.partner))

        def send_out(j):
            sh = place.share(j)
            pltpu.make_async_copy(sup.at[j], sup.at[j], sems.st.at[0]).wait()
            up_exchange(j, sh).start()
            pltpu.make_async_copy(sd.at[j, 1], sd.at[j, 1], sems.st.at[3]).wait()
            pltpu.make_async_copy(sd.at[j, 0], sd.at[j, 0], sems.st.at[2]).wait()

            @pl.when(sh.away == 0)
            def _():
                slot = sh.kc
                remote(
                    sd.at[j, 1], dd.at[j, slot], sems.d_send, sems.d_recv.at[j, slot], at(sh.core_peer)
                ).start()

            @pl.when(sh.away == 1)
            def _():
                remote(sd.at[j, 1], rb.at[j], sems.d_send, sems.r_recv.at[j], at(sh.core_peer)).start()
                down_same(j, sh).start()

            pltpu.make_async_copy(kup.at[j], kup.at[j], sems.st.at[1]).wait()

        def relay(j):
            sh = place.share(j)

            @pl.when((sh.away == 0) & (sh.kc == 0))
            def _():
                cp = remote(rb.at[j], rb.at[j], sems.r_send, sems.r_recv.at[j], z_peer)
                cp.wait_recv()
                remote(rb.at[j], dd.at[j, 1], sems.r_send, sems.d_recv.at[j, 1], at(sh.partner)).start()

        def tail_sends(j):
            sh = place.share(j)
            b = j % 2
            out = []
            for i in range(4):
                row = sh.piece(i) + sh.wu * (1 - 2 * sh.u)
                src = gu.at[b, pl.ds(pl.multiple_of(row * seg_u, 8), seg_u), :]
                out.append(remote(src, ub.at[j, i], sems.t_send, sems.u_recv.at[j], at(sh.partner)))
            base = sh.base(ff)
            same, other = [gd.at[b, pl.ds(pl.multiple_of(base + seg_d * i, 8), seg_d), :] for i in (c, 1 - c)]
            out.append(remote(other, dd.at[j, 1], sems.td_send, sems.d_recv.at[j, 1], at(sh.core_peer)))
            out.append(pltpu.make_async_copy(same, dd.at[j, 0], sems.st.at[2]))
            return out

        def piece_sends(j, b):
            sh = place.share(j)
            out = [pltpu.make_async_copy(cb.at[b, 0], upp.at[j, 0], sems.p_here.at[b])]
            for i in range(1, 4):
                out.append(remote(cb.at[b, i], upp.at[j, i], sems.p_send.at[b], sems.p_recv.at[j], at(sh.piece(i))))
            return out

        def wait_pieces(j, b):
            piece_sends(j, b)[0].wait()
            ref = cb.at[b, pl.ds(1, 3)]
            remote(ref, ref, sems.p_send.at[b], sems.p_recv.at[j], z_peer).wait_send()

        def sum_loads(j, b):
            return (
                pltpu.make_async_copy(kup.at[j], cb.at[b], sems.cl.at[0]),
                pltpu.make_async_copy(ub.at[j], ubb, sems.cl.at[1]),
            )

        def sum_load(j, b):
            up_exchange(j, place.share(j)).wait_recv()
            for cp in sum_loads(j, b):
                cp.start()

        def sum_add(j, b):
            for cp in sum_loads(j, b):
                cp.wait()
            cb[b] += ubb[:]
            for cp in piece_sends(j, b):
                cp.start()

        for cp in (*weight_copies(0), *fetches(0), z_fetch(0)):
            cp.start()

        loss_peers = [at(local_peers[i]) for i in (0, 1, 3)] + [z_peer]

        def loss_copy(r):
            return remote(lbuf.at[0, r], lbuf.at[1, r], sems.l_send, sems.l_recv.at[r], loss_peers[r])

        def step(n, _):
            j, t = n // N_STEP, n % N_STEP
            b, jb = n % 2, j % 2

            with jax.named_scope("w_fwd"):
                @pl.when(n < DELAY)
                def _():
                    forward(n + N_TILE - DELAY)

            with jax.named_scope("w_arr"):
                for group, first in enumerate((0, 3, 4, 5)):
                    pl.when(n == first * N_STEP + 3)(lambda group=group: arrived(group))

            @pl.when(n + 1 < N_GRAD * N_STEP)
            def _():
                for cp in fetches(n + 1):
                    cp.start()

                pl.when((n + 1) % N_STEP < 2)(lambda: z_fetch(n + 1).start())

            with jax.named_scope("w_pre"):
                for r in range(5):

                    @pl.when(n == LOSS_AT[r])
                    def _():
                        if r:
                            loss_copy(r - 1).wait()
                            loss_ref[:] += lbuf[1, r - 1]
                        if r < 4:
                            lbuf[0, r] = loss_ref[:]

                    if r < 4:

                        @pl.when(n == LOSS_AT[r] + 1)
                        def _():
                            loss_copy(r).start()

                @pl.when(t == 0)
                def _():
                    for cp in weight_copies(j):
                        cp.wait()

                @pl.when((t == 1) & (j + 1 < N_GRAD))
                def _():
                    for cp in weight_copies(j + 1):
                        cp.start()

                @pl.when((t == 0) & (j >= 1))
                def _():
                    stage_out(j - 1)

                @pl.when((t == 1) & (j >= 1))
                def _():
                    send_out(j - 1)

                @pl.when((t == 2) & (j >= 1) & (j <= N_CHUNK))
                def _():
                    relay(j - 1)

            with jax.named_scope("w_sum"):
                for i, (b_, when) in SUM_AT.items():
                    here = (stage == 0) | (i != 3)

                    @pl.when((n == when) & here)
                    def _():
                        if i == 4:
                            wait_pieces(0, 0)
                        sum_load(i, b_)

                    @pl.when((n == when + 1) & here)
                    def _():
                        sum_add(i, b_)

            with jax.named_scope("w_fetch"):
                for cp in fetches(n):
                    cp.wait()
            h = hb[b].reshape(2 * rows, d)
            g = gb[b].reshape(2 * rows, d)

            def accumulate(own):
                for off, w in grad_blocks(width):
                    cut = slice(off, off + w)
                    if own:
                        z = zw[b, :, :, cut].reshape(2 * rows, w)
                    else:
                        z = jnp.dot(h, wub[jb, :, cut], preferred_element_type=F32)
                    da = lax.dot_general(g, wdb[jb, cut, :], NT, preferred_element_type=F32).astype(BF16).astype(F32)
                    a, slope = gelu_and_slope(z)
                    a = a.astype(BF16)
                    dz = (slope * da).astype(BF16)
                    down = lax.dot_general(a, g, TN, preferred_element_type=F32)
                    up = lax.dot_general(h, dz, TN, preferred_element_type=F32)
                    if own:
                        gd[jb, cut, :] = jnp.where(t == 0, 0.0, gd[jb, cut, :]) + down
                        gu[jb, :, cut] = jnp.where(t == 0, 0.0, gu[jb, :, cut]) + up
                    else:
                        gd[jb, cut, :] += down
                        gu[jb, :, cut] += up

            with jax.named_scope("w_mm"):
                @pl.when(t < 2)
                def _():
                    z_fetch(n).wait()
                    accumulate(True)

                pl.when(t >= 2)(lambda: accumulate(False))
            return 0

        lax.fori_loop(0, N_GRAD * N_STEP, step, 0)
        with jax.named_scope("t_stage"):
            last = N_GRAD - 1
            for cp in tail_sends(last):
                cp.start()
        with jax.named_scope("t_sum5"):
            wait_pieces(1, 1)
            up_exchange(last, place.share(last)).wait_recv()
            load = sum_loads(last, 1)[1]
            load.start()
            load.wait()
            for i in range(4):
                row = pl.multiple_of(place.share(last).piece(i) * seg_u, 8)
                cb[1, i] = gu[last % 2, pl.ds(row, seg_u), :] + ubb[i]
            for cp in piece_sends(last, 1):
                cp.start()

        with jax.named_scope("t_sum3"):
            @pl.when(stage == 1)
            def _():
                sum_load(3, 3)
                sum_add(3, 3)

        with jax.named_scope("t_pieces"):
            for j, b in ((2, 2), (4, 0), (last, 1), (3, 3)):
                wait_pieces(j, b)
            tail_sends(last)[-1].wait()
            remote(ub.at[last], ub.at[last], sems.t_send, sems.u_recv.at[last], z_peer).wait_send()
            tail_sends(last)[4].wait_send()

    pl.run_scoped(
        chain,
        pltpu.VMEM((N_LAYER, d, ff), BF16),
        pltpu.VMEM((N_LAYER, ff, d), BF16),
        pltpu.VMEM((3, *tile), BF16),
        pltpu.VMEM(tile, BF16),
        pltpu.VMEM((len(sub_blocks(ff)) + N_SPARE, rows, sub_blocks(ff)[0][1]), F32),
        pltpu.VMEM(tile, BF16),
        pltpu.VMEM(tile, F32),
        pltpu.VMEM((1, d), F32),
    )
    pl.run_scoped(
        grads,
        pltpu.VMEM((2, d, width), BF16),
        pltpu.VMEM((2, width, d), BF16),
        pltpu.VMEM((2, 2, *tile), BF16),
        pltpu.VMEM((2, 2, *tile), BF16),
        pltpu.VMEM((2, width, d), F32),
        pltpu.VMEM((2, d, width), F32),
        pltpu.VMEM((4, 4, seg_u, width), F32),
        pltpu.VMEM((2, 2, rows, width), F32),
        pltpu.VMEM((4, seg_u, width), F32),
    )

    with jax.named_scope("t_all"):
        for j in range(N_GRAD):
            sh = place.share(j)
            ref = upp.at[j, pl.ds(1, 3)]
            remote(ref, ref, sems.p_send.at[0], sems.p_recv.at[j], z_peer).wait_recv()
            ref = dd.at[j, 0]
            remote(ref, ref, sems.d_send, sems.d_recv.at[j, 1], z_peer).wait_recv()

            @pl.when(sh.away == 1)
            def _():
                remote(ref, ref, sems.ds_send, sems.d_recv.at[j, 0], z_peer).wait()

            @pl.when((sh.away == 0) & (sh.kc == 0))
            def _():
                remote(ref, ref, sems.r_send, sems.d_recv.at[j, 0], z_peer).wait_send()

        ref = sup.at[pl.ds(0, N_GRAD - 1)]
        remote(ref, ref, sems.u_send, sems.u_recv.at[0], z_peer).wait_send()
        ref = sd.at[pl.ds(0, N_GRAD - 1), 1]
        remote(ref, ref, sems.d_send, sems.d_recv.at[0, 0], z_peer).wait_send()
        for sem in (sems.a_send, sems.c_send, sems.f_send):
            remote(hg.at[0], hg.at[0], sem, sems.a_recv.at[0], z_peer).wait_send()


SEMS = {
    "w": (N_LAYER, 2),
    "zo": (N_RING,),
    "zi": (N_RING,),
    "z_recv": (N_CHUNK,),
    "a_recv": (N_TILE,),
    "c_recv": (N_CHUNK,),
    "f_recv": (N_CHUNK,),
    "ww": (2, 2),
    "hb": (2,),
    "gb": (2,),
    "zw": (2,),
    "st": (N_CHUNK,),
    "u_recv": (N_GRAD,),
    "d_recv": (N_GRAD, 2),
    "r_recv": (N_GRAD,),
    "cl": (2,),
    "p_send": (N_CHUNK,),
    "p_here": (N_CHUNK,),
    "p_recv": (N_GRAD,),
    "l_recv": (N_CHUNK,),
}
SEMS |= dict.fromkeys(("ld", "t", "z_send", "a_send", "c_send", "f_send", "u_send", "d_send"), ())
SEMS |= dict.fromkeys(("ds_send", "r_send", "t_send", "td_send", "l_send"), ())


class Sems:
    def __init__(self, refs):
        for name, ref in zip(SEMS, refs, strict=True):
            setattr(self, name, ref)


def step_call(tokens, targets, wu, wd, n_tok, n_data):
    n_chunk, rows, d = tokens.shape
    ff = wu.shape[-1]
    width = window_width(ff)
    pieces = jax.ShapeDtypeStruct((N_GRAD, 4, d // n_data, width), F32)
    parts = jax.ShapeDtypeStruct((N_GRAD, 2, ff // n_data, d), F32)

    def body(*refs):
        n = 14 + 2
        step_kernel(n_tok, *refs[:n], Sems(refs[n:]))

    return pl.pallas_call(
        body,
        in_specs=[ANY] * 4,
        out_specs=[ANY] * 3 + [pl.BlockSpec(memory_space=pltpu.VMEM)] + [ANY] * 6,
        out_shape=[
            jax.ShapeDtypeStruct((4, 2 * HALF, N_LAYER, rows, d), BF16),
            parts,
            pieces,
            jax.ShapeDtypeStruct((8, 128), F32),
            pieces,
            pieces,
            pieces,
            parts,
            jax.ShapeDtypeStruct((N_GRAD, ff // n_data, d), F32),
            jax.ShapeDtypeStruct((HALF, N_LAYER, rows, ff), F32),
        ],
        scratch_shapes=[
            pltpu.VMEM((n_chunk, rows, d), BF16),
            pltpu.VMEM((2, 4, 8, 128), F32),
            *[pltpu.SemaphoreType.DMA(shape) for shape in SEMS.values()],
        ],
        compiler_params=pltpu.CompilerParams(collective_id=0, has_side_effects=True, vmem_limit_bytes=67043328),
        name="step",
    )(tokens, targets, wu, wd)


def final_kernel(scal, dd, upp, down_ref, up_ref):
    down_ref[0, 0] = dd[0, 0] + dd[0, 1]
    width = upp.shape[-1]
    for i in range(4):
        start = pl.multiple_of(scal[4 * pl.program_id(0) + i], 128)
        up_ref[0, 0, :, pl.ds(start, width)] = upp[0, i]


def final_call(scal, dd, upp, n_data):
    seg_d, d = dd.shape[2:]
    seg_u, width = upp.shape[2:]
    ff = seg_d * n_data
    return pl.pallas_call(
        final_kernel,
        grid_spec=pltpu.PrefetchScalarGridSpec(
            num_scalar_prefetch=1,
            grid=(N_GRAD,),
            in_specs=[
                pl.BlockSpec((1, 2, seg_d, d), lambda j, s: (j, 0, 0, 0)),
                pl.BlockSpec((1, 4, seg_u, width), lambda j, s: (j, 0, 0, 0)),
            ],
            out_specs=[
                pl.BlockSpec((1, 1, seg_d, d), lambda j, s: (1 - j // N_LAYER, N_LAYER - 1 - j % N_LAYER, 0, 0)),
                pl.BlockSpec((1, 1, seg_u, ff), lambda j, s: (1 - j // N_LAYER, N_LAYER - 1 - j % N_LAYER, 0, 0)),
            ],
        ),
        out_shape=[
            jax.ShapeDtypeStruct((2, N_LAYER, seg_d, d), F32),
            jax.ShapeDtypeStruct((2, N_LAYER, seg_u, ff), F32),
        ],
        compiler_params=pltpu.CompilerParams(dimension_semantics=("arbitrary",), vmem_limit_bytes=62 * 2**20),
        name="final",
    )(scal, dd, upp)


def window_table(n_data, ff):
    table = []
    for i in range(2 * n_data):
        stage, dev = i // n_data, i % n_data
        shares = [(j, Place(stage, dev).share(j)) for j in range(N_GRAD)]
        table.append([Place(stage, sh.piece(i)).share(j).start(ff) for j, sh in shares for i in range(4)])
    return np.array(table, np.int32)


def solution(mesh):
    n_data = mesh.shape["data"]

    def device_fn(tokens_loc, targets_loc, wu, wd):
        n_micro, seq_len, d = tokens_loc.shape
        n_tok = n_data * n_micro * seq_len
        ff = wu.shape[-1]
        rows = n_micro * seq_len // N_CHUNK
        tokens = tokens_loc.reshape(N_CHUNK, rows, d)
        targets = targets_loc.reshape(N_CHUNK, rows, d)
        out = step_call(tokens, targets, wu, wd, n_tok, n_data)
        dd, upp, loss = out[1:4]
        starts = jnp.asarray(window_table(n_data, ff))
        row = lax.axis_index("stage") * n_data + lax.axis_index("data")
        scal = lax.dynamic_index_in_dim(starts, row, 0, keepdims=False)
        down, up = final_call(scal, dd, upp, n_data)
        return loss[0, 0] / (2.0 * n_tok), up, down

    return jax.shard_map(
        device_fn,
        mesh=mesh,
        in_specs=(P("data"), P("data"), P(None, "stage"), P(None, "stage")),
        out_specs=(P(), P(None, "stage", "data"), P(None, "stage", "data")),
        check_vma=False,
    )
```

```python
import jax
import jax.numpy as jnp
import numpy as np
from jax import lax
from jax.experimental import pallas as pl
from jax.experimental.pallas import tpu as pltpu
from jax.sharding import PartitionSpec as P

F32, BF16 = jnp.float32, jnp.bfloat16
MESH = pl.DeviceIdType.MESH
N_CHUNK = 4
N_LAYER = 3
HALF = 2 * N_CHUNK
N_TILE = 2 * HALF * N_LAYER
N_GRAD = 2 * N_LAYER
N_SPARE = 2
N_RING = 12
LOSS_AT = (0, 6, 15, 27, 36)
SUM_AT = {0: (0, 29), 3: (3, 35), 1: (1, 37), 2: (2, 42), 4: (0, 44)}
BWD_BLOCK = 256
N_STEP = 8
DELAY = 5 * N_LAYER
NT = (((1,), (1,)), ((), ()))
TN = (((0,), (0,)), ((), ()))
C0 = 0.7978845608028654
C1 = 0.044715
ANY = pl.BlockSpec(memory_space=pl.ANY)


def gelu(z):
    return z * (0.5 * (1.0 + jnp.tanh(C0 * (z + C1 * (z * z * z)))))


def gelu_and_slope(z):
    z2 = z * z
    t = jnp.tanh(C0 * (z + C1 * (z2 * z)))
    cdf = 0.5 * (1.0 + t)
    slope = cdf + (0.5 * z) * ((1.0 - t * t) * (C0 + (3.0 * C0 * C1) * z2))
    return cdf * z, slope


def sub_blocks(ff):
    step = 512
    return [(o, min(step, ff - o)) for o in range(0, ff, step)]


def grad_blocks(width):
    return [(o, min(768, width - o)) for o in range(0, width, 768)]


def window_width(ff):
    return (ff // 4 + 127) // 128 * 128


class Place:
    def __init__(self, stage, dev):
        self.stage, self.dev = stage, dev
        self.y, self.x, self.c = dev // 4, (dev // 2) % 2, dev % 2

    def flip(self, fy, fx, fc):
        return self.dev + fy * (4 - 8 * self.y) + fx * (2 - 4 * self.x) + fc * (1 - 2 * self.c)

    def gather(self, v, k):
        is_y = (v + k) % 2
        kind_c = (1 - v) * (1 - k // 2 * self.stage)
        one = self.flip(is_y, 1 - is_y, 0)
        two = self.flip(kind_c * (1 - is_y), kind_c * is_y, 1 - kind_c)
        return one, two

    def layer(self, j):
        return 1 - j // N_LAYER, N_LAYER - 1 - j % N_LAYER

    def group(self, v, k):
        return (1 - v) * (N_LAYER - k)

    def share(self, j):
        y, x, c = self.y, self.x, self.c
        v, k = self.layer(j)
        kc = (j + 1 - self.stage) // N_CHUNK
        dy = (1 - kc) * ((v + k) % 2)
        dx = (1 - kc) * (1 - (v + k) % 2)
        sh = Share()
        sh.kc = kc
        sh.p = (dy + kc) * y + dx * c
        sh.q = dy * c + (dx + kc) * x
        sh.wu, sh.w1, sh.w2 = 2 * dy + 4 * dx + kc, 4 * dy + 2 * dx + 4 * kc, dy + dx + 2 * kc
        sh.u = dy * x + dx * y + kc * c
        sh.r1 = dy * y + dx * x + kc * y
        sh.r2 = (dy + dx) * c + kc * x
        sh.partner = self.dev + sh.wu * (1 - 2 * sh.u)
        away = (1 - kc) * (sh.u * (1 - c) + c * (1 - sh.u))
        sh.away = away
        sh.dest_same = self.dev + away * sh.wu * (1 - 2 * sh.u)
        sh.core_peer = self.dev + (1 - 2 * c)
        return sh


class Share:
    def piece(self, i):
        r1 = self.r1 + (i // 2) * (1 - 2 * self.r1)
        r2 = self.r2 + (i % 2) * (1 - 2 * self.r2)
        return self.w1 * r1 + self.w2 * r2 + self.wu * self.u

    def start(self, ff):
        return (ff // 2) * self.p + (ff // 2 - window_width(ff)) * self.q

    def base(self, ff):
        return (ff // 4 - (ff // 2 - window_width(ff))) * self.q


def layer_of(s):
    e = s // N_LAYER
    r = s - N_LAYER * e
    back = e // HALF
    return e, r + back * (N_LAYER - 1 - 2 * r)


def block_of(e):
    back = e // HALF
    first = (e - HALF * back) // N_CHUNK
    return first + back * (1 - 2 * first)


def step_kernel(n_tok, tokens, targets, wu, wd, hg, dd, upp, loss_ref, sup, kup, ub, sd, rb, zs, zin, lbuf, sems):
    place = Place(lax.axis_index("stage"), lax.axis_index("data"))
    stage, dev, c = place.stage, place.dev, place.c
    d, ff = wu.shape[2:]
    rows = zin.shape[1]
    tile = (rows, d)

    def remote(src, dst, send, recv, to):
        return pltpu.make_async_remote_copy(src, dst, send, recv, to, MESH)

    def at(index):
        return (stage, index)

    z_peer = (1 - stage, dev)
    local_peers = [place.flip(i // 4, i // 2 % 2, i % 2) for i in range(1, 7)]

    @pl.when(stage == 0)
    def _():
        for m in range(N_CHUNK):
            pltpu.make_async_copy(tokens.at[m], zin.at[m], sems.z_recv.at[m]).start()

    barrier = pltpu.get_barrier_semaphore()
    for peer in [z_peer] + [at(i) for i in local_peers]:
        pl.semaphore_signal(barrier, inc=1, device_id=peer, device_id_type=MESH)
    pl.semaphore_wait(barrier, 1 + len(local_peers))

    def a_copy(s):
        e, l = layer_of(s)
        one, _ = place.gather(block_of(e), l)
        return remote(hg.at[0, e, l], hg.at[1, e, l], sems.a_send, sems.a_recv.at[s], at(one))

    def c_copy(s):
        e, l = layer_of(s)
        v = block_of(e)
        _, two = place.gather(v, l)
        return remote(hg.at[0, e, l], hg.at[2, e, l], sems.c_send, sems.c_recv.at[place.group(v, l)], at(two))

    def forward(s):
        e, l = layer_of(s)
        v = block_of(e)
        _, two = place.gather(v, l)
        a_copy(s).wait_recv()
        remote(hg.at[1, e, l], hg.at[3, e, l], sems.f_send, sems.f_recv.at[place.group(v, l)], at(two)).start()

    def chain(wub, wdb, ring, zout, zb, tgt, acc, loss_row):
        subs = sub_blocks(ff)
        n_sub = len(subs)
        n_ring = n_sub + N_SPARE
        assert n_ring <= N_RING

        def weight_copies(v, l):
            return (
                pltpu.make_async_copy(wu.at[v, l], wub.at[l], sems.w.at[l, 0]),
                pltpu.make_async_copy(wd.at[v, l], wdb.at[l], sems.w.at[l, 1]),
            )

        def load_weights(v, l):
            for cp in weight_copies(v, l):
                cp.start()

        def wait_weights(l):
            for cp in weight_copies(0, l):
                cp.wait()

        def z_copy(m):
            return remote(zout, zin.at[m], sems.z_send, sems.z_recv.at[m], z_peer)

        def sent(e):
            fwd = (e < HALF) & ((stage == 0) | (e < N_CHUNK))
            return fwd | ((e >= HALF) & ((stage == 1) | (e < HALF + N_CHUNK)))

        def start_tile(s, e, l, first):
            @pl.when(first)
            def _():
                @pl.when(jnp.logical_not((stage == 1) & (e >= HALF) & (e < HALF + N_CHUNK)))
                def _():
                    z_copy(e % N_CHUNK).wait_recv()

                ring[s % 3] = zin[e % N_CHUNK]

            pltpu.make_async_copy(ring.at[s % 3], hg.at[0, e, l], sems.ld).start()

        def end_tile(s, e, l, last):
            pltpu.make_async_copy(ring.at[s % 3], hg.at[0, e, l], sems.ld).wait()
            a_copy(s).start()
            c_copy(s).start()

            @pl.when(s >= DELAY)
            def _():
                forward(s - DELAY)

            @pl.when(last & (e >= 1))
            def _():
                @pl.when(sent(e - 1))
                def _():
                    z_copy(0).wait_send()

        for l in range(N_LAYER):
            load_weights(0, l)

        def z_block(s, i, forward_pass):
            e, l = layer_of(s)
            off, w = subs[i]
            q = e if forward_pass else N_CHUNK * block_of(e) + e % N_CHUNK
            b = (n_sub * s + i) % n_ring
            return zs.at[q, l, :, pl.ds(off, w)], zb.at[b, :, pl.ds(0, w)], b

        def z_out(s, i):
            store, buf, b = z_block(s, i, True)
            return pltpu.make_async_copy(buf, store, sems.zo.at[b])

        def z_in(s, i):
            store, buf, b = z_block(s, i, False)
            return pltpu.make_async_copy(store, buf, sems.zi.at[b])

        loss_row[:] = jnp.zeros_like(loss_row)

        def fwd_step(s, _):
            e, l = layer_of(s)
            v, m = e // N_CHUNK, e % N_CHUNK
            top = (stage == 1) & (v == 1)
            start_tile(s, e, l, l == 0)

            @pl.when(top & (l == 0))
            def _():
                pltpu.make_async_copy(targets.at[m], tgt, sems.t).start()

            @pl.when(m == 0)
            def _():
                wait_weights(l)

            @pl.when(s >= 1)
            def _():
                for i in range(n_sub - N_SPARE):
                    z_out(s - 1, i).wait()

            @pl.when(s >= 2)
            def _():
                for i in range(n_sub - N_SPARE, n_sub):
                    z_out(s - 2, i).wait()

            for i, (off, w) in enumerate(subs):
                h = ring[s % 3]
                z = jnp.dot(h, wub[l, :, off : off + w], preferred_element_type=F32)
                zb[(n_sub * s + i) % n_ring, :, :w] = z
                if i:
                    z_out(s, i - 1).start()
                a = gelu(z).astype(BF16)
                part = jnp.dot(a, wdb[l, off : off + w, :], preferred_element_type=F32)
                acc[:] = (h.astype(F32) if i == 0 else acc[:]) + part

            z_out(s, n_sub - 1).start()
            end_tile(s, e, l, l == N_LAYER - 1)

            @pl.when(e == N_CHUNK - 1)
            def _():
                load_weights(1, l)

            @pl.when(l < N_LAYER - 1)
            def _():
                ring[(s + 1) % 3] = acc[:].astype(BF16)

            @pl.when(l == N_LAYER - 1)
            def _():
                @pl.when(top)
                def _():
                    pltpu.make_async_copy(targets.at[m], tgt, sems.t).wait()
                    err = acc[:].astype(BF16).astype(F32) - tgt[:].astype(F32)
                    loss_row[:] += jnp.sum(err * err, axis=0, keepdims=True)
                    zin[m] = (err * (1.0 / n_tok)).astype(BF16)

                @pl.when(jnp.logical_not(top))
                def _():
                    zout[:] = acc[:].astype(BF16)

                @pl.when(sent(e))
                def _():
                    z_copy(m).start()

            return 0

        n_fwd = N_TILE // 2
        lax.fori_loop(0, n_fwd, fwd_step, 0)
        for i in range(n_sub - N_SPARE, n_sub):
            z_out(n_fwd - 2, i).wait()
        for i in range(n_sub):
            z_out(n_fwd - 1, i).wait()
        for i in range(n_sub):
            z_in(n_fwd, i).start()

        def bwd_step(s, _):
            e, l = layer_of(s)
            m = e % N_CHUNK

            start_tile(s, e, l, l == N_LAYER - 1)
            for i in range(n_sub):
                z_in(s, i).wait()
            after = jnp.minimum(s + 1, N_TILE - 1)

            def z_next(i):
                store, _, _ = z_block(after, i, False)
                _, buf, b = z_block(s + 1, i, False)
                pltpu.make_async_copy(store, buf, sems.zi.at[b]).start()

            for i in range(N_SPARE):
                z_next(i)

            @pl.when(e == HALF + N_CHUNK)
            def _():
                wait_weights(l)

            for i, (off, w) in enumerate(subs):
                for o in range(0, w, BWD_BLOCK):
                    cut = slice(off + o, off + o + BWD_BLOCK)
                    g = ring[s % 3]
                    da = lax.dot_general(g, wdb[l, cut, :], NT, preferred_element_type=F32)
                    _, slope = gelu_and_slope(zb[(n_sub * s + i) % n_ring, :, o : o + BWD_BLOCK])
                    dz = (slope * da.astype(BF16).astype(F32)).astype(BF16)
                    part = lax.dot_general(dz, wub[l, :, cut], NT, preferred_element_type=F32)
                    acc[:] = (g.astype(F32) if i + o == 0 else acc[:]) + part
                if i + N_SPARE < n_sub:
                    z_next(i + N_SPARE)

            end_tile(s, e, l, l == 0)

            @pl.when(e == HALF + N_CHUNK - 1)
            def _():
                load_weights(0, l)

            @pl.when(l > 0)
            def _():
                ring[(s + 1) % 3] = acc[:].astype(BF16)

            @pl.when(l == 0)
            def _():
                zout[:] = acc[:].astype(BF16)

                @pl.when(sent(e))
                def _():
                    z_copy(m).start()

            return 0

        lax.fori_loop(n_fwd, N_TILE, bwd_step, 0)
        for i in range(n_sub):
            store, _, _ = z_block(N_TILE - 1, i, False)
            _, buf, b = z_block(N_TILE, i, False)
            pltpu.make_async_copy(store, buf, sems.zi.at[b]).wait()

        @pl.when(sent(2 * HALF - 1))
        def _():
            z_copy(0).wait_send()

        loss_ref[:] = jnp.broadcast_to(jnp.sum(loss_row[:], axis=1, keepdims=True), loss_ref.shape)

    width = window_width(ff)
    seg_d, seg_u = dd.shape[2], upp.shape[2]

    def grads(wub, wdb, hb, gb, gd, gu, cb, zw, ubb):
        def weight_copies(j):
            v, k = place.layer(j)
            start = pl.multiple_of(place.share(j).start(ff), 128)
            b = j % 2
            return (
                pltpu.make_async_copy(wu.at[v, k, :, pl.ds(start, width)], wub.at[b], sems.ww.at[b, 0]),
                pltpu.make_async_copy(wd.at[v, k, pl.ds(start, width), :], wdb.at[b], sems.ww.at[b, 1]),
            )

        def fetches(n):
            v, k = place.layer(n // N_STEP)
            t = n % N_STEP
            m, part = t // 2, 2 * (t % 2)
            h_at = N_CHUNK * v + part
            g_at = HALF + N_CHUNK * (1 - v) + part
            b = n % 2
            return (
                pltpu.make_async_copy(hg.at[m, pl.ds(h_at, 2), k], hb.at[b], sems.hb.at[b]),
                pltpu.make_async_copy(hg.at[m, pl.ds(g_at, 2), k], gb.at[b], sems.gb.at[b]),
            )

        def z_fetch(n):
            v, k = place.layer(n // N_STEP)
            start = pl.multiple_of(place.share(n // N_STEP).start(ff), 128)
            src = zs.at[pl.ds(N_CHUNK * v + 2 * (n % N_STEP), 2), k, :, pl.ds(start, width)]
            return pltpu.make_async_copy(src, zw.at[n % 2], sems.zw.at[n % 2])

        def arrived(group):
            ref = hg.at[2, pl.ds(0, HALF), 0] if group else hg.at[2, pl.ds(0, HALF)]
            remote(ref, ref, sems.c_send, sems.c_recv.at[group], z_peer).wait_recv()
            remote(ref, ref, sems.f_send, sems.f_recv.at[group], z_peer).wait_recv()

        def stage_copies(j):
            sh = place.share(j)
            b = j % 2
            up = []
            for i in range(4):
                keep = sh.piece(i)
                send = keep + sh.wu * (1 - 2 * sh.u)
                for to, row, sem in ((sup, send, 0), (kup, keep, 1)):
                    src = gu.at[b, pl.ds(pl.multiple_of(row * seg_u, 8), seg_u), :]
                    up.append(pltpu.make_async_copy(src, to.at[j, i], sems.st.at[sem]))
            base = sh.base(ff)
            part = [gd.at[b, pl.ds(pl.multiple_of(base + seg_d * i, 8), seg_d), :] for i in (c, 1 - c)]
            same = [pltpu.make_async_copy(part[0], to.at[j, 0], sems.st.at[2]) for to in (dd, sd)]
            other = pltpu.make_async_copy(part[1], sd.at[j, 1], sems.st.at[3])
            return sh, up, same, other

        def stage_out(j):
            sh, up, same, other = stage_copies(j)
            for cp in up:
                cp.start()
            other.start()
            pl.when(sh.away == 0)(same[0].start)
            pl.when(sh.away == 1)(same[1].start)

        def down_same(j, sh):
            return remote(sd.at[j, 0], dd.at[j, 1], sems.ds_send, sems.d_recv.at[j, 1], at(sh.dest_same))

        def up_exchange(j, sh):
            return remote(sup.at[j], ub.at[j], sems.u_send, sems.u_recv.at[j], at(sh.partner))

        def send_out(j):
            sh = place.share(j)
            pltpu.make_async_copy(sup.at[j], sup.at[j], sems.st.at[0]).wait()
            up_exchange(j, sh).start()
            pltpu.make_async_copy(sd.at[j, 1], sd.at[j, 1], sems.st.at[3]).wait()
            pltpu.make_async_copy(sd.at[j, 0], sd.at[j, 0], sems.st.at[2]).wait()

            @pl.when(sh.away == 0)
            def _():
                slot = sh.kc
                remote(
                    sd.at[j, 1], dd.at[j, slot], sems.d_send, sems.d_recv.at[j, slot], at(sh.core_peer)
                ).start()

            @pl.when(sh.away == 1)
            def _():
                remote(sd.at[j, 1], rb.at[j], sems.d_send, sems.r_recv.at[j], at(sh.core_peer)).start()
                down_same(j, sh).start()

            pltpu.make_async_copy(kup.at[j], kup.at[j], sems.st.at[1]).wait()

        def relay(j):
            sh = place.share(j)

            @pl.when((sh.away == 0) & (sh.kc == 0))
            def _():
                cp = remote(rb.at[j], rb.at[j], sems.r_send, sems.r_recv.at[j], z_peer)
                cp.wait_recv()
                remote(rb.at[j], dd.at[j, 1], sems.r_send, sems.d_recv.at[j, 1], at(sh.partner)).start()

        def tail_sends(j):
            sh = place.share(j)
            b = j % 2
            out = []
            for i in range(4):
                row = sh.piece(i) + sh.wu * (1 - 2 * sh.u)
                src = gu.at[b, pl.ds(pl.multiple_of(row * seg_u, 8), seg_u), :]
                out.append(remote(src, ub.at[j, i], sems.t_send, sems.u_recv.at[j], at(sh.partner)))
            base = sh.base(ff)
            same, other = [gd.at[b, pl.ds(pl.multiple_of(base + seg_d * i, 8), seg_d), :] for i in (c, 1 - c)]
            out.append(remote(other, dd.at[j, 1], sems.td_send, sems.d_recv.at[j, 1], at(sh.core_peer)))
            out.append(pltpu.make_async_copy(same, dd.at[j, 0], sems.st.at[2]))
            return out

        def piece_sends(j, b):
            sh = place.share(j)
            out = [pltpu.make_async_copy(cb.at[b, 0], upp.at[j, 0], sems.p_here.at[b])]
            for i in range(1, 4):
                out.append(remote(cb.at[b, i], upp.at[j, i], sems.p_send.at[b], sems.p_recv.at[j], at(sh.piece(i))))
            return out

        def wait_pieces(j, b):
            piece_sends(j, b)[0].wait()
            ref = cb.at[b, pl.ds(1, 3)]
            remote(ref, ref, sems.p_send.at[b], sems.p_recv.at[j], z_peer).wait_send()

        def sum_loads(j, b):
            return (
                pltpu.make_async_copy(kup.at[j], cb.at[b], sems.cl.at[0]),
                pltpu.make_async_copy(ub.at[j], ubb, sems.cl.at[1]),
            )

        def sum_load(j, b):
            up_exchange(j, place.share(j)).wait_recv()
            for cp in sum_loads(j, b):
                cp.start()

        def sum_add(j, b):
            for cp in sum_loads(j, b):
                cp.wait()
            cb[b] += ubb[:]
            for cp in piece_sends(j, b):
                cp.start()

        for cp in (*weight_copies(0), *fetches(0), z_fetch(0)):
            cp.start()

        loss_peers = [at(local_peers[i]) for i in (0, 1, 3)] + [z_peer]

        def loss_copy(r):
            return remote(lbuf.at[0, r], lbuf.at[1, r], sems.l_send, sems.l_recv.at[r], loss_peers[r])

        def step(n, _):
            j, t = n // N_STEP, n % N_STEP
            b, jb = n % 2, j % 2

            @pl.when(n < DELAY)
            def _():
                forward(n + N_TILE - DELAY)

            for group, first in enumerate((0, 3, 4, 5)):
                pl.when(n == first * N_STEP + 3)(lambda group=group: arrived(group))

            @pl.when(n + 1 < N_GRAD * N_STEP)
            def _():
                for cp in fetches(n + 1):
                    cp.start()

                pl.when((n + 1) % N_STEP < 2)(lambda: z_fetch(n + 1).start())

            for r in range(5):

                @pl.when(n == LOSS_AT[r])
                def _():
                    if r:
                        loss_copy(r - 1).wait()
                        loss_ref[:] += lbuf[1, r - 1]
                    if r < 4:
                        lbuf[0, r] = loss_ref[:]

                if r < 4:

                    @pl.when(n == LOSS_AT[r] + 1)
                    def _():
                        loss_copy(r).start()

            @pl.when(t == 0)
            def _():
                for cp in weight_copies(j):
                    cp.wait()

            @pl.when((t == 1) & (j + 1 < N_GRAD))
            def _():
                for cp in weight_copies(j + 1):
                    cp.start()

            @pl.when((t == 0) & (j >= 1))
            def _():
                stage_out(j - 1)

            @pl.when((t == 1) & (j >= 1))
            def _():
                send_out(j - 1)

            @pl.when((t == 2) & (j >= 1) & (j <= N_CHUNK))
            def _():
                relay(j - 1)

            for i, (b_, when) in SUM_AT.items():
                here = (stage == 0) | (i != 3)

                @pl.when((n == when) & here)
                def _():
                    if i == 4:
                        wait_pieces(0, 0)
                    sum_load(i, b_)

                @pl.when((n == when + 1) & here)
                def _():
                    sum_add(i, b_)

            for cp in fetches(n):
                cp.wait()
            h = hb[b].reshape(2 * rows, d)
            g = gb[b].reshape(2 * rows, d)

            def accumulate(own):
                for off, w in grad_blocks(width):
                    cut = slice(off, off + w)
                    if own:
                        z = zw[b, :, :, cut].reshape(2 * rows, w)
                    else:
                        z = jnp.dot(h, wub[jb, :, cut], preferred_element_type=F32)
                    da = lax.dot_general(g, wdb[jb, cut, :], NT, preferred_element_type=F32).astype(BF16).astype(F32)
                    a, slope = gelu_and_slope(z)
                    a = a.astype(BF16)
                    dz = (slope * da).astype(BF16)
                    down = lax.dot_general(a, g, TN, preferred_element_type=F32)
                    up = lax.dot_general(h, dz, TN, preferred_element_type=F32)
                    if own:
                        gd[jb, cut, :] = jnp.where(t == 0, 0.0, gd[jb, cut, :]) + down
                        gu[jb, :, cut] = jnp.where(t == 0, 0.0, gu[jb, :, cut]) + up
                    else:
                        gd[jb, cut, :] += down
                        gu[jb, :, cut] += up

            @pl.when(t < 2)
            def _():
                z_fetch(n).wait()
                accumulate(True)

            pl.when(t >= 2)(lambda: accumulate(False))
            return 0

        lax.fori_loop(0, N_GRAD * N_STEP, step, 0)
        last = N_GRAD - 1
        for cp in tail_sends(last):
            cp.start()
        wait_pieces(1, 1)
        up_exchange(last, place.share(last)).wait_recv()
        load = sum_loads(last, 1)[1]
        load.start()
        load.wait()
        for i in range(4):
            row = pl.multiple_of(place.share(last).piece(i) * seg_u, 8)
            cb[1, i] = gu[last % 2, pl.ds(row, seg_u), :] + ubb[i]
        for cp in piece_sends(last, 1):
            cp.start()

        @pl.when(stage == 1)
        def _():
            sum_load(3, 3)
            sum_add(3, 3)

        for j, b in ((2, 2), (4, 0), (last, 1), (3, 3)):
            wait_pieces(j, b)
        tail_sends(last)[-1].wait()
        remote(ub.at[last], ub.at[last], sems.t_send, sems.u_recv.at[last], z_peer).wait_send()
        tail_sends(last)[4].wait_send()

    pl.run_scoped(
        chain,
        pltpu.VMEM((N_LAYER, d, ff), BF16),
        pltpu.VMEM((N_LAYER, ff, d), BF16),
        pltpu.VMEM((3, *tile), BF16),
        pltpu.VMEM(tile, BF16),
        pltpu.VMEM((len(sub_blocks(ff)) + N_SPARE, rows, sub_blocks(ff)[0][1]), F32),
        pltpu.VMEM(tile, BF16),
        pltpu.VMEM(tile, F32),
        pltpu.VMEM((1, d), F32),
    )
    pl.run_scoped(
        grads,
        pltpu.VMEM((2, d, width), BF16),
        pltpu.VMEM((2, width, d), BF16),
        pltpu.VMEM((2, 2, *tile), BF16),
        pltpu.VMEM((2, 2, *tile), BF16),
        pltpu.VMEM((2, width, d), F32),
        pltpu.VMEM((2, d, width), F32),
        pltpu.VMEM((4, 4, seg_u, width), F32),
        pltpu.VMEM((2, 2, rows, width), F32),
        pltpu.VMEM((4, seg_u, width), F32),
    )

    for j in range(N_GRAD):
        sh = place.share(j)
        ref = upp.at[j, pl.ds(1, 3)]
        remote(ref, ref, sems.p_send.at[0], sems.p_recv.at[j], z_peer).wait_recv()
        ref = dd.at[j, 0]
        remote(ref, ref, sems.d_send, sems.d_recv.at[j, 1], z_peer).wait_recv()

        @pl.when(sh.away == 1)
        def _():
            remote(ref, ref, sems.ds_send, sems.d_recv.at[j, 0], z_peer).wait()

        @pl.when((sh.away == 0) & (sh.kc == 0))
        def _():
            remote(ref, ref, sems.r_send, sems.d_recv.at[j, 0], z_peer).wait_send()

    ref = sup.at[pl.ds(0, N_GRAD - 1)]
    remote(ref, ref, sems.u_send, sems.u_recv.at[0], z_peer).wait_send()
    ref = sd.at[pl.ds(0, N_GRAD - 1), 1]
    remote(ref, ref, sems.d_send, sems.d_recv.at[0, 0], z_peer).wait_send()
    for sem in (sems.a_send, sems.c_send, sems.f_send):
        remote(hg.at[0], hg.at[0], sem, sems.a_recv.at[0], z_peer).wait_send()


SEMS = {
    "w": (N_LAYER, 2),
    "zo": (N_RING,),
    "zi": (N_RING,),
    "z_recv": (N_CHUNK,),
    "a_recv": (N_TILE,),
    "c_recv": (N_CHUNK,),
    "f_recv": (N_CHUNK,),
    "ww": (2, 2),
    "hb": (2,),
    "gb": (2,),
    "zw": (2,),
    "st": (N_CHUNK,),
    "u_recv": (N_GRAD,),
    "d_recv": (N_GRAD, 2),
    "r_recv": (N_GRAD,),
    "cl": (2,),
    "p_send": (N_CHUNK,),
    "p_here": (N_CHUNK,),
    "p_recv": (N_GRAD,),
    "l_recv": (N_CHUNK,),
}
SEMS |= dict.fromkeys(("ld", "t", "z_send", "a_send", "c_send", "f_send", "u_send", "d_send"), ())
SEMS |= dict.fromkeys(("ds_send", "r_send", "t_send", "td_send", "l_send"), ())


class Sems:
    def __init__(self, refs):
        for name, ref in zip(SEMS, refs, strict=True):
            setattr(self, name, ref)


def step_call(tokens, targets, wu, wd, n_tok, n_data):
    n_chunk, rows, d = tokens.shape
    ff = wu.shape[-1]
    width = window_width(ff)
    pieces = jax.ShapeDtypeStruct((N_GRAD, 4, d // n_data, width), F32)
    parts = jax.ShapeDtypeStruct((N_GRAD, 2, ff // n_data, d), F32)

    def body(*refs):
        n = 14 + 2
        step_kernel(n_tok, *refs[:n], Sems(refs[n:]))

    return pl.pallas_call(
        body,
        in_specs=[ANY] * 4,
        out_specs=[ANY] * 3 + [pl.BlockSpec(memory_space=pltpu.VMEM)] + [ANY] * 6,
        out_shape=[
            jax.ShapeDtypeStruct((4, 2 * HALF, N_LAYER, rows, d), BF16),
            parts,
            pieces,
            jax.ShapeDtypeStruct((8, 128), F32),
            pieces,
            pieces,
            pieces,
            parts,
            jax.ShapeDtypeStruct((N_GRAD, ff // n_data, d), F32),
            jax.ShapeDtypeStruct((HALF, N_LAYER, rows, ff), F32),
        ],
        scratch_shapes=[
            pltpu.VMEM((n_chunk, rows, d), BF16),
            pltpu.VMEM((2, 4, 8, 128), F32),
            *[pltpu.SemaphoreType.DMA(shape) for shape in SEMS.values()],
        ],
        compiler_params=pltpu.CompilerParams(collective_id=0, has_side_effects=True, vmem_limit_bytes=67043328),
        name="step",
    )(tokens, targets, wu, wd)


def final_kernel(scal, dd, upp, down_ref, up_ref):
    down_ref[0, 0] = dd[0, 0] + dd[0, 1]
    width = upp.shape[-1]
    for i in range(4):
        start = pl.multiple_of(scal[4 * pl.program_id(0) + i], 128)
        up_ref[0, 0, :, pl.ds(start, width)] = upp[0, i]


def final_call(scal, dd, upp, n_data):
    seg_d, d = dd.shape[2:]
    seg_u, width = upp.shape[2:]
    ff = seg_d * n_data
    return pl.pallas_call(
        final_kernel,
        grid_spec=pltpu.PrefetchScalarGridSpec(
            num_scalar_prefetch=1,
            grid=(N_GRAD,),
            in_specs=[
                pl.BlockSpec((1, 2, seg_d, d), lambda j, s: (j, 0, 0, 0)),
                pl.BlockSpec((1, 4, seg_u, width), lambda j, s: (j, 0, 0, 0)),
            ],
            out_specs=[
                pl.BlockSpec((1, 1, seg_d, d), lambda j, s: (1 - j // N_LAYER, N_LAYER - 1 - j % N_LAYER, 0, 0)),
                pl.BlockSpec((1, 1, seg_u, ff), lambda j, s: (1 - j // N_LAYER, N_LAYER - 1 - j % N_LAYER, 0, 0)),
            ],
        ),
        out_shape=[
            jax.ShapeDtypeStruct((2, N_LAYER, seg_d, d), F32),
            jax.ShapeDtypeStruct((2, N_LAYER, seg_u, ff), F32),
        ],
        compiler_params=pltpu.CompilerParams(dimension_semantics=("arbitrary",), vmem_limit_bytes=62 * 2**20),
        name="final",
    )(scal, dd, upp)


def window_table(n_data, ff):
    table = []
    for i in range(2 * n_data):
        stage, dev = i // n_data, i % n_data
        shares = [(j, Place(stage, dev).share(j)) for j in range(N_GRAD)]
        table.append([Place(stage, sh.piece(i)).share(j).start(ff) for j, sh in shares for i in range(4)])
    return np.array(table, np.int32)


def solution(mesh):
    n_data = mesh.shape["data"]

    def device_fn(tokens_loc, targets_loc, wu, wd):
        n_micro, seq_len, d = tokens_loc.shape
        n_tok = n_data * n_micro * seq_len
        ff = wu.shape[-1]
        rows = n_micro * seq_len // N_CHUNK
        tokens = tokens_loc.reshape(N_CHUNK, rows, d)
        targets = targets_loc.reshape(N_CHUNK, rows, d)
        out = step_call(tokens, targets, wu, wd, n_tok, n_data)
        dd, upp, loss = out[1:4]
        starts = jnp.asarray(window_table(n_data, ff))
        row = lax.axis_index("stage") * n_data + lax.axis_index("data")
        scal = lax.dynamic_index_in_dim(starts, row, 0, keepdims=False)
        down, up = final_call(scal, dd, upp, n_data)
        return loss[0, 0] / (2.0 * n_tok), up, down

    return jax.shard_map(
        device_fn,
        mesh=mesh,
        in_specs=(P("data"), P("data"), P(None, "stage"), P(None, "stage")),
        out_specs=(P(), P(None, "stage", "data"), P(None, "stage", "data")),
        check_vma=False,
    )
```
